256 devices in a mesh: layer: 4 (over z_lo, core), harm: 64 (over y, z_hi, x).
Axes of the slice: x: 4, y: 4, z: 8 (z_hi: 4, z_lo: 2; z = z_hi * 2 + z_lo), core: 2. Of those that a mesh axis runs over, the one named last changes fastest.
Arguments:
- source: bfloat16 [2, 2048, 128], P(None, 'harm'), may hold values from -6 to 6
- transfer: bfloat16 [4, 2, 2048, 2048], P('layer', None, 'harm'), may hold values from -0.09375 to 0.09375
- fields: bfloat16 [4, 2, 2048, 128], P('layer', None, 'harm'), may hold values from -6 to 6
- orders: int32 [2048], replicated, may hold values from 0 to 2047, each once
Outputs:
- gradients: float32 [4, 2, 4096], P('layer', None, 'harm')
- boundary: bfloat16 [4, 2, 2048, 128], P('layer', None, 'harm')
The draws below stay inside these ranges and needn't reach their ends.
Inputs may be any that keep to these rules, and one draw needn't show every extreme that they name: `orders`: every value from 0 to 2047 appears exactly once.
All inputs are finite; a program needn't handle non-finite values.
Results may differ from the reference program's by a relative error of at most 0.006.
Values may be sent and summed in bfloat16 or wider, within the bound.
A program may use at most 64 MiB of HBM per device.

```python
import math
import jax
import jax.numpy as jnp
from jax import lax

HARM = 2048
LAYERS_DEV = 1
BATCH = 128
LAYERS = 4
N_HARM = 64


def shard_levels(key, extent, shards, least, high):
    def one(dim, blocks):
        draws = jax.random.uniform(jax.random.fold_in(jax.random.fold_in(key, 6), dim), (blocks,), jnp.float32, least / len(shards), high / len(shards))
        return jnp.repeat(jnp.exp(draws), extent[dim] // blocks).reshape((-1,) + (1,) * (len(extent) - dim - 1))

    level = one(*shards[0])
    for cut in shards[1:]:
        level = level * one(*cut)
    return level


def normal_values(stream_key, shape, deviation, bound, cuts=(), kind=jnp.bfloat16):
    drawn = jax.random.normal(stream_key, shape, jnp.float32) * deviation
    if len(cuts) > 0:
        drawn = shard_levels(stream_key, shape, cuts, -0.22, 0.18) * drawn
    return jnp.clip(drawn, min=-bound, max=bound).astype(kind)


def setup_inputs(seed: int = 0) -> dict:
    splits = jax.random.split(jax.random.key(seed), 5)
    source = normal_values(splits[0], (2, HARM, BATCH), 1.0, 6.0, ((1, 64),))
    transfer = normal_values(splits[1], (LAYERS, 2, HARM, HARM), (2 * HARM) ** -0.5, 0.09375, ((0, 4), (2, 64)))
    fields = normal_values(splits[2], (LAYERS, 2, HARM, BATCH), 1.0, 6.0, ((0, 4), (2, 64)))
    orders = jax.random.permutation(splits[3], HARM).astype(jnp.int32)
    return dict(source=source, transfer=transfer, fields=fields, orders=orders)


def correlate(adjoint, forward, position, band_start, band_width):
    harmonics = adjoint.shape[1]
    columns = adjoint.shape[2]
    adj_sorted = jnp.take(adjoint, position, axis=1).astype(jnp.float32)
    fwd_sorted = jnp.take(forward, position, axis=1).astype(jnp.float32)
    padded = jnp.pad(adj_sorted, ((0, 0), (harmonics, harmonics + 1), (0, 0)))
    window_slab = lax.dynamic_slice_in_dim(padded, band_start + 1, harmonics + band_width, 1)
    count = harmonics // band_width
    blocks = window_slab.reshape(2, count + 1, band_width, columns)
    windows = jnp.concatenate([blocks[:, :-1], blocks[:, 1:]], axis=2)
    forward_blocks = fwd_sorted.reshape(2, count, band_width, columns)

    def product(left_part, right_part):
        return jnp.einsum('nkb,ncb->nkc', left_part, right_part)
    real_part = product(forward_blocks[0], windows[0]) - product(forward_blocks[1], windows[1])
    imag_part = product(forward_blocks[0], windows[1]) + product(forward_blocks[1], windows[0])

    def diagonals(result_block):
        flattened = result_block.reshape(count, band_width * 2 * band_width)
        flattened = jnp.pad(flattened, ((0, 0), (0, band_width)))
        shaped = flattened.reshape(count, band_width, 2 * band_width + 1)[:, :, :band_width]
        return lax.optimization_barrier(jnp.sum(shaped, axis=(0, 1)))
    return jnp.stack([diagonals(real_part), diagonals(imag_part)])

def reference(source, transfer, fields, orders):
    harmonics = orders.shape[0]
    columns = source.shape[2]
    layer_count = transfer.shape[0]
    position = jnp.zeros((harmonics,), jnp.int32).at[orders].set(jnp.arange(harmonics, dtype=jnp.int32))
    band_width = 2 * harmonics // N_HARM
    norm_scale = 1.0 / math.sqrt(harmonics * columns)
    starts = jnp.arange(0, 2 * harmonics, band_width, dtype=jnp.int32)
    adjoint = source
    grads = [None] * layer_count
    bounds = []
    for layer_index in range(layer_count - 1, -1, -1):
        forward = fields[layer_index]
        bands = lax.map(lambda band_start: correlate(adjoint, forward, position, band_start, band_width), starts)
        grads[layer_index] = jnp.transpose(bands, (1, 0, 2)).reshape(2, 2 * harmonics) * norm_scale
        matrix = transfer[layer_index]
        real_part = jnp.dot(matrix[0], adjoint[0], preferred_element_type=jnp.float32) - jnp.dot(matrix[1], adjoint[1], preferred_element_type=jnp.float32)
        imag_part = jnp.dot(matrix[0], adjoint[1], preferred_element_type=jnp.float32) + jnp.dot(matrix[1], adjoint[0], preferred_element_type=jnp.float32)
        adjoint = jnp.stack([real_part, imag_part]).astype(jnp.bfloat16)
        if layer_index % LAYERS_DEV == 0:
            bounds.append(adjoint)
    return (jnp.stack(grads), jnp.stack(bounds[::-1]))
```

```python
import functools
import math

import jax
import jax.numpy as jnp
from jax import lax
from jax.experimental import pallas as pl
from jax.experimental.pallas import tpu as pltpu
from jax.sharding import PartitionSpec as P

MESH = pl.DeviceIdType.MESH
F32 = jnp.float32
BF16 = jnp.bfloat16


def pick(total, want):
    return want if total % want == 0 else total


def kernel(
    layers, peers, scale,
    source_ref, transfer_ref, fields_ref, orders_ref, grads_ref, bound_ref,
    adj, fwd, onehot, lined, factor, outgoing,
    src_sem, out_sem, fld_sem, adj_sem, fwd_sem,
):
    group = lax.axis_index("layer")
    me = lax.axis_index("harm")
    rows = source_ref.shape[1]
    cols = source_ref.shape[2]
    harm = rows * peers
    band = 2 * rows
    blocks = harm // band
    depth = min(256, harm)
    steps = harm // depth
    others = peers - 1
    mine = pl.ds(pl.multiple_of(me * rows, rows), rows)

    def send(src, dst, send_sem, recv_sem, target, index):
        return pltpu.make_async_remote_copy(
            src_ref=src, dst_ref=dst.at[:, mine, :], send_sem=send_sem, recv_sem=recv_sem,
            device_id=(target, index), device_id_type=MESH,
        )

    def to_others(src, dst, send_sem, recv_sem, target):
        @pl.loop(1, peers)
        def _(j):
            send(src, dst, send_sem, recv_sem, target, lax.rem(me + j, peers)).start()

    def wait_bytes(buffer, sem, count):
        part = buffer.at[:, pl.ds(0, count * rows), :]
        pltpu.make_async_copy(part, part, sem).wait()

    def columns(buffer, start, size):
        at = pl.ds(start, size)
        return jnp.concatenate([buffer[0, at, :], buffer[1, at, :]], axis=1)

    def propagate():
        total = jnp.zeros((2 * rows, 2 * cols), F32)
        for k in range(steps):
            at = pl.ds(k * depth, depth)
            matrix = jnp.concatenate([transfer_ref[0, 0, :, at], transfer_ref[0, 1, :, at]], axis=0)
            total += jnp.dot(matrix, columns(adj, k * depth, depth), preferred_element_type=F32)
        real = total[:rows, :cols] - total[rows:, cols:]
        imag = total[:rows, cols:] + total[rows:, :cols]
        result = jnp.stack([real, imag]).astype(BF16)
        bound_ref[0] = result
        outgoing[...] = result

        @pl.when(group > 0)
        def _():
            below = jnp.maximum(group - 1, 0)

            @pl.loop(0, peers)
            def _(j):
                send(outgoing, adj, out_sem, adj_sem, below, lax.rem(me + j, peers)).start()

    @pl.when(group == layers - 1)
    def _():
        to_others(source_ref, adj, src_sem, adj_sem, layers - 1)
        adj[:, mine, :] = source_ref[...]

    to_others(fields_ref.at[0], fwd, fld_sem, fwd_sem, group)
    fwd[:, mine, :] = fields_ref[0]

    border = harm - 16
    lined[pl.ds(0, border), :] = jnp.zeros((border, 2 * cols), BF16)
    lined[pl.ds(2 * harm, harm), :] = jnp.zeros((harm, 2 * cols), BF16)

    @pl.when(group == layers - 1)
    def _():
        wait_bytes(adj, adj_sem, others)
        propagate()

    chunk = min(256, harm)

    @pl.loop(0, harm // chunk)
    def _(r):
        index = lax.broadcasted_iota(jnp.int32, (chunk, depth), 0)
        order = r * chunk + (index // band) * band + (band - 1) - index % band
        for k in range(steps):
            hit = orders_ref[:, pl.ds(k * depth, depth)] == order
            onehot[pl.ds(pl.multiple_of(r * chunk, chunk), chunk), pl.ds(k * depth, depth)] = (
                jnp.where(hit, 1.0, 0.0).astype(BF16)
            )

    wait_bytes(fwd, fwd_sem, others)

    @pl.loop(0, harm // chunk)
    def _(r):
        at = pl.ds(pl.multiple_of(r * chunk, chunk), chunk)
        total = jnp.zeros((chunk, 2 * cols), F32)
        for k in range(steps):
            total += jnp.dot(
                onehot[at, pl.ds(k * depth, depth)], columns(fwd, k * depth, depth),
                preferred_element_type=F32,
            )
        for n in range(chunk // band):
            real = total[n * band : (n + 1) * band, :cols]
            imag = total[n * band : (n + 1) * band, cols:]
            pair = jnp.concatenate(
                [jnp.concatenate([real, -imag], axis=1), jnp.concatenate([imag, real], axis=1)], axis=0
            )
            factor[r * (chunk // band) + n] = pair.T.astype(BF16)

    tall = harm + 16
    part = pick(tall, 688)

    @pl.loop(0, tall // part)
    def _(r):
        order = r * part - 15 + lax.broadcasted_iota(jnp.int32, (part, depth), 0)

        @pl.loop(0, steps)
        def _(k):
            at = pl.ds(pl.multiple_of(k * depth, depth), depth)
            onehot[pl.ds(pl.multiple_of(r * part, 16), part), at] = (
                jnp.where(orders_ref[:, at] == order, 1.0, 0.0).astype(BF16)
            )

    @pl.when(group < layers - 1)
    def _():
        wait_bytes(adj, adj_sem, peers)
        propagate()

    @pl.loop(0, tall // part)
    def _(r):
        at = pl.ds(pl.multiple_of(r * part, 16), part)
        total = jnp.zeros((part, 2 * cols), F32)
        for k in range(steps):
            total += jnp.dot(
                onehot[at, pl.ds(k * depth, depth)], columns(adj, k * depth, depth),
                preferred_element_type=F32,
            )
        lined[pl.ds(pl.multiple_of(border + r * part, 16), part), :] = total.astype(BF16)

    gram = jnp.zeros((2 * band, 2 * band), F32)
    for n in range(blocks):
        window = lined[pl.ds(pl.multiple_of((me + n) * band, band), 2 * band), :]
        gram += jnp.dot(window, factor[n], preferred_element_type=F32)
    turned = pltpu.roll(gram.T, band + 1, 1, stride=1, stride_axis=0)
    real = jnp.sum(turned[:band], axis=0, keepdims=True)
    imag = jnp.sum(turned[band:], axis=0, keepdims=True)
    grads_ref[0, 0:1, :] = real[:, :band] * scale
    grads_ref[0, 1:2, :] = imag[:, band:] * scale

    wait_bytes(fwd, fld_sem, others)

    @pl.when(group == layers - 1)
    def _():
        wait_bytes(adj, src_sem, others)

    @pl.when(group > 0)
    def _():
        wait_bytes(adj, out_sem, peers)


def solution(mesh):
    layers, peers = mesh.shape["layer"], mesh.shape["harm"]

    def per_device(source, transfer, fields, orders):
        rows, cols = source.shape[1], source.shape[2]
        harm = rows * peers
        band = 2 * rows
        vmem = pl.BlockSpec(memory_space=pltpu.VMEM)
        return pl.pallas_call(
            functools.partial(kernel, layers, peers, 1.0 / math.sqrt(harm * cols)),
            out_shape=(
                jax.ShapeDtypeStruct((1, 2, band), F32),
                jax.ShapeDtypeStruct((1, 2, rows, cols), BF16),
            ),
            in_specs=[vmem] * 4,
            out_specs=(vmem, vmem),
            scratch_shapes=[
                pltpu.VMEM((2, harm, cols), BF16),
                pltpu.VMEM((2, harm, cols), BF16),
                pltpu.VMEM((harm + 16, harm), BF16),
                pltpu.VMEM((3 * harm, 2 * cols), BF16),
                pltpu.VMEM((harm // band, 2 * cols, 2 * band), BF16),
                pltpu.VMEM((2, rows, cols), BF16),
                pltpu.SemaphoreType.DMA,
                pltpu.SemaphoreType.DMA,
                pltpu.SemaphoreType.DMA,
                pltpu.SemaphoreType.DMA,
                pltpu.SemaphoreType.DMA,
            ],
            compiler_params=pltpu.CompilerParams(
                has_side_effects=True, vmem_limit_bytes=48 * 1024 * 1024
            ),
        )(source, transfer, fields, orders.reshape(1, harm))

    return jax.shard_map(
        per_device,
        mesh=mesh,
        in_specs=(
            P(None, "harm", None),
            P("layer", None, "harm", None),
            P("layer", None, "harm", None),
            P(),
        ),
        out_specs=(P("layer", None, "harm"), P("layer", None, "harm", None)),
        check_vma=False,
    )
```

```python
import functools
import math

import jax
import jax.numpy as jnp
from jax import lax
from jax.experimental import pallas as pl
from jax.experimental.pallas import tpu as pltpu
from jax.sharding import PartitionSpec as P

MESH = pl.DeviceIdType.MESH
F32 = jnp.float32
BF16 = jnp.bfloat16
MATES = 4


def kernel(
    layers, peers, scale,
    source_hbm, transfer_hbm, fields_hbm, orders_hbm, grads_ref, bound_ref,
    source, fields, orders, rows_all, adj, fwd, flat, hot_fwd, hot_adj, lined, factor,
    packed_src, packed_fld, outgoing, landed, partial, gathered,
    load_sem, send_sem, rows_sem, adj_sem, fwd_sem, land_sem, part_sem,
):
    group = lax.axis_index("layer")
    me = lax.axis_index("harm")
    mate = me % MATES
    clan = me // MATES
    clans = peers // MATES
    rows = source.shape[1]
    half = rows // 2
    cols = source.shape[2]
    slice_b = cols // MATES
    harm = rows * peers
    band = 2 * rows
    depth = min(256, harm)
    steps = harm // depth
    top = layers - 1

    loads = [
        pltpu.make_async_copy(source_hbm, source, load_sem.at[0]),
        pltpu.make_async_copy(orders_hbm, orders, load_sem.at[1]),
        pltpu.make_async_copy(fields_hbm.at[0], fields, load_sem.at[2]),
        pltpu.make_async_copy(transfer_hbm.at[0], rows_all.at[mate], load_sem.at[3]),
    ]
    for load in loads:
        load.start()

    barrier = pltpu.get_barrier_semaphore()
    with jax.named_scope("signal"):

        @pl.loop(1, peers)
        def _(j):
            pl.semaphore_signal(
                barrier, inc=1, device_id=(group, lax.rem(me + j, peers)), device_id_type=MESH
            )

        @pl.when(group < top)
        def _():
            above = jnp.minimum(group + 1, top)

            @pl.loop(0, clans)
            def _(j):
                pl.semaphore_signal(
                    barrier, inc=1, device_id=(above, j * MATES + mate), device_id_type=MESH
                )

    lane = lax.broadcasted_iota(jnp.int32, (1, cols), 1)
    in_slice = lax.rem(lane, 2 * slice_b)

    def pack(block, into):
        value = block[...].astype(F32)
        for m in range(MATES):
            parts = []
            for where in range(4):
                plane, upper = where % 2, where // 2
                piece = value[plane, upper * half : (upper + 1) * half, :]
                shift = (where - m) * slice_b % cols
                parts.append(pltpu.roll(piece, shift, 1) if shift else piece)
            tile = parts[3]
            for where in range(2, -1, -1):
                tile = jnp.where(lane < (where + 1) * slice_b, parts[where], tile)
            into[m] = tile.astype(BF16)

    with jax.named_scope("pack"):
        loads[0].wait()
        pack(source, packed_src)
        loads[2].wait()
        pack(fields, packed_fld)
        loads[1].wait()

    border = harm - 16
    chunk = min(256, harm)
    tall = harm + 16
    part = 688 if tall % 688 == 0 else tall

    with jax.named_scope("hots"):
        lined[pl.ds(0, border), :] = jnp.zeros((border, cols), BF16)
        lined[pl.ds(2 * harm, harm), :] = jnp.zeros((harm, cols), BF16)

    def build_fwd():
        @pl.loop(0, harm // chunk)
        def _(r):
            index = lax.broadcasted_iota(jnp.int32, (chunk, depth), 0)
            order = r * chunk + (index // band) * band + (band - 1) - index % band
            for k in range(steps):
                hit = orders[:, pl.ds(k * depth, depth)] == order
                hot_fwd[pl.ds(pl.multiple_of(r * chunk, chunk), chunk), pl.ds(k * depth, depth)] = (
                    jnp.where(hit, 1.0, 0.0).astype(BF16)
                )

    def build_adj():
        @pl.loop(0, tall // part)
        def _(r):
            order = r * part - 15 + lax.broadcasted_iota(jnp.int32, (part, depth), 0)

            @pl.loop(0, steps)
            def _(k):
                at = pl.ds(pl.multiple_of(k * depth, depth), depth)
                hot_adj[pl.ds(pl.multiple_of(r * part, 16), part), at] = (
                    jnp.where(orders[:, at] == order, 1.0, 0.0).astype(BF16)
                )

    with jax.named_scope("hots"):
        build_fwd()

    with jax.named_scope("barrier"):

        @pl.when(group > 0)
        def _():
            pl.semaphore_wait(barrier, peers - 1 + clans)

        @pl.when(group == 0)
        def _():
            pl.semaphore_wait(barrier, peers - 1)

    def remote(src, dst, sem, arrived, target, index):
        return pltpu.make_async_remote_copy(
            src_ref=src, dst_ref=dst, send_sem=send_sem.at[sem], recv_sem=arrived,
            device_id=(target, index), device_id_type=MESH,
        )

    def wait_for(buffer, count, sem):
        part_of = buffer.at[pl.ds(0, count)]
        pltpu.make_async_copy(part_of, part_of, sem).wait()

    def to_mates(sources, dst, sem, arrived):
        for j in range(1, MATES):
            other = lax.rem(mate + j, MATES)
            src = sources(other)
            remote(src, dst.at[mate], sem, arrived, group, clan * MATES + other).start()

    def scatter(tiles, dst, sem, arrived):
        @pl.loop(1, peers)
        def _(j):
            index = lax.rem(me + j, peers)
            remote(tiles.at[lax.rem(index, MATES)], dst.at[me], sem, arrived, group, index).start()

        dst[me] = tiles[mate]

    def send_fields():
        with jax.named_scope("sendf"):
            scatter(packed_fld, fwd, 2, fwd_sem)

    loads[3].wait()
    with jax.named_scope("spread"):
        to_mates(lambda other: rows_all.at[mate], rows_all, 0, rows_sem)

        @pl.when(group == top)
        def _():
            scatter(packed_src, adj, 1, adj_sem)

        @pl.when(group < top)
        def _():
            send_fields()

    def unpack(tiles, into):
        count = depth // rows
        for k in range(steps):
            value = tiles[pl.ds(k * count, count)].astype(F32)
            turned = pltpu.roll(value.reshape(count * half, cols), cols // 2, 1).reshape(value.shape)
            lower = jnp.where(lane < cols // 2, value, turned)
            upper = jnp.where(lane < cols // 2, turned, value)
            both = jnp.concatenate([lower, upper], axis=1).reshape(depth, cols)
            into[pl.ds(k * depth, depth), :] = both.astype(BF16)

    def propagate():
        with jax.named_scope("propagate"):
            unpack(adj, flat)
            total = jnp.zeros((MATES * 2 * rows, cols), F32)
            for k in range(steps):
                at = pl.ds(k * depth, depth)
                matrix = rows_all[:, :, :, at].reshape(MATES * 2 * rows, depth)
                total += jnp.dot(matrix, flat[at, :], preferred_element_type=F32)
            total = total.reshape(MATES, 2, rows, cols)
            cross = pltpu.roll(total[:, 1].reshape(MATES * rows, cols), slice_b, 1)
            cross = cross.reshape(MATES, rows, cols)
            result = total[:, 0] + jnp.where(in_slice < slice_b, -cross, cross)
            outgoing[...] = jnp.where(lane < cols // 2, result[:, :half], result[:, half:]).astype(BF16)

        with jax.named_scope("forward"):

            @pl.when(group > 0)
            def _():
                below = jnp.maximum(group - 1, 0)

                @pl.loop(0, clans)
                def _(j):
                    index = lax.rem(clan + j, clans) * MATES + mate
                    remote(
                        outgoing, adj.at[pl.ds(clan * MATES, MATES)], 3, adj_sem, below, index
                    ).start()

            landed[mate] = outgoing[mate]
            to_mates(lambda other: outgoing.at[other], landed, 4, land_sem)

    @pl.when(group == top)
    def _():
        with jax.named_scope("wait_t"):
            wait_for(rows_all, MATES - 1, rows_sem)
        with jax.named_scope("wait_a"):
            wait_for(adj, peers - 1, adj_sem)
        propagate()
        send_fields()

    with jax.named_scope("hots"):
        build_adj()

    with jax.named_scope("wait_f"):
        wait_for(fwd, peers - 1, fwd_sem)
    with jax.named_scope("sortf"):
        unpack(fwd, flat)
        sign = jnp.where(in_slice < slice_b, 1.0, -1.0)
        quads = chunk // band

        @pl.loop(0, harm // chunk)
        def _(r):
            at = pl.ds(pl.multiple_of(r * chunk, chunk), chunk)
            total = jnp.zeros((chunk, cols), F32)
            for k in range(steps):
                total += jnp.dot(
                    hot_fwd[at, pl.ds(k * depth, depth)], flat[pl.ds(k * depth, depth), :],
                    preferred_element_type=F32,
                )
            real = total * sign
            imag = pltpu.roll(total, slice_b, 1)
            for pair in range(quads // 2):
                lo, mid, hi = 2 * pair * band, (2 * pair + 1) * band, (2 * pair + 2) * band
                upper = jnp.where(lane < cols // 2, real[lo:mid], real[mid:hi])
                lower = jnp.where(lane < cols // 2, imag[lo:mid], imag[mid:hi])
                turned = jnp.concatenate([upper, lower], axis=0).T
                factor[r, pl.ds(pair * cols, cols), :] = turned.astype(BF16)

    @pl.when(group < top)
    def _():
        with jax.named_scope("wait_t"):
            wait_for(rows_all, MATES - 1, rows_sem)
        with jax.named_scope("wait_a"):
            wait_for(adj, peers, adj_sem)
        propagate()

    @pl.when(group == top)
    def _():
        unpack(adj, flat)

    with jax.named_scope("sorta"):

        @pl.loop(0, tall // part)
        def _(r):
            at = pl.ds(pl.multiple_of(r * part, 16), part)
            total = jnp.zeros((part, cols), F32)
            for k in range(steps):
                total += jnp.dot(
                    hot_adj[at, pl.ds(k * depth, depth)], flat[pl.ds(k * depth, depth), :],
                    preferred_element_type=F32,
                )
            lined[pl.ds(pl.multiple_of(border + r * part, 16), part), :] = total.astype(BF16)

    with jax.named_scope("gram"):
        quad = chunk // band
        tall_window = (MATES + 1) * band
        gram = jnp.zeros((tall_window, 2 * band), F32)
        for n in range(harm // chunk):
            start = (MATES * clan + quad * n) * band

            def window(m):
                return lined[pl.ds(pl.multiple_of(start + m * band, band), tall_window), :]

            left = jnp.concatenate(
                [
                    jnp.where(lane < cols // 2, window(2 * pair), window(2 * pair + 1))
                    for pair in range(quad // 2)
                ],
                axis=1,
            )
            gram += jnp.dot(left, factor[n], preferred_element_type=F32)
        for m in range(MATES):
            turned = pltpu.roll(gram[m * band : (m + 2) * band].T, band + 1, 1, stride=1, stride_axis=0)
            real = jnp.sum(turned[:band], axis=0, keepdims=True)
            imag = jnp.sum(turned[band:], axis=0, keepdims=True)
            partial[m] = jnp.where(lane < band, real, imag)

    with jax.named_scope("reduce"):
        gathered[mate] = partial[mate]
        to_mates(lambda other: partial.at[other], gathered, 5, part_sem)

    with jax.named_scope("land"):
        wait_for(landed, MATES - 1, land_sem)
        pieces = [landed[m].astype(F32) for m in range(MATES)]
        for plane in range(2):
            for upper in range(2):
                where = 2 * upper + plane
                tile = None
                for m in range(MATES):
                    shift = (m - where) * slice_b % cols
                    moved = pltpu.roll(pieces[m], shift, 1) if shift else pieces[m]
                    tile = moved if m == 0 else jnp.where(lane < m * slice_b, tile, moved)
                bound_ref[0, plane, pl.ds(upper * half, half), :] = tile.astype(BF16)

    with jax.named_scope("sum"):
        wait_for(gathered, MATES - 1, part_sem)
        total = gathered[0]
        for m in range(1, MATES):
            total = total + gathered[m]
        total = total * scale
        grads_ref[0, 0:1, :] = total[:, :band]
        grads_ref[0, 1:2, :] = total[:, band:]

    with jax.named_scope("drain"):
        wait_for(rows_all, MATES - 1, send_sem.at[0])
        wait_for(fwd, peers - 1, send_sem.at[2])
        wait_for(landed, MATES - 1, send_sem.at[4])
        wait_for(gathered, MATES - 1, send_sem.at[5])

        @pl.when(group == top)
        def _():
            wait_for(adj, peers - 1, send_sem.at[1])

        @pl.when(group > 0)
        def _():
            wait_for(adj, peers, send_sem.at[3])


def solution(mesh):
    layers, peers = mesh.shape["layer"], mesh.shape["harm"]

    def per_device(source, transfer, fields, orders):
        rows, cols = source.shape[1], source.shape[2]
        harm = rows * peers
        band = 2 * rows
        chunk = min(256, harm)
        vmem = pl.BlockSpec(memory_space=pltpu.VMEM)
        hbm = pl.BlockSpec(memory_space=pltpu.HBM)
        tile = (rows // 2, cols)
        return pl.pallas_call(
            functools.partial(kernel, layers, peers, 1.0 / math.sqrt(harm * cols)),
            out_shape=(
                jax.ShapeDtypeStruct((1, 2, band), F32),
                jax.ShapeDtypeStruct((1, 2, rows, cols), BF16),
            ),
            in_specs=[hbm] * 4,
            out_specs=(vmem, vmem),
            scratch_shapes=[
                pltpu.VMEM((2, rows, cols), BF16),
                pltpu.VMEM((2, rows, cols), BF16),
                pltpu.VMEM((1, harm), jnp.int32),
                pltpu.VMEM((MATES, 2, rows, harm), BF16),
                pltpu.VMEM((peers, *tile), BF16),
                pltpu.VMEM((peers, *tile), BF16),
                pltpu.VMEM((harm, cols), BF16),
                pltpu.VMEM((harm, harm), BF16),
                pltpu.VMEM((harm + 16, harm), BF16),
                pltpu.VMEM((3 * harm, cols), BF16),
                pltpu.VMEM((harm // chunk, chunk // band * 2 * (cols // MATES), 2 * band), BF16),
                pltpu.VMEM((MATES, *tile), BF16),
                pltpu.VMEM((MATES, *tile), BF16),
                pltpu.VMEM((MATES, *tile), BF16),
                pltpu.VMEM((MATES, *tile), BF16),
                pltpu.VMEM((MATES, 1, cols), F32),
                pltpu.VMEM((MATES, 1, cols), F32),
                pltpu.SemaphoreType.DMA((4,)),
                pltpu.SemaphoreType.DMA((6,)),
                pltpu.SemaphoreType.DMA,
                pltpu.SemaphoreType.DMA,
                pltpu.SemaphoreType.DMA,
                pltpu.SemaphoreType.DMA,
                pltpu.SemaphoreType.DMA,
            ],
            compiler_params=pltpu.CompilerParams(
                collective_id=0, has_side_effects=True, vmem_limit_bytes=56 * 1024 * 1024
            ),
        )(source, transfer, fields, orders.reshape(1, harm))

    return jax.shard_map(
        per_device,
        mesh=mesh,
        in_specs=(
            P(None, "harm", None),
            P("layer", None, "harm", None),
            P("layer", None, "harm", None),
            P(),
        ),
        out_specs=(P("layer", None, "harm"), P("layer", None, "harm", None)),
        check_vma=False,
    )
```

```python
import functools
import math

import jax
import jax.numpy as jnp
from jax import lax
from jax.experimental import pallas as pl
from jax.experimental.pallas import tpu as pltpu
from jax.sharding import PartitionSpec as P

MESH = pl.DeviceIdType.MESH
F32 = jnp.float32
BF16 = jnp.bfloat16
MATES = 4
LINES = 4


def kernel(
    layers, peers, scale,
    source_hbm, transfer_hbm, fields_hbm, orders_hbm, grads_ref, bound_ref,
    source, fields, orders, rows_all, adj, fwd, flat, stretched, hot_fwd, hot_adj, lined, factor,
    packed_src, packed_fld, stage_src, stage_fld, outgoing, landed, partial, gathered, sorting,
    load_sem, send_sem, rows_sem, adj_sem, fwd_sem, stage_sem, land_sem, part_sem, clear_sem, go_sem,
):
    group = lax.axis_index("layer")
    me = lax.axis_index("harm")
    mate = me % MATES
    clan = me // MATES
    clans = peers // MATES
    lines = min(LINES, clans)
    planes = clans // lines
    line = clan % lines
    plane_at = clan // lines
    rows = source.shape[1]
    half = rows // 2
    cols = source.shape[2]
    slice_b = cols // MATES
    harm = rows * peers
    band = 2 * rows
    depth = min(256, harm)
    steps = harm // depth
    top = layers - 1
    clan_rows = MATES * rows
    share = planes * clan_rows

    loads = [
        pltpu.make_async_copy(transfer_hbm.at[0], rows_all.at[mate], load_sem.at[3]),
        pltpu.make_async_copy(source_hbm, source, load_sem.at[0]),
        pltpu.make_async_copy(fields_hbm.at[0], fields, load_sem.at[2]),
        pltpu.make_async_copy(orders_hbm, orders, load_sem.at[1]),
    ]
    for load in loads:
        load.start()

    barrier = pltpu.get_barrier_semaphore()

    def mate_index(j):
        return clan * MATES + lax.rem(mate + j, MATES)

    def clan_index(far_line, far_plane):
        other = lax.rem(plane_at + far_plane, planes) * lines + lax.rem(line + far_line, lines)
        return other * MATES + mate

    def by_distance(size):
        return sorted(range(size), key=lambda d: -min(d, size - d))

    offsets = [(a, b) for a in by_distance(lines) for b in by_distance(planes)]

    with jax.named_scope("signal"):
        for a, b in offsets[:-1]:
            pl.semaphore_signal(
                barrier, inc=1, device_id=(group, clan_index(a, b)), device_id_type=MESH
            )
        for j in (2, 1, 3):
            pl.semaphore_signal(barrier, inc=1, device_id=(group, mate_index(j)), device_id_type=MESH)

        @pl.when(group > 0)
        def _():
            pl.semaphore_signal(
                barrier, inc=1, device_id=(jnp.maximum(group - 1, 0), me), device_id_type=MESH
            )

    lane = lax.broadcasted_iota(jnp.int32, (1, cols), 1)
    in_slice = lax.rem(lane, 2 * slice_b)

    def pack(block, into):
        value = block[...].astype(F32)
        for m in range(MATES):
            parts = []
            for where in range(4):
                plane, upper = where % 2, where // 2
                piece = value[plane, upper * half : (upper + 1) * half, :]
                shift = (where - m) * slice_b % cols
                parts.append(pltpu.roll(piece, shift, 1) if shift else piece)
            tile = parts[3]
            for where in range(2, -1, -1):
                tile = jnp.where(lane < (where + 1) * slice_b, parts[where], tile)
            into[m] = tile.astype(BF16)

    border = harm - 16
    chunk = min(256, harm)
    tall = harm + 16
    part = 688 if tall % 688 == 0 else tall

    with jax.named_scope("pack"):
        loads[1].wait()
        pack(source, packed_src)
        loads[2].wait()
        pack(fields, packed_fld)
        lined[pl.ds(0, border), :] = jnp.zeros((border, cols), BF16)
        lined[pl.ds(2 * harm, harm), :] = jnp.zeros((harm, cols), BF16)
        loads[3].wait()
        loads[0].wait()

    def build_fwd():
        with jax.named_scope("hotf"):

            @pl.loop(0, harm // chunk)
            def _(r):
                index = lax.broadcasted_iota(jnp.int32, (chunk, depth), 0)
                order = r * chunk + (index // band) * band + (band - 1) - index % band
                for k in range(steps):
                    hit = orders[:, pl.ds(k * depth, depth)] == order
                    hot_fwd[
                        pl.ds(pl.multiple_of(r * chunk, chunk), chunk), pl.ds(k * depth, depth)
                    ] = jnp.where(hit, 1.0, 0.0).astype(BF16)

    def build_adj():
        with jax.named_scope("hota"):

            @pl.loop(0, tall // part)
            def _(r):
                order = r * part - 15 + lax.broadcasted_iota(jnp.int32, (part, clan_rows), 0)

                @pl.loop(0, clans)
                def _(k):
                    at = pl.ds(pl.multiple_of(k * clan_rows, clan_rows), clan_rows)
                    to = (k % lines) * planes + k // lines
                    to = pl.ds(pl.multiple_of(to * clan_rows, clan_rows), clan_rows)
                    hot_adj[pl.ds(pl.multiple_of(r * part, 16), part), to] = (
                        jnp.where(orders[:, at] == order, 1.0, 0.0).astype(BF16)
                    )

    with jax.named_scope("barrier"):

        @pl.when(group < top)
        def _():
            pl.semaphore_wait(barrier, clans - 1 + MATES)
            pl.semaphore_signal(
                clear_sem, inc=1, device_id=(jnp.minimum(group + 1, top), me), device_id_type=MESH
            )

        @pl.when(group == top)
        def _():
            pl.semaphore_wait(barrier, clans - 1 + MATES - 1)

    def remote(src, dst, sem, arrived, target, index):
        return pltpu.make_async_remote_copy(
            src_ref=src, dst_ref=dst, send_sem=send_sem.at[sem], recv_sem=arrived,
            device_id=(target, index), device_id_type=MESH,
        )

    def wait_for(buffer, count, sem):
        part_of = buffer.at[pl.ds(0, count)]
        pltpu.make_async_copy(part_of, part_of, sem).wait()

    def to_mates(tiles, dst, sem, arrived):
        for j in (2, 1, 3):
            other = lax.rem(mate + j, MATES)
            remote(
                tiles.at[other], dst.at[mate], sem, arrived, group, clan * MATES + other
            ).start()
        dst[mate] = tiles[mate]

    clan_tiles = pl.ds(clan * MATES, MATES)

    def to_clans(tiles, dst, sem, arrived, target, everyone):
        for a, b in offsets if everyone else offsets[:-1]:
            remote(tiles, dst.at[clan_tiles], sem, arrived, target, clan_index(a, b)).start()

    right, left = mate_index(1), mate_index(MATES - 1)
    from_left, from_right = lax.rem(mate + MATES - 1, MATES), lax.rem(mate + 1, MATES)

    def start_rows():
        for first in (0, 1):
            to_right = rows_all.at[mate, first]
            to_left = rows_all.at[mate, 1 - first]
            remote(to_right, to_right, 0, rows_sem.at[2 * first], group, right).start()
            remote(to_left, to_left, 0, rows_sem.at[2 * first + 1], group, left).start()

    def wait_half(sem):
        wait_for(rows_all.at[0], 1, rows_sem.at[sem])

    def relay_rows():
        with jax.named_scope("relay_t"):
            wait_half(0)
            block = rows_all.at[from_left, 0]
            remote(block, block, 1, rows_sem.at[4], group, right).start()
            wait_half(1)
            block = rows_all.at[from_right, 1]
            remote(block, block, 1, rows_sem.at[5], group, left).start()

    def wait_rows():
        with jax.named_scope("wait_t"):
            for k in (2, 3, 4, 5):
                wait_half(k)

    def start_fields():
        to_mates(packed_fld, stage_fld, 2, stage_sem.at[0])

    def relay_fields():
        with jax.named_scope("relay_f"):
            wait_for(stage_fld, MATES - 1, stage_sem.at[0])
            to_clans(stage_fld, fwd, 3, fwd_sem, group, False)
            fwd[clan_tiles] = stage_fld[...]

    with jax.named_scope("spread"):

        @pl.when(group == top)
        def _():
            to_mates(packed_src, stage_src, 4, stage_sem.at[1])
            start_rows()
            with jax.named_scope("relay_s"):
                wait_for(stage_src, MATES - 1, stage_sem.at[1])
                to_clans(stage_src, adj, 5, adj_sem.at[line], top, False)
                adj[clan_tiles] = stage_src[...]
            relay_rows()
            pl.semaphore_wait(clear_sem, 1)
            pl.semaphore_signal(go_sem, inc=1, device_id=(top - 1, me), device_id_type=MESH)

        @pl.when(group == top - 1)
        def _():
            build_fwd()
            build_adj()
            with jax.named_scope("wait_go"):
                pl.semaphore_wait(go_sem, 1)
            start_fields()
            start_rows()
            relay_fields()
            relay_rows()

        @pl.when(group < top - 1)
        def _():
            build_fwd()
            build_adj()
            start_fields()
            start_rows()
            relay_fields()
            relay_rows()

    def unpack(tiles):
        count = tiles.shape[0]
        value = tiles.astype(F32)
        turned = pltpu.roll(value.reshape(count * half, cols), cols // 2, 1).reshape(value.shape)
        lower = jnp.where(lane < cols // 2, value, turned)
        upper = jnp.where(lane < cols // 2, turned, value)
        return jnp.concatenate([lower, upper], axis=1).reshape(count * rows, cols).astype(BF16)

    def sort_share(far, first, last):
        z = lax.rem(line + far, lines)
        at = pl.ds(pl.multiple_of(z * share, share), share)

        @pl.loop(0, tall // part)
        def _(r):
            here = pl.ds(pl.multiple_of(r * part, 16), part)
            total = jnp.dot(hot_adj[here, at], flat[at, :], preferred_element_type=F32)
            if not first:
                total += sorting[here, :]
            if last:
                lined[pl.ds(pl.multiple_of(border + r * part, 16), part), :] = total.astype(BF16)
            else:
                sorting[here, :] = total

    near_first = by_distance(lines)[::-1]

    def receive(sort):
        total = jnp.zeros((MATES * 2 * rows, cols), F32)
        for step, far in enumerate(near_first):
            z = lax.rem(line + far, lines)
            with jax.named_scope("wait_a%d" % step):
                if step == 0:

                    @pl.when(group == top)
                    def _():
                        wait_for(adj, MATES * (planes - 1), adj_sem.at[z])

                    @pl.when(group < top)
                    def _():
                        wait_for(adj, MATES * planes, adj_sem.at[z])
                else:
                    wait_for(adj, MATES * planes, adj_sem.at[z])
            with jax.named_scope("propagate"):
                blocks = [adj[pl.ds((p * lines + z) * MATES, MATES)] for p in range(planes)]
                right_side = unpack(jnp.concatenate(blocks, axis=0))
                flat[pl.ds(pl.multiple_of(z * share, share), share), :] = right_side
                matrix = jnp.concatenate(
                    [
                        rows_all[
                            :, :, :, pl.ds(pl.multiple_of((p * lines + z) * clan_rows, clan_rows), clan_rows)
                        ].reshape(MATES * 2 * rows, clan_rows)
                        for p in range(planes)
                    ],
                    axis=1,
                )
                total += jnp.dot(matrix, right_side, preferred_element_type=F32)
            last = step == lines - 1
            if last:
                with jax.named_scope("forward"):
                    total = total.reshape(MATES, 2, rows, cols)
                    cross = pltpu.roll(total[:, 1].reshape(MATES * rows, cols), slice_b, 1)
                    cross = cross.reshape(MATES, rows, cols)
                    result = total[:, 0] + jnp.where(in_slice < slice_b, -cross, cross)
                    outgoing[...] = jnp.where(
                        lane < cols // 2, result[:, :half], result[:, half:]
                    ).astype(BF16)
                    if not sort:
                        below = jnp.maximum(group - 1, 0)

                        @pl.when(group < top)
                        def _():
                            pl.semaphore_wait(clear_sem, 1)

                        to_clans(outgoing, adj, 6, adj_sem.at[line], below, True)
                    to_mates(outgoing, landed, 7, land_sem)
            if sort:
                with jax.named_scope("sort0"):
                    sort_share(far, step == 0, last)

    @pl.when(group >= top - 1)
    def _():
        wait_rows()
        receive(False)

    @pl.when(group == top)
    def _():
        start_fields()
        build_fwd()
        relay_fields()
        build_adj()

    with jax.named_scope("wait_f"):
        wait_for(fwd, peers - MATES, fwd_sem)
    with jax.named_scope("sortf"):
        for k in range(steps):
            count = depth // rows
            flat_fwd = unpack(fwd[pl.ds(k * count, count)])
            stretched[pl.ds(k * depth, depth), :] = flat_fwd
        sign = jnp.where(in_slice < slice_b, 1.0, -1.0)
        quads = chunk // band

        @pl.loop(0, harm // chunk)
        def _(r):
            at = pl.ds(pl.multiple_of(r * chunk, chunk), chunk)
            total = jnp.zeros((chunk, cols), F32)
            for k in range(steps):
                total += jnp.dot(
                    hot_fwd[at, pl.ds(k * depth, depth)], stretched[pl.ds(k * depth, depth), :],
                    preferred_element_type=F32,
                )
            real = total * sign
            imag = pltpu.roll(total, slice_b, 1)
            for pair in range(quads // 2):
                lo, mid, hi = 2 * pair * band, (2 * pair + 1) * band, (2 * pair + 2) * band
                upper = jnp.where(lane < cols // 2, real[lo:mid], real[mid:hi])
                lower = jnp.where(lane < cols // 2, imag[lo:mid], imag[mid:hi])
                turned = jnp.concatenate([upper, lower], axis=0).T
                factor[r, pl.ds(pair * cols, cols), :] = turned.astype(BF16)

    @pl.when(group == 1)
    def _():
        wait_rows()
        receive(False)

    @pl.when(group == 0)
    def _():
        wait_rows()
        receive(True)

    @pl.when(group > 0)
    def _():
        with jax.named_scope("sorta"):
            for step, far in enumerate(near_first):
                sort_share(far, step == 0, step == lines - 1)

    with jax.named_scope("gram"):
        quad = chunk // band
        tall_window = (MATES + 1) * band
        gram = jnp.zeros((tall_window, 2 * band), F32)
        for n in range(harm // chunk):
            start = (MATES * clan + quad * n) * band

            def window(m):
                return lined[pl.ds(pl.multiple_of(start + m * band, band), tall_window), :]

            left = jnp.concatenate(
                [
                    jnp.where(lane < cols // 2, window(2 * pair), window(2 * pair + 1))
                    for pair in range(quad // 2)
                ],
                axis=1,
            )
            gram += jnp.dot(left, factor[n], preferred_element_type=F32)
        for m in range(MATES):
            turned = pltpu.roll(gram[m * band : (m + 2) * band].T, band + 1, 1, stride=1, stride_axis=0)
            real = jnp.sum(turned[:band], axis=0, keepdims=True)
            imag = jnp.sum(turned[band:], axis=0, keepdims=True)
            partial[m] = jnp.where(lane < band, real, imag)

    with jax.named_scope("reduce"):
        to_mates(partial, gathered, 8, part_sem)

    with jax.named_scope("land"):
        wait_for(landed, MATES - 1, land_sem)
        pieces = [landed[m].astype(F32) for m in range(MATES)]
        for plane in range(2):
            for upper in range(2):
                where = 2 * upper + plane
                tile = None
                for m in range(MATES):
                    shift = (m - where) * slice_b % cols
                    moved = pltpu.roll(pieces[m], shift, 1) if shift else pieces[m]
                    tile = moved if m == 0 else jnp.where(lane < m * slice_b, tile, moved)
                bound_ref[0, plane, pl.ds(upper * half, half), :] = tile.astype(BF16)

    with jax.named_scope("sum"):
        wait_for(gathered, MATES - 1, part_sem)
        total = gathered[0]
        for m in range(1, MATES):
            total = total + gathered[m]
        total = total * scale
        grads_ref[0, 0:1, :] = total[:, :band]
        grads_ref[0, 1:2, :] = total[:, band:]

    with jax.named_scope("drain"):
        wait_for(rows_all, 2, send_sem.at[0])
        wait_for(rows_all, 1, send_sem.at[1])
        wait_for(stage_fld, MATES - 1, send_sem.at[2])
        wait_for(fwd, peers - MATES, send_sem.at[3])
        wait_for(landed, MATES - 1, send_sem.at[7])
        wait_for(gathered, MATES - 1, send_sem.at[8])

        @pl.when(group == top)
        def _():
            wait_for(stage_src, MATES - 1, send_sem.at[4])
            wait_for(adj, peers - MATES, send_sem.at[5])

        @pl.when(group > 0)
        def _():
            wait_for(adj, peers, send_sem.at[6])


def solution(mesh):
    layers, peers = mesh.shape["layer"], mesh.shape["harm"]

    def per_device(source, transfer, fields, orders):
        rows, cols = source.shape[1], source.shape[2]
        harm = rows * peers
        band = 2 * rows
        chunk = min(256, harm)
        vmem = pl.BlockSpec(memory_space=pltpu.VMEM)
        hbm = pl.BlockSpec(memory_space=pltpu.HBM)
        tile = (rows // 2, cols)
        return pl.pallas_call(
            functools.partial(kernel, layers, peers, 1.0 / math.sqrt(harm * cols)),
            out_shape=(
                jax.ShapeDtypeStruct((1, 2, band), F32),
                jax.ShapeDtypeStruct((1, 2, rows, cols), BF16),
            ),
            in_specs=[hbm] * 4,
            out_specs=(vmem, vmem),
            scratch_shapes=[
                pltpu.VMEM((2, rows, cols), BF16),
                pltpu.VMEM((2, rows, cols), BF16),
                pltpu.VMEM((1, harm), jnp.int32),
                pltpu.VMEM((MATES, 2, rows, harm), BF16),
                pltpu.VMEM((peers, *tile), BF16),
                pltpu.VMEM((peers, *tile), BF16),
                pltpu.VMEM((harm, cols), BF16),
                pltpu.VMEM((harm, cols), BF16),
                pltpu.VMEM((harm, harm), BF16),
                pltpu.VMEM((harm + 16, harm), BF16),
                pltpu.VMEM((3 * harm, cols), BF16),
                pltpu.VMEM((harm // chunk, chunk // band * 2 * (cols // MATES), 2 * band), BF16),
                *[pltpu.VMEM((MATES, *tile), BF16)] * 6,
                pltpu.VMEM((MATES, 1, cols), F32),
                pltpu.VMEM((MATES, 1, cols), F32),
                pltpu.VMEM((harm + 16, cols), F32),
                pltpu.SemaphoreType.DMA((4,)),
                pltpu.SemaphoreType.DMA((9,)),
                pltpu.SemaphoreType.DMA((6,)),
                pltpu.SemaphoreType.DMA((LINES,)),
                pltpu.SemaphoreType.DMA,
                pltpu.SemaphoreType.DMA((2,)),
                pltpu.SemaphoreType.DMA,
                pltpu.SemaphoreType.DMA,
                pltpu.SemaphoreType.REGULAR,
                pltpu.SemaphoreType.REGULAR,
            ],
            compiler_params=pltpu.CompilerParams(
                collective_id=0, has_side_effects=True, vmem_limit_bytes=44 * 1024 * 1024
            ),
        )(
            *(
                pltpu.with_memory_space_constraint(value, pltpu.HBM)
                for value in (source, transfer, fields, orders.reshape(1, harm))
            )
        )

    return jax.shard_map(
        per_device,
        mesh=mesh,
        in_specs=(
            P(None, "harm", None),
            P("layer", None, "harm", None),
            P("layer", None, "harm", None),
            P(),
        ),
        out_specs=(P("layer", None, "harm"), P("layer", None, "harm", None)),
        check_vma=False,
    )
```

```python
import functools
import math

import jax
import jax.numpy as jnp
from jax import lax
from jax.experimental import pallas as pl
from jax.experimental.pallas import tpu as pltpu
from jax.sharding import PartitionSpec as P

MESH = pl.DeviceIdType.MESH
F32 = jnp.float32
BF16 = jnp.bfloat16
MATES = 4
LINES = 4


def kernel(
    layers, peers, scale,
    source_hbm, transfer_hbm, fields_hbm, orders_hbm, grads_ref, bound_ref,
    source, fields, orders, rows_all, adj, fwd, stretched, column, hot_fwd, hot_adj, lined, shifted, factor,
    packed_src, packed_fld, stage_src, stage_fld, outgoing, landed, partial, gathered, sorting,
    load_sem, send_sem, rows_sem, adj_sem, fwd_sem, stage_sem, land_sem, part_sem, clear_sem, go_sem,
    line_sem, plane_sem,
):
    group = lax.axis_index("layer")
    me = lax.axis_index("harm")
    mate = me % MATES
    clan = me // MATES
    clans = peers // MATES
    lines = min(LINES, clans)
    planes = clans // lines
    line = clan % lines
    plane_at = clan // lines
    rows = source.shape[1]
    half = rows // 2
    cols = source.shape[2]
    slice_b = cols // MATES
    harm = rows * peers
    band = 2 * rows
    depth = min(256, harm)
    steps = harm // depth
    top = layers - 1
    clan_rows = MATES * rows
    share = planes * clan_rows

    loads = [
        pltpu.make_async_copy(transfer_hbm.at[0], rows_all.at[mate], load_sem.at[3]),
        pltpu.make_async_copy(source_hbm, source, load_sem.at[0]),
        pltpu.make_async_copy(fields_hbm.at[0], fields, load_sem.at[2]),
        pltpu.make_async_copy(orders_hbm, orders, load_sem.at[1]),
    ]
    for load in loads:
        load.start()

    barrier = pltpu.get_barrier_semaphore()

    def mate_index(j):
        return clan * MATES + lax.rem(mate + j, MATES)

    def place(plane, line_of):
        return (plane * lines + line_of) * MATES + mate

    def clan_index(far_line, far_plane):
        return place(lax.rem(plane_at + far_plane, planes), lax.rem(line + far_line, lines))

    def by_distance(size):
        return sorted(range(size), key=lambda d: -min(d, size - d))

    offsets = [(a, b) for a in by_distance(lines) for b in by_distance(planes)]

    near_lines = [place(plane_at, lax.rem(line + far, lines)) for far in (1, lines - 1)]
    near_planes = [place(lax.rem(plane_at + far, planes), line) for far in (2, 1, 3)]

    with jax.named_scope("signal"):
        for index in near_lines + near_planes + [mate_index(j) for j in (2, 1, 3)]:
            pl.semaphore_signal(barrier, inc=1, device_id=(group, index), device_id_type=MESH)

        @pl.when(group > 0)
        def _():
            pl.semaphore_signal(
                barrier, inc=1, device_id=(jnp.maximum(group - 1, 0), me), device_id_type=MESH
            )

    lane = lax.broadcasted_iota(jnp.int32, (1, cols), 1)
    in_slice = lax.rem(lane, 2 * slice_b)

    def pack(block, into):
        value = block[...].astype(F32)
        for m in range(MATES):
            parts = []
            for where in range(4):
                plane, upper = where % 2, where // 2
                piece = value[plane, upper * half : (upper + 1) * half, :]
                shift = (where - m) * slice_b % cols
                parts.append(pltpu.roll(piece, shift, 1) if shift else piece)
            tile = parts[3]
            for where in range(2, -1, -1):
                tile = jnp.where(lane < (where + 1) * slice_b, parts[where], tile)
            into[m] = tile.astype(BF16)

    border = harm - cols
    wide = harm + 2 * cols
    chunk = min(256, harm)

    with jax.named_scope("pack"):
        loads[1].wait()
        pack(source, packed_src)
        loads[2].wait()
        pack(fields, packed_fld)
        for buffer in (lined, shifted):
            buffer[:, pl.ds(0, border)] = jnp.zeros((2 * slice_b, border), BF16)
            buffer[:, pl.ds(border + wide, border)] = jnp.zeros((2 * slice_b, border), BF16)
        loads[3].wait()
        loads[0].wait()

    def build_fwd():
        with jax.named_scope("hotf"):

            @pl.loop(0, harm // chunk)
            def _(r):
                index = lax.broadcasted_iota(jnp.int32, (chunk, depth), 0)
                order = r * chunk + (index // band) * band + (band - 1) - index % band
                for k in range(steps):
                    hit = orders[:, pl.ds(k * depth, depth)] == order
                    hot_fwd[
                        pl.ds(pl.multiple_of(r * chunk, chunk), chunk), pl.ds(k * depth, depth)
                    ] = jnp.where(hit, 1.0, 0.0).astype(BF16)

    def build_adj():
        with jax.named_scope("hota"):
            for k in range(harm // cols):
                row = orders[:, pl.ds(k * cols, cols)].astype(F32)
                column[pl.ds(k * cols, cols), :] = jnp.broadcast_to(row, (cols, cols)).T

            @pl.loop(0, peers)
            def _(tile):
                owner = tile // MATES
                spot = (owner // lines) * MATES + tile % MATES
                for upper in range(2):
                    order = column[pl.ds(pl.multiple_of(tile * rows + upper * half, half), half), :]
                    row = (owner % lines) * share + upper * (share // 2) + spot * half
                    row = pl.ds(pl.multiple_of(row, half), half)
                    for k in range(wide // cols):
                        want = (lane + (k * cols - cols + 1)).astype(F32)
                        hot_adj[row, pl.ds(k * cols, cols)] = jnp.where(order == want, 1.0, 0.0).astype(BF16)

    with jax.named_scope("barrier"):

        @pl.when(group < top)
        def _():
            pl.semaphore_wait(barrier, len(near_lines) + len(near_planes) + MATES)

        @pl.when(group == top)
        def _():
            pl.semaphore_wait(barrier, len(near_lines) + len(near_planes) + MATES - 1)

        for index in near_lines:
            pl.semaphore_signal(line_sem, inc=1, device_id=(group, index), device_id_type=MESH)

    def all_here():
        with jax.named_scope("here"):
            pl.semaphore_wait(line_sem, len(near_lines))
            for index in near_planes:
                pl.semaphore_signal(plane_sem, inc=1, device_id=(group, index), device_id_type=MESH)
            pl.semaphore_wait(plane_sem, len(near_planes))

            @pl.when(group < top)
            def _():
                pl.semaphore_signal(
                    clear_sem, inc=1, device_id=(jnp.minimum(group + 1, top), me), device_id_type=MESH
                )

    def remote(src, dst, sem, arrived, target, index):
        return pltpu.make_async_remote_copy(
            src_ref=src, dst_ref=dst, send_sem=send_sem.at[sem], recv_sem=arrived,
            device_id=(target, index), device_id_type=MESH,
        )

    def wait_for(buffer, count, sem):
        part_of = buffer.at[pl.ds(0, count)]
        pltpu.make_async_copy(part_of, part_of, sem).wait()

    def to_mates(tiles, dst, sem, arrived):
        for j in (2, 1, 3):
            other = lax.rem(mate + j, MATES)
            remote(
                tiles.at[other], dst.at[mate], sem, arrived, group, clan * MATES + other
            ).start()
        dst[mate] = tiles[mate]

    clan_tiles = pl.ds(clan * MATES, MATES)

    def to_clans(tiles, dst, sem, arrived, target, everyone):
        for a, b in offsets if everyone else offsets[:-1]:
            remote(tiles, dst.at[clan_tiles], sem, arrived, target, clan_index(a, b)).start()

    right, left = mate_index(1), mate_index(MATES - 1)
    from_left, from_right = lax.rem(mate + MATES - 1, MATES), lax.rem(mate + 1, MATES)

    def start_rows():
        for first in (0, 1):
            to_right = rows_all.at[mate, first]
            to_left = rows_all.at[mate, 1 - first]
            remote(to_right, to_right, 0, rows_sem.at[2 * first], group, right).start()
            remote(to_left, to_left, 0, rows_sem.at[2 * first + 1], group, left).start()

    def wait_half(sem):
        wait_for(rows_all.at[0], 1, rows_sem.at[sem])

    def relay_rows():
        with jax.named_scope("relay_t"):
            wait_half(0)
            block = rows_all.at[from_left, 0]
            remote(block, block, 1, rows_sem.at[4], group, right).start()
            wait_half(1)
            block = rows_all.at[from_right, 1]
            remote(block, block, 1, rows_sem.at[5], group, left).start()

    def wait_rows():
        with jax.named_scope("wait_t"):
            for k in (2, 3, 4, 5):
                wait_half(k)

    def start_fields():
        to_mates(packed_fld, stage_fld, 2, stage_sem.at[0])

    def relay_fields():
        with jax.named_scope("relay_f"):
            wait_for(stage_fld, MATES - 1, stage_sem.at[0])
            to_clans(stage_fld, fwd, 3, fwd_sem, group, False)
            fwd[clan_tiles] = stage_fld[...]

    with jax.named_scope("spread"):

        @pl.when(group == top)
        def _():
            to_mates(packed_src, stage_src, 4, stage_sem.at[1])
            start_rows()
            all_here()
            with jax.named_scope("relay_s"):
                wait_for(stage_src, MATES - 1, stage_sem.at[1])
                to_clans(stage_src, adj, 5, adj_sem.at[line], top, False)
                adj[clan_tiles] = stage_src[...]
            relay_rows()
            pl.semaphore_wait(clear_sem, 1)
            pl.semaphore_signal(go_sem, inc=1, device_id=(top - 1, me), device_id_type=MESH)

        @pl.when(group == top - 1)
        def _():
            all_here()
            build_fwd()
            build_adj()
            with jax.named_scope("wait_go"):
                pl.semaphore_wait(go_sem, 1)
            start_fields()
            start_rows()
            relay_fields()
            relay_rows()

        @pl.when(group < top - 1)
        def _():
            all_here()
            build_fwd()
            build_adj()
            start_fields()
            start_rows()
            relay_fields()
            relay_rows()

    def unpack(tiles):
        count = tiles.shape[0]
        value = tiles.astype(F32)
        turned = pltpu.roll(value.reshape(count * half, cols), cols // 2, 1).reshape(value.shape)
        lower = jnp.where(lane < cols // 2, value, turned)
        upper = jnp.where(lane < cols // 2, turned, value)
        return jnp.concatenate([lower, upper], axis=1).reshape(count * rows, cols).astype(BF16)

    def sort_share(far, first, last):
        z = lax.rem(line + far, lines)
        tiles = jnp.concatenate(
            [adj[pl.ds((p * lines + z) * MATES, MATES)].reshape(MATES * half, cols) for p in range(planes)],
            axis=0,
        )
        turned = tiles.astype(F32).T.astype(BF16)
        left = jnp.concatenate([turned[: cols // 2], turned[cols // 2 :]], axis=1)
        at = pl.ds(pl.multiple_of(z * share, share), share)
        span = 3 * depth if wide % (3 * depth) == 0 else wide
        tail = None
        for k in reversed(range(wide // span)):
            here = pl.ds(k * span, span)
            total = jnp.dot(left, hot_adj[at, here], preferred_element_type=F32)
            if not first:
                total += sorting[:, here]
            if not last:
                sorting[:, here] = total
                continue
            lined[:, pl.ds(border + k * span, span)] = total.astype(BF16)
            pieces = [
                pltpu.roll(total[:, i * cols : (i + 1) * cols], cols // 2, 1) for i in range(span // cols)
            ]
            pieces.append(jnp.zeros_like(pieces[0]) if tail is None else tail)
            tail = pieces[0]
            for i in range(span // cols):
                shifted[:, pl.ds(border + k * span + i * cols, cols)] = jnp.where(
                    lane < cols // 2, pieces[i], pieces[i + 1]
                ).astype(BF16)
        if last:
            shifted[:, pl.ds(border - cols, cols)] = jnp.where(lane < cols // 2, 0.0, tail).astype(BF16)

    near_first = by_distance(lines)[::-1]

    def receive(sort):
        total = jnp.zeros((MATES * 2 * rows, cols), F32)
        for step, far in enumerate(near_first):
            z = lax.rem(line + far, lines)
            with jax.named_scope("wait_a%d" % step):
                if step == 0:

                    @pl.when(group == top)
                    def _():
                        wait_for(adj, MATES * (planes - 1), adj_sem.at[z])

                    @pl.when(group < top)
                    def _():
                        wait_for(adj, MATES * planes, adj_sem.at[z])
                else:
                    wait_for(adj, MATES * planes, adj_sem.at[z])
            with jax.named_scope("propagate"):
                blocks = [adj[pl.ds((p * lines + z) * MATES, MATES)] for p in range(planes)]
                right_side = unpack(jnp.concatenate(blocks, axis=0))
                matrix = jnp.concatenate(
                    [
                        rows_all[
                            :, :, :, pl.ds(pl.multiple_of((p * lines + z) * clan_rows, clan_rows), clan_rows)
                        ].reshape(MATES * 2 * rows, clan_rows)
                        for p in range(planes)
                    ],
                    axis=1,
                )
                total += jnp.dot(matrix, right_side, preferred_element_type=F32)
            last = step == lines - 1
            if last:
                with jax.named_scope("forward"):
                    total = total.reshape(MATES, 2, rows, cols)
                    cross = pltpu.roll(total[:, 1].reshape(MATES * rows, cols), slice_b, 1)
                    cross = cross.reshape(MATES, rows, cols)
                    result = total[:, 0] + jnp.where(in_slice < slice_b, -cross, cross)
                    outgoing[...] = jnp.where(
                        lane < cols // 2, result[:, :half], result[:, half:]
                    ).astype(BF16)
                    if not sort:
                        below = jnp.maximum(group - 1, 0)

                        @pl.when(group < top)
                        def _():
                            pl.semaphore_wait(clear_sem, 1)

                        to_clans(outgoing, adj, 6, adj_sem.at[line], below, True)
                    to_mates(outgoing, landed, 7, land_sem)
            if sort:
                with jax.named_scope("sort0"):
                    sort_share(far, step == 0, last)

    @pl.when(group >= top - 1)
    def _():
        wait_rows()
        receive(False)

    @pl.when(group == top)
    def _():
        start_fields()
        build_fwd()
        relay_fields()
        build_adj()

    with jax.named_scope("wait_f"):
        wait_for(fwd, peers - MATES, fwd_sem)
    with jax.named_scope("sortf"):
        for k in range(steps):
            count = depth // rows
            flat_fwd = unpack(fwd[pl.ds(k * count, count)])
            stretched[pl.ds(k * depth, depth), :] = flat_fwd
        sign = jnp.where(in_slice < slice_b, 1.0, -1.0)
        quads = chunk // band

        @pl.loop(0, harm // chunk)
        def _(r):
            at = pl.ds(pl.multiple_of(r * chunk, chunk), chunk)
            total = jnp.zeros((chunk, cols), F32)
            for k in range(steps):
                total += jnp.dot(
                    hot_fwd[at, pl.ds(k * depth, depth)], stretched[pl.ds(k * depth, depth), :],
                    preferred_element_type=F32,
                )
            real = total * sign
            imag = pltpu.roll(total, slice_b, 1)
            for pair in range(quads // 2):
                lo, mid, hi = 2 * pair * band, (2 * pair + 1) * band, (2 * pair + 2) * band
                upper = jnp.where(lane < cols // 2, real[lo:mid], real[mid:hi])
                lower = jnp.where(lane < cols // 2, imag[lo:mid], imag[mid:hi])
                both = jnp.concatenate([upper, lower], axis=0)
                factor[r, :, pl.ds(pair * cols, cols)] = both.astype(BF16)

    @pl.when(group == 1)
    def _():
        wait_rows()
        receive(False)

    @pl.when(group == 0)
    def _():
        wait_rows()
        receive(True)

    @pl.when(group > 0)
    def _():
        with jax.named_scope("sorta"):
            for step, far in enumerate(near_first):
                sort_share(far, step == 0, step == lines - 1)

    with jax.named_scope("gram"):
        quad = chunk // band
        view = (MATES + 2) * band
        gram = jnp.zeros((2 * band, view), F32)
        for n in range(harm // chunk):
            start = (MATES * clan + quad * n) * band
            window = []
            for k in range(quad):
                buffer = shifted if k % 2 else lined
                at = pl.ds(pl.multiple_of(start + (k - k % 2) * band, 2 * band), view)
                window.append(buffer[:, at])
            gram += jnp.dot(factor[n], jnp.concatenate(window, axis=0), preferred_element_type=F32)
        for m in range(MATES):
            if m % 2:
                both = gram[:, (m - 1) * band : (m + 3) * band]
                turned = pltpu.roll(both, 2 * band + 1, 1, stride=1, stride_axis=0)[:, : 2 * band]
            else:
                both = gram[:, m * band : (m + 2) * band]
                turned = pltpu.roll(both, band + 1, 1, stride=1, stride_axis=0)
            real = jnp.sum(turned[:band], axis=0, keepdims=True)
            imag = jnp.sum(turned[band:], axis=0, keepdims=True)
            partial[m] = jnp.where(lane < band, real, imag)

    with jax.named_scope("reduce"):
        to_mates(partial, gathered, 8, part_sem)

    with jax.named_scope("land"):
        wait_for(landed, MATES - 1, land_sem)
        pieces = [landed[m].astype(F32) for m in range(MATES)]
        for plane in range(2):
            for upper in range(2):
                where = 2 * upper + plane
                tile = None
                for m in range(MATES):
                    shift = (m - where) * slice_b % cols
                    moved = pltpu.roll(pieces[m], shift, 1) if shift else pieces[m]
                    tile = moved if m == 0 else jnp.where(lane < m * slice_b, tile, moved)
                bound_ref[0, plane, pl.ds(upper * half, half), :] = tile.astype(BF16)

    with jax.named_scope("sum"):
        wait_for(gathered, MATES - 1, part_sem)
        total = gathered[0]
        for m in range(1, MATES):
            total = total + gathered[m]
        total = total * scale
        grads_ref[0, 0:1, :] = total[:, :band]
        grads_ref[0, 1:2, :] = total[:, band:]

    with jax.named_scope("drain"):
        wait_for(rows_all, 2, send_sem.at[0])
        wait_for(rows_all, 1, send_sem.at[1])
        wait_for(stage_fld, MATES - 1, send_sem.at[2])
        wait_for(fwd, peers - MATES, send_sem.at[3])
        wait_for(landed, MATES - 1, send_sem.at[7])
        wait_for(gathered, MATES - 1, send_sem.at[8])

        @pl.when(group == top)
        def _():
            wait_for(stage_src, MATES - 1, send_sem.at[4])
            wait_for(adj, peers - MATES, send_sem.at[5])

        @pl.when(group > 0)
        def _():
            wait_for(adj, peers, send_sem.at[6])


def solution(mesh):
    layers, peers = mesh.shape["layer"], mesh.shape["harm"]

    def per_device(source, transfer, fields, orders):
        rows, cols = source.shape[1], source.shape[2]
        harm = rows * peers
        band = 2 * rows
        chunk = min(256, harm)
        vmem = pl.BlockSpec(memory_space=pltpu.VMEM)
        hbm = pl.BlockSpec(memory_space=pltpu.HBM)
        tile = (rows // 2, cols)
        return pl.pallas_call(
            functools.partial(kernel, layers, peers, 1.0 / math.sqrt(harm * cols)),
            out_shape=(
                jax.ShapeDtypeStruct((1, 2, band), F32),
                jax.ShapeDtypeStruct((1, 2, rows, cols), BF16),
            ),
            in_specs=[hbm] * 4,
            out_specs=(vmem, vmem),
            scratch_shapes=[
                pltpu.VMEM((2, rows, cols), BF16),
                pltpu.VMEM((2, rows, cols), BF16),
                pltpu.VMEM((1, harm), jnp.int32),
                pltpu.VMEM((MATES, 2, rows, harm), BF16),
                pltpu.VMEM((peers, *tile), BF16),
                pltpu.VMEM((peers, *tile), BF16),
                pltpu.VMEM((harm, cols), BF16),
                pltpu.VMEM((harm, cols), F32),
                pltpu.VMEM((harm, harm), BF16),
                pltpu.VMEM((harm, harm + 2 * cols), BF16),
                pltpu.VMEM((2 * cols // MATES, 3 * harm), BF16),
                pltpu.VMEM((2 * cols // MATES, 3 * harm), BF16),
                pltpu.VMEM((harm // chunk, 2 * band, chunk // band * 2 * (cols // MATES)), BF16),
                *[pltpu.VMEM((MATES, *tile), BF16)] * 6,
                pltpu.VMEM((MATES, 1, cols), F32),
                pltpu.VMEM((MATES, 1, cols), F32),
                pltpu.VMEM((2 * cols // MATES, harm + 2 * cols), F32),
                pltpu.SemaphoreType.DMA((4,)),
                pltpu.SemaphoreType.DMA((9,)),
                pltpu.SemaphoreType.DMA((6,)),
                pltpu.SemaphoreType.DMA((LINES,)),
                pltpu.SemaphoreType.DMA,
                pltpu.SemaphoreType.DMA((2,)),
                pltpu.SemaphoreType.DMA,
                pltpu.SemaphoreType.DMA,
                *[pltpu.SemaphoreType.REGULAR] * 4,
            ],
            compiler_params=pltpu.CompilerParams(
                collective_id=0, has_side_effects=True, vmem_limit_bytes=44 * 1024 * 1024
            ),
        )(
            *(
                pltpu.with_memory_space_constraint(value, pltpu.HBM)
                for value in (source, transfer, fields, orders.reshape(1, harm))
            )
        )

    return jax.shard_map(
        per_device,
        mesh=mesh,
        in_specs=(
            P(None, "harm", None),
            P("layer", None, "harm", None),
            P("layer", None, "harm", None),
            P(),
        ),
        out_specs=(P("layer", None, "harm"), P("layer", None, "harm", None)),
        check_vma=False,
    )
```

```python
import functools
import math

import jax
import jax.numpy as jnp
from jax import lax
from jax.experimental import pallas as pl
from jax.experimental.pallas import tpu as pltpu
from jax.sharding import PartitionSpec as P

MESH = pl.DeviceIdType.MESH
F32 = jnp.float32
BF16 = jnp.bfloat16
MATES = 4
LINES = 4


def kernel(
    layers, peers, scale,
    source_hbm, transfer_hbm, fields_hbm, orders_hbm, grads_ref, bound_ref,
    source, fields, orders, rows_all, adj, fwd, stretched, column, hot_fwd, hot_adj, lined, shifted, factor,
    packed_src, packed_fld, stage_src, stage_fld, outgoing, landed, partial, gathered, sorting,
    load_sem, send_sem, rows_sem, adj_sem, fwd_sem, stage_sem, land_sem, part_sem, clear_sem, go_sem,
    line_sem, plane_sem,
):
    group = lax.axis_index("layer")
    me = lax.axis_index("harm")
    mate = me % MATES
    clan = me // MATES
    clans = peers // MATES
    lines = min(LINES, clans)
    planes = clans // lines
    line = clan % lines
    plane_at = clan // lines
    rows = source.shape[1]
    half = rows // 2
    cols = source.shape[2]
    slice_b = cols // MATES
    harm = rows * peers
    band = 2 * rows
    depth = min(256, harm)
    steps = harm // depth
    top = layers - 1
    helper = top - 2
    far_line = lines // 2
    clan_rows = MATES * rows
    share = planes * clan_rows

    loads = [
        pltpu.make_async_copy(transfer_hbm.at[0], rows_all.at[mate], load_sem.at[3]),
        pltpu.make_async_copy(source_hbm, source, load_sem.at[0]),
        pltpu.make_async_copy(fields_hbm.at[0], fields, load_sem.at[2]),
        pltpu.make_async_copy(orders_hbm, orders, load_sem.at[1]),
    ]
    for load in loads:
        load.start()

    barrier = pltpu.get_barrier_semaphore()

    def mate_index(j):
        return clan * MATES + lax.rem(mate + j, MATES)

    def place(plane, line_of):
        return (plane * lines + line_of) * MATES + mate

    def clan_index(far_line, far_plane):
        return place(lax.rem(plane_at + far_plane, planes), lax.rem(line + far_line, lines))

    def by_distance(size):
        return sorted(range(size), key=lambda d: -min(d, size - d))

    offsets = [(a, b) for a in by_distance(lines) for b in by_distance(planes)]

    near_lines = [place(plane_at, lax.rem(line + far, lines)) for far in (1, lines - 1)]
    near_planes = [place(lax.rem(plane_at + far, planes), line) for far in (2, 1, 3)]

    with jax.named_scope("signal"):
        for index in near_lines + near_planes + [mate_index(j) for j in (2, 1, 3)]:
            pl.semaphore_signal(barrier, inc=1, device_id=(group, index), device_id_type=MESH)

        @pl.when(group > 0)
        def _():
            pl.semaphore_signal(
                barrier, inc=1, device_id=(jnp.maximum(group - 1, 0), me), device_id_type=MESH
            )

        @pl.when(group == top)
        def _():
            pl.semaphore_signal(
                barrier, inc=1, device_id=(helper, clan_index(far_line, 0)), device_id_type=MESH
            )

    lane = lax.broadcasted_iota(jnp.int32, (1, cols), 1)
    in_slice = lax.rem(lane, 2 * slice_b)

    def pack(block, into):
        value = block[...].astype(F32)
        for m in range(MATES):
            parts = []
            for where in range(4):
                plane, upper = where % 2, where // 2
                piece = value[plane, upper * half : (upper + 1) * half, :]
                shift = (where - m) * slice_b % cols
                parts.append(pltpu.roll(piece, shift, 1) if shift else piece)
            tile = parts[3]
            for where in range(2, -1, -1):
                tile = jnp.where(lane < (where + 1) * slice_b, parts[where], tile)
            into[m] = tile.astype(BF16)

    border = harm - cols
    wide = harm + 2 * cols
    chunk = min(256, harm)

    with jax.named_scope("pack"):
        loads[1].wait()
        pack(source, packed_src)
        loads[2].wait()
        pack(fields, packed_fld)
        for buffer in (lined, shifted):
            buffer[:, pl.ds(0, border)] = jnp.zeros((2 * slice_b, border), BF16)
            buffer[:, pl.ds(border + wide, border)] = jnp.zeros((2 * slice_b, border), BF16)
        loads[3].wait()
        loads[0].wait()

    def build_fwd():
        with jax.named_scope("hotf"):

            @pl.loop(0, harm // chunk)
            def _(r):
                index = lax.broadcasted_iota(jnp.int32, (chunk, depth), 0)
                order = r * chunk + (index // band) * band + (band - 1) - index % band
                for k in range(steps):
                    hit = orders[:, pl.ds(k * depth, depth)] == order
                    hot_fwd[
                        pl.ds(pl.multiple_of(r * chunk, chunk), chunk), pl.ds(k * depth, depth)
                    ] = jnp.where(hit, 1.0, 0.0).astype(BF16)

    def build_adj():
        with jax.named_scope("hota"):
            for k in range(harm // cols):
                row = orders[:, pl.ds(k * cols, cols)].astype(F32)
                column[pl.ds(k * cols, cols), :] = jnp.broadcast_to(row, (cols, cols)).T

            @pl.loop(0, peers)
            def _(tile):
                owner = tile // MATES
                spot = (owner // lines) * MATES + tile % MATES
                for upper in range(2):
                    order = column[pl.ds(pl.multiple_of(tile * rows + upper * half, half), half), :]
                    row = (owner % lines) * share + upper * (share // 2) + spot * half
                    row = pl.ds(pl.multiple_of(row, half), half)
                    for k in range(wide // cols):
                        want = (lane + (k * cols - cols + 1)).astype(F32)
                        hot_adj[row, pl.ds(k * cols, cols)] = jnp.where(order == want, 1.0, 0.0).astype(BF16)

    with jax.named_scope("barrier"):

        close = len(near_lines) + len(near_planes) + MATES - 1

        @pl.when((group < top) & (group != helper))
        def _():
            pl.semaphore_wait(barrier, close + 1)

        @pl.when(group == helper)
        def _():
            pl.semaphore_wait(barrier, close + 2)

        @pl.when(group == top)
        def _():
            pl.semaphore_wait(barrier, close)

        for index in near_planes:
            pl.semaphore_signal(plane_sem, inc=1, device_id=(group, index), device_id_type=MESH)

    def near_here():
        with jax.named_scope("near"):
            pl.semaphore_wait(plane_sem, len(near_planes))
            for index in near_lines:
                pl.semaphore_signal(line_sem, inc=1, device_id=(group, index), device_id_type=MESH)

    def all_here():
        with jax.named_scope("here"):
            pl.semaphore_wait(line_sem, len(near_lines))

            @pl.when(group < top)
            def _():
                pl.semaphore_signal(
                    clear_sem, inc=1, device_id=(jnp.minimum(group + 1, top), me), device_id_type=MESH
                )

    def remote(src, dst, sem, arrived, target, index):
        return pltpu.make_async_remote_copy(
            src_ref=src, dst_ref=dst, send_sem=send_sem.at[sem], recv_sem=arrived,
            device_id=(target, index), device_id_type=MESH,
        )

    def wait_for(buffer, count, sem):
        part_of = buffer.at[pl.ds(0, count)]
        pltpu.make_async_copy(part_of, part_of, sem).wait()

    def to_mates(tiles, dst, sem, arrived):
        for j in (2, 1, 3):
            other = lax.rem(mate + j, MATES)
            remote(
                tiles.at[other], dst.at[mate], sem, arrived, group, clan * MATES + other
            ).start()
        dst[mate] = tiles[mate]

    clan_tiles = pl.ds(clan * MATES, MATES)

    def to_clans(tiles, dst, sem, arrived, target, to):
        for a, b in to:
            remote(tiles, dst.at[clan_tiles], sem, arrived, target, clan_index(a, b)).start()

    right, left = mate_index(1), mate_index(MATES - 1)
    from_left, from_right = lax.rem(mate + MATES - 1, MATES), lax.rem(mate + 1, MATES)

    def start_rows():
        for first in (0, 1):
            to_right = rows_all.at[mate, first]
            to_left = rows_all.at[mate, 1 - first]
            remote(to_right, to_right, 0, rows_sem.at[2 * first], group, right).start()
            remote(to_left, to_left, 0, rows_sem.at[2 * first + 1], group, left).start()

    def wait_half(sem):
        wait_for(rows_all.at[0], 1, rows_sem.at[sem])

    def relay_rows():
        with jax.named_scope("relay_t"):
            wait_half(0)
            block = rows_all.at[from_left, 0]
            remote(block, block, 1, rows_sem.at[4], group, right).start()
            wait_half(1)
            block = rows_all.at[from_right, 1]
            remote(block, block, 1, rows_sem.at[5], group, left).start()

    def wait_rows():
        with jax.named_scope("wait_t"):
            for k in (2, 3, 4, 5):
                wait_half(k)

    def start_fields():
        to_mates(packed_fld, stage_fld, 2, stage_sem.at[0])

    def relay_fields():
        with jax.named_scope("relay_f"):
            wait_for(stage_fld, MATES - 1, stage_sem.at[0])
            to_clans(stage_fld, fwd, 3, fwd_sem, group, offsets[:-1])
            fwd[clan_tiles] = stage_fld[...]

    with jax.named_scope("spread"):

        near = [offset for offset in offsets[:-1] if offset[0] != far_line]
        far = [offset for offset in offsets if offset[0] == far_line]

        def relay_source(to):
            with jax.named_scope("relay_s"):
                wait_for(stage_src, MATES - 1, stage_sem.at[1])
                to_clans(stage_src, adj, 5, adj_sem.at[line], top, to)

        @pl.when(group == top)
        def _():
            to_mates(packed_src, stage_src, 4, stage_sem.at[1])
            start_rows()
            near_here()
            relay_source(near)
            adj[clan_tiles] = stage_src[...]
            relay_rows()
            all_here()
            pl.semaphore_wait(clear_sem, 1)
            pl.semaphore_signal(go_sem, inc=1, device_id=(top - 1, me), device_id_type=MESH)

        @pl.when(group == top - 1)
        def _():
            near_here()
            all_here()
            with jax.named_scope("wait_go"):
                pl.semaphore_wait(go_sem, 1)
            start_fields()
            start_rows()
            build_fwd()
            relay_rows()
            build_adj()

        @pl.when(group < top - 1)
        def _():
            @pl.when(group == helper)
            def _():
                to_mates(packed_src, stage_src, 4, stage_sem.at[1])

            near_here()

            @pl.when(group == helper)
            def _():
                relay_source(far)

            all_here()
            start_fields()
            start_rows()
            build_fwd()
            relay_fields()
            relay_rows()
            build_adj()

    def unpack(tiles):
        count = tiles.shape[0]
        value = tiles.astype(F32)
        turned = pltpu.roll(value.reshape(count * half, cols), cols // 2, 1).reshape(value.shape)
        lower = jnp.where(lane < cols // 2, value, turned)
        upper = jnp.where(lane < cols // 2, turned, value)
        return jnp.concatenate([lower, upper], axis=1).reshape(count * rows, cols).astype(BF16)

    def sort_share(far, first, last):
        z = lax.rem(line + far, lines)
        tiles = jnp.concatenate(
            [adj[pl.ds((p * lines + z) * MATES, MATES)].reshape(MATES * half, cols) for p in range(planes)],
            axis=0,
        )
        turned = tiles.astype(F32).T.astype(BF16)
        left = jnp.concatenate([turned[: cols // 2], turned[cols // 2 :]], axis=1)
        at = pl.ds(pl.multiple_of(z * share, share), share)
        span = 3 * depth if wide % (3 * depth) == 0 else wide
        tail = None
        for k in reversed(range(wide // span)):
            here = pl.ds(k * span, span)
            total = jnp.dot(left, hot_adj[at, here], preferred_element_type=F32)
            if not first:
                total += sorting[:, here]
            if not last:
                sorting[:, here] = total
                continue
            lined[:, pl.ds(border + k * span, span)] = total.astype(BF16)
            pieces = [
                pltpu.roll(total[:, i * cols : (i + 1) * cols], cols // 2, 1) for i in range(span // cols)
            ]
            pieces.append(jnp.zeros_like(pieces[0]) if tail is None else tail)
            tail = pieces[0]
            for i in range(span // cols):
                shifted[:, pl.ds(border + k * span + i * cols, cols)] = jnp.where(
                    lane < cols // 2, pieces[i], pieces[i + 1]
                ).astype(BF16)
        if last:
            shifted[:, pl.ds(border - cols, cols)] = jnp.where(lane < cols // 2, 0.0, tail).astype(BF16)

    near_first = by_distance(lines)[::-1]

    def receive(sort):
        total = jnp.zeros((MATES * 2 * rows, cols), F32)
        for step, far in enumerate(near_first):
            z = lax.rem(line + far, lines)
            with jax.named_scope("wait_a%d" % step):
                if step == 0:

                    @pl.when(group == top)
                    def _():
                        wait_for(adj, MATES * (planes - 1), adj_sem.at[z])

                    @pl.when(group < top)
                    def _():
                        wait_for(adj, MATES * planes, adj_sem.at[z])
                else:
                    wait_for(adj, MATES * planes, adj_sem.at[z])
            with jax.named_scope("propagate"):
                blocks = [adj[pl.ds((p * lines + z) * MATES, MATES)] for p in range(planes)]
                right_side = unpack(jnp.concatenate(blocks, axis=0))
                matrix = jnp.concatenate(
                    [
                        rows_all[
                            :, :, :, pl.ds(pl.multiple_of((p * lines + z) * clan_rows, clan_rows), clan_rows)
                        ].reshape(MATES * 2 * rows, clan_rows)
                        for p in range(planes)
                    ],
                    axis=1,
                )
                total += jnp.dot(matrix, right_side, preferred_element_type=F32)
            last = step == lines - 1
            if last:
                with jax.named_scope("forward"):
                    total = total.reshape(MATES, 2, rows, cols)
                    cross = pltpu.roll(total[:, 1].reshape(MATES * rows, cols), slice_b, 1)
                    cross = cross.reshape(MATES, rows, cols)
                    result = total[:, 0] + jnp.where(in_slice < slice_b, -cross, cross)
                    outgoing[...] = jnp.where(
                        lane < cols // 2, result[:, :half], result[:, half:]
                    ).astype(BF16)
                    if not sort:
                        below = jnp.maximum(group - 1, 0)

                        @pl.when(group < top)
                        def _():
                            pl.semaphore_wait(clear_sem, 1)

                        to_clans(outgoing, adj, 6, adj_sem.at[line], below, offsets)
                    to_mates(outgoing, landed, 7, land_sem)
            if sort:
                with jax.named_scope("sort0"):
                    sort_share(far, step == 0, last)

    @pl.when(group > 0)
    def _():
        wait_rows()
        receive(False)

    @pl.when(group == top)
    def _():
        start_fields()
        build_fwd()
        build_adj()

    @pl.when(group >= top - 1)
    def _():
        relay_fields()

    with jax.named_scope("wait_f"):
        wait_for(fwd, peers - MATES, fwd_sem)
    with jax.named_scope("sortf"):
        for k in range(steps):
            count = depth // rows
            flat_fwd = unpack(fwd[pl.ds(k * count, count)])
            stretched[pl.ds(k * depth, depth), :] = flat_fwd
        sign = jnp.where(in_slice < slice_b, 1.0, -1.0)
        quads = chunk // band

        @pl.loop(0, harm // chunk)
        def _(r):
            at = pl.ds(pl.multiple_of(r * chunk, chunk), chunk)
            total = jnp.zeros((chunk, cols), F32)
            for k in range(steps):
                total += jnp.dot(
                    hot_fwd[at, pl.ds(k * depth, depth)], stretched[pl.ds(k * depth, depth), :],
                    preferred_element_type=F32,
                )
            real = total * sign
            imag = pltpu.roll(total, slice_b, 1)
            for pair in range(quads // 2):
                lo, mid, hi = 2 * pair * band, (2 * pair + 1) * band, (2 * pair + 2) * band
                upper = jnp.where(lane < cols // 2, real[lo:mid], real[mid:hi])
                lower = jnp.where(lane < cols // 2, imag[lo:mid], imag[mid:hi])
                both = jnp.concatenate([upper, lower], axis=0)
                factor[r, :, pl.ds(pair * cols, cols)] = both.astype(BF16)

    @pl.when(group == 0)
    def _():
        wait_rows()
        receive(True)

    @pl.when(group > 0)
    def _():
        with jax.named_scope("sorta"):
            for step, far in enumerate(near_first):
                sort_share(far, step == 0, step == lines - 1)

    with jax.named_scope("gram"):
        quad = chunk // band
        view = (MATES + 2) * band
        gram = jnp.zeros((2 * band, view), F32)
        for n in range(harm // chunk):
            start = (MATES * clan + quad * n) * band
            window = []
            for k in range(quad):
                buffer = shifted if k % 2 else lined
                at = pl.ds(pl.multiple_of(start + (k - k % 2) * band, 2 * band), view)
                window.append(buffer[:, at])
            gram += jnp.dot(factor[n], jnp.concatenate(window, axis=0), preferred_element_type=F32)
        for m in range(MATES):
            if m % 2:
                both = gram[:, (m - 1) * band : (m + 3) * band]
                turned = pltpu.roll(both, 2 * band + 1, 1, stride=1, stride_axis=0)[:, : 2 * band]
            else:
                both = gram[:, m * band : (m + 2) * band]
                turned = pltpu.roll(both, band + 1, 1, stride=1, stride_axis=0)
            real = jnp.sum(turned[:band], axis=0, keepdims=True)
            imag = jnp.sum(turned[band:], axis=0, keepdims=True)
            partial[m] = jnp.where(lane < band, real, imag)

    with jax.named_scope("reduce"):
        to_mates(partial, gathered, 8, part_sem)

    with jax.named_scope("land"):
        wait_for(landed, MATES - 1, land_sem)
        pieces = [landed[m].astype(F32) for m in range(MATES)]
        for plane in range(2):
            for upper in range(2):
                where = 2 * upper + plane
                tile = None
                for m in range(MATES):
                    shift = (m - where) * slice_b % cols
                    moved = pltpu.roll(pieces[m], shift, 1) if shift else pieces[m]
                    tile = moved if m == 0 else jnp.where(lane < m * slice_b, tile, moved)
                bound_ref[0, plane, pl.ds(upper * half, half), :] = tile.astype(BF16)

    with jax.named_scope("sum"):
        wait_for(gathered, MATES - 1, part_sem)
        total = gathered[0]
        for m in range(1, MATES):
            total = total + gathered[m]
        total = total * scale
        grads_ref[0, 0:1, :] = total[:, :band]
        grads_ref[0, 1:2, :] = total[:, band:]

    with jax.named_scope("drain"):
        wait_for(rows_all, 2, send_sem.at[0])
        wait_for(rows_all, 1, send_sem.at[1])
        wait_for(stage_fld, MATES - 1, send_sem.at[2])
        wait_for(fwd, peers - MATES, send_sem.at[3])
        wait_for(landed, MATES - 1, send_sem.at[7])
        wait_for(gathered, MATES - 1, send_sem.at[8])

        @pl.when(group == helper)
        def _():
            wait_for(adj, MATES * len(far), send_sem.at[5])

        @pl.when((group == top) | (group == helper))
        def _():
            wait_for(stage_src, MATES - 1, send_sem.at[4])

        @pl.when(group == top)
        def _():
            wait_for(adj, MATES * len(near), send_sem.at[5])

        @pl.when(group > 0)
        def _():
            wait_for(adj, peers, send_sem.at[6])


def solution(mesh):
    layers, peers = mesh.shape["layer"], mesh.shape["harm"]

    def per_device(source, transfer, fields, orders):
        rows, cols = source.shape[1], source.shape[2]
        harm = rows * peers
        band = 2 * rows
        chunk = min(256, harm)
        vmem = pl.BlockSpec(memory_space=pltpu.VMEM)
        hbm = pl.BlockSpec(memory_space=pltpu.HBM)
        tile = (rows // 2, cols)
        return pl.pallas_call(
            functools.partial(kernel, layers, peers, 1.0 / math.sqrt(harm * cols)),
            out_shape=(
                jax.ShapeDtypeStruct((1, 2, band), F32),
                jax.ShapeDtypeStruct((1, 2, rows, cols), BF16),
            ),
            in_specs=[hbm] * 4,
            out_specs=(vmem, vmem),
            scratch_shapes=[
                pltpu.VMEM((2, rows, cols), BF16),
                pltpu.VMEM((2, rows, cols), BF16),
                pltpu.VMEM((1, harm), jnp.int32),
                pltpu.VMEM((MATES, 2, rows, harm), BF16),
                pltpu.VMEM((peers, *tile), BF16),
                pltpu.VMEM((peers, *tile), BF16),
                pltpu.VMEM((harm, cols), BF16),
                pltpu.VMEM((harm, cols), F32),
                pltpu.VMEM((harm, harm), BF16),
                pltpu.VMEM((harm, harm + 2 * cols), BF16),
                pltpu.VMEM((2 * cols // MATES, 3 * harm), BF16),
                pltpu.VMEM((2 * cols // MATES, 3 * harm), BF16),
                pltpu.VMEM((harm // chunk, 2 * band, chunk // band * 2 * (cols // MATES)), BF16),
                *[pltpu.VMEM((MATES, *tile), BF16)] * 6,
                pltpu.VMEM((MATES, 1, cols), F32),
                pltpu.VMEM((MATES, 1, cols), F32),
                pltpu.VMEM((2 * cols // MATES, harm + 2 * cols), F32),
                pltpu.SemaphoreType.DMA((4,)),
                pltpu.SemaphoreType.DMA((9,)),
                pltpu.SemaphoreType.DMA((6,)),
                pltpu.SemaphoreType.DMA((LINES,)),
                pltpu.SemaphoreType.DMA,
                pltpu.SemaphoreType.DMA((2,)),
                pltpu.SemaphoreType.DMA,
                pltpu.SemaphoreType.DMA,
                *[pltpu.SemaphoreType.REGULAR] * 4,
            ],
            compiler_params=pltpu.CompilerParams(
                collective_id=0, has_side_effects=True, vmem_limit_bytes=44 * 1024 * 1024
            ),
        )(
            *(
                pltpu.with_memory_space_constraint(value, pltpu.HBM)
                for value in (source, transfer, fields, orders.reshape(1, harm))
            )
        )

    return jax.shard_map(
        per_device,
        mesh=mesh,
        in_specs=(
            P(None, "harm", None),
            P("layer", None, "harm", None),
            P("layer", None, "harm", None),
            P(),
        ),
        out_specs=(P("layer", None, "harm"), P("layer", None, "harm", None)),
        check_vma=False,
    )
```

```python
import functools
import math

import jax
import jax.numpy as jnp
from jax import lax
from jax.experimental import pallas as pl
from jax.experimental.pallas import tpu as pltpu
from jax.sharding import PartitionSpec as P

MESH = pl.DeviceIdType.MESH
F32 = jnp.float32
BF16 = jnp.bfloat16
MATES = 4
LINES = 4


def kernel(
    layers, peers, scale,
    source_hbm, transfer_hbm, fields_hbm, orders_hbm, grads_ref, bound_ref,
    source, fields, orders, rows_own, rows_all, rows_two, adj, adj_two, fwd, stretched, column, hot_fwd, hot_adj, lined, shifted, factor, factor_two,
    packed_src, packed_fld, stage_src, stage_fld, outgoing, outgoing_two, landed, partial, partial_two, gathered, sorting,
    load_sem, send_sem, rows_sem, adj_sem, two_sem, hand_sem, fwd_sem, stage_sem, land_sem, part_sem, clear_sem, line_sem, plane_sem, go_sem,
):
    group = lax.axis_index("layer")
    me = lax.axis_index("harm")
    mate = me % MATES
    clan = me // MATES
    clans = peers // MATES
    lines = min(LINES, clans)
    planes = clans // lines
    line = clan % lines
    plane_at = clan // lines
    rows = source.shape[1]
    half = rows // 2
    cols = source.shape[2]
    slice_b = cols // MATES
    harm = rows * peers
    band = 2 * rows
    depth = min(256, harm)
    steps = harm // depth
    top = layers - 1
    helper = top - 2
    chain = (group == top) | (group == helper)
    sibling = jnp.where(chain, jnp.maximum(group - 1, 0), jnp.minimum(group + 1, top))
    far_line = lines // 2
    clan_rows = MATES * rows
    share = planes * clan_rows

    loads = [
        pltpu.make_async_copy(transfer_hbm.at[0], rows_own, load_sem.at[3]),
        pltpu.make_async_copy(source_hbm, source, load_sem.at[0]),
        pltpu.make_async_copy(fields_hbm.at[0], fields, load_sem.at[2]),
        pltpu.make_async_copy(orders_hbm, orders, load_sem.at[1]),
    ]
    for load in loads:
        load.start()

    barrier = pltpu.get_barrier_semaphore()

    def mate_index(j):
        return clan * MATES + lax.rem(mate + j, MATES)

    def place(plane, line_of):
        return (plane * lines + line_of) * MATES + mate

    def clan_index(far_line, far_plane):
        return place(lax.rem(plane_at + far_plane, planes), lax.rem(line + far_line, lines))

    def by_distance(size):
        return sorted(range(size), key=lambda d: -min(d, size - d))

    offsets = [(a, b) for a in by_distance(lines) for b in by_distance(planes)]

    near_lines = [place(plane_at, lax.rem(line + far, lines)) for far in (1, lines - 1)]
    near_planes = [place(lax.rem(plane_at + far, planes), line) for far in (2, 1, 3)]

    with jax.named_scope("signal"):
        for index in near_lines + near_planes + [mate_index(j) for j in (2, 1, 3)]:
            pl.semaphore_signal(barrier, inc=1, device_id=(group, index), device_id_type=MESH)

        @pl.when(chain)
        def _():
            pl.semaphore_signal(barrier, inc=1, device_id=(sibling, me), device_id_type=MESH)

        @pl.when(group == top)
        def _():
            pl.semaphore_signal(barrier, inc=1, device_id=(helper, me), device_id_type=MESH)
            pl.semaphore_signal(
                barrier, inc=1, device_id=(helper, clan_index(far_line, 0)), device_id_type=MESH
            )

    lane = lax.broadcasted_iota(jnp.int32, (1, cols), 1)
    in_slice = lax.rem(lane, 2 * slice_b)

    def pack(block, into):
        value = block[...].astype(F32)
        for m in range(MATES):
            parts = []
            for where in range(4):
                plane, upper = where % 2, where // 2
                piece = value[plane, upper * half : (upper + 1) * half, :]
                shift = (where - m) * slice_b % cols
                parts.append(pltpu.roll(piece, shift, 1) if shift else piece)
            tile = parts[3]
            for where in range(2, -1, -1):
                tile = jnp.where(lane < (where + 1) * slice_b, parts[where], tile)
            into[m] = tile.astype(BF16)

    border = harm - cols
    wide = harm + 2 * cols
    chunk = min(256, harm)

    with jax.named_scope("pack"):
        loads[1].wait()
        pack(source, packed_src)
        loads[2].wait()
        pack(fields, packed_fld)
        for buffer in (lined, shifted):
            buffer[:, pl.ds(0, border)] = jnp.zeros((2 * slice_b, border), BF16)
            buffer[:, pl.ds(border + wide, border)] = jnp.zeros((2 * slice_b, border), BF16)
        loads[3].wait()

    def arrange():
        value = rows_own[...].reshape(2 * rows, harm)
        count = harm // clan_rows
        stacked = jnp.concatenate(
            [value[:, k * clan_rows : (k + 1) * clan_rows] for k in range(count)], axis=0
        )
        at = lax.broadcasted_iota(jnp.int32, (clan_rows, 2 * clan_rows), 0)
        to = lax.broadcasted_iota(jnp.int32, (clan_rows, 2 * clan_rows), 1)
        inside = to % clan_rows
        upper = (inside // (clan_rows // 2) + to // clan_rows) % 2
        origin = inside % (clan_rows // 2) // half * rows + upper * half + inside % half
        order = jnp.where(at == origin, 1.0, 0.0).astype(BF16)
        moved = jnp.dot(stacked, order, preferred_element_type=F32)
        moved = moved.reshape(count, 2, rows, 2 * clan_rows)
        for z in range(lines):
            for pair in range(planes // 2):
                first = moved[2 * pair * lines + z]
                second = moved[(2 * pair + 1) * lines + z]
                lower = jnp.where(lane < cols // 2, first[:, :, :clan_rows], second[:, :, clan_rows:])
                upper = jnp.where(lane < cols // 2, first[:, :, clan_rows:], second[:, :, :clan_rows])
                start = z * share + pair * clan_rows
                rows_all[mate, :, :, pl.ds(start, clan_rows)] = lower.astype(BF16)
                rows_all[mate, :, :, pl.ds(start + share // 2, clan_rows)] = upper.astype(BF16)

    with jax.named_scope("arrange"):
        loads[0].wait()
        arrange()

    def build_fwd():
        with jax.named_scope("hotf"):

            @pl.loop(0, harm // chunk)
            def _(r):
                index = lax.broadcasted_iota(jnp.int32, (chunk, depth), 0)
                order = r * chunk + (index // band) * band + (band - 1) - index % band
                for k in range(steps):
                    hit = orders[:, pl.ds(k * depth, depth)] == order
                    hot_fwd[
                        pl.ds(pl.multiple_of(r * chunk, chunk), chunk), pl.ds(k * depth, depth)
                    ] = jnp.where(hit, 1.0, 0.0).astype(BF16)

    def build_adj():
        with jax.named_scope("hota"):
            for k in range(harm // cols):
                row = orders[:, pl.ds(k * cols, cols)].astype(F32)
                column[pl.ds(k * cols, cols), :] = jnp.broadcast_to(row, (cols, cols)).T

            @pl.loop(0, peers)
            def _(tile):
                owner = tile // MATES
                spot = (owner // lines) * MATES + tile % MATES
                for upper in range(2):
                    order = column[pl.ds(pl.multiple_of(tile * rows + upper * half, half), half), :]
                    row = (owner % lines) * share + upper * (share // 2) + spot * half
                    row = pl.ds(pl.multiple_of(row, half), half)
                    for k in range(wide // cols):
                        want = (lane + (k * cols - cols + 1)).astype(F32)
                        hot_adj[row, pl.ds(k * cols, cols)] = jnp.where(order == want, 1.0, 0.0).astype(BF16)

    with jax.named_scope("barrier"):

        close = len(near_lines) + len(near_planes) + MATES - 1

        @pl.when(jnp.logical_not(chain))
        def _():
            pl.semaphore_wait(barrier, close + 1)

        @pl.when(group == helper)
        def _():
            pl.semaphore_wait(barrier, close + 2)

        @pl.when(group == top)
        def _():
            pl.semaphore_wait(barrier, close)

        for index in near_planes:
            pl.semaphore_signal(plane_sem, inc=1, device_id=(group, index), device_id_type=MESH)

    def near_here():
        with jax.named_scope("near"):
            pl.semaphore_wait(plane_sem, len(near_planes))
            for index in near_lines:
                pl.semaphore_signal(line_sem, inc=1, device_id=(group, index), device_id_type=MESH)

    def all_here():
        with jax.named_scope("here"):
            pl.semaphore_wait(line_sem, len(near_lines))

            @pl.when(jnp.logical_not(chain))
            def _():
                pl.semaphore_signal(clear_sem, inc=1, device_id=(sibling, me), device_id_type=MESH)

            @pl.when(group == helper)
            def _():
                pl.semaphore_signal(clear_sem, inc=1, device_id=(top, me), device_id_type=MESH)

    def remote(src, dst, sem, arrived, target, index):
        return pltpu.make_async_remote_copy(
            src_ref=src, dst_ref=dst, send_sem=send_sem.at[sem], recv_sem=arrived,
            device_id=(target, index), device_id_type=MESH,
        )

    def wait_for(buffer, count, sem):
        part_of = buffer.at[pl.ds(0, count)]
        pltpu.make_async_copy(part_of, part_of, sem).wait()

    def to_mates(tiles, dst, sem, arrived):
        for j in (2, 1, 3):
            other = lax.rem(mate + j, MATES)
            remote(
                tiles.at[other], dst.at[mate], sem, arrived, group, clan * MATES + other
            ).start()
        dst[mate] = tiles[mate]

    clan_tiles = pl.ds(clan * MATES, MATES)

    def to_clans(tiles, dst, sem, arrived, target, to):
        for a, b in to:
            remote(tiles, dst.at[clan_tiles], sem, arrived, target, clan_index(a, b)).start()

    right, left = mate_index(1), mate_index(MATES - 1)
    from_left, from_right = lax.rem(mate + MATES - 1, MATES), lax.rem(mate + 1, MATES)

    def start_rows(buffer, turn):
        for first in (0, 1):
            to_right = buffer.at[mate, first]
            to_left = buffer.at[mate, 1 - first]
            for block, to, sem in ((to_right, right, 2 * first), (to_left, left, 2 * first + 1)):
                remote(block, block, 9 * turn, rows_sem.at[6 * turn + sem], group, to).start()

    def wait_half(turn, sem):
        wait_for(rows_all.at[0], 1, rows_sem.at[6 * turn + sem])

    def relay_rows(buffer, turn):
        with jax.named_scope("relay_t%d" % turn):
            wait_half(turn, 0)
            block = buffer.at[from_left, 0]
            remote(block, block, 9 * turn + 1, rows_sem.at[6 * turn + 4], group, right).start()
            wait_half(turn, 1)
            block = buffer.at[from_right, 1]
            remote(block, block, 9 * turn + 1, rows_sem.at[6 * turn + 5], group, left).start()

    def wait_rows(turn):
        with jax.named_scope("wait_t%d" % turn):
            for k in (2, 3, 4, 5):
                wait_half(turn, k)

    def to_sibling(src, dst, sem, arrived):
        remote(src, dst, sem, arrived, sibling, me).start()

    def to_sibling_mates(tiles, dst, sem, arrived):
        for j in (2, 1, 3, 0):
            other = lax.rem(mate + j, MATES)
            remote(
                tiles.at[other], dst.at[mate], sem, arrived, sibling, clan * MATES + other
            ).start()

    def start_fields():
        to_mates(packed_fld, stage_fld, 2, stage_sem.at[0])

    def relay_fields():
        with jax.named_scope("relay_f"):
            wait_for(stage_fld, MATES - 1, stage_sem.at[0])
            to_clans(stage_fld, fwd, 3, fwd_sem, group, offsets[:-1])
            fwd[clan_tiles] = stage_fld[...]

    with jax.named_scope("spread"):

        near = [offset for offset in offsets[:-1] if offset[0] != far_line]
        far = [offset for offset in offsets if offset[0] == far_line]

        def relay_source(to):
            with jax.named_scope("relay_s"):
                wait_for(stage_src, MATES - 1, stage_sem.at[1])
                to_clans(stage_src, adj, 5, adj_sem.at[line], top, to)

        @pl.when(group == top)
        def _():
            to_mates(packed_src, stage_src, 4, stage_sem.at[1])
            start_rows(rows_all, 0)
            near_here()
            relay_source(near)
            adj[clan_tiles] = stage_src[...]
            relay_rows(rows_all, 0)
            wait_for(rows_all, 1, hand_sem.at[0])
            start_rows(rows_two, 1)
            all_here()
            pl.semaphore_wait(clear_sem, 2)

        @pl.when(group == helper)
        def _():
            to_mates(packed_src, stage_src, 4, stage_sem.at[1])
            near_here()
            relay_source(far)
            all_here()
            start_fields()
            start_rows(rows_all, 0)
            build_fwd()
            relay_fields()
            relay_rows(rows_all, 0)
            wait_for(rows_all, 1, hand_sem.at[0])
            start_rows(rows_two, 1)
            build_adj()
            relay_rows(rows_two, 1)
            pl.semaphore_wait(clear_sem, 1)

        @pl.when(jnp.logical_not(chain))
        def _():
            to_sibling(rows_all.at[mate], rows_two.at[mate], 11, hand_sem.at[0])
            near_here()
            all_here()
            start_fields()
            build_fwd()

            @pl.when(group == top - 1)
            def _():
                build_adj()
                pl.semaphore_wait(go_sem, 1)

            relay_fields()

    def unpack(tiles):
        count = tiles.shape[0]
        value = tiles.astype(F32)
        turned = pltpu.roll(value.reshape(count * half, cols), cols // 2, 1).reshape(value.shape)
        lower = jnp.where(lane < cols // 2, value, turned)
        upper = jnp.where(lane < cols // 2, turned, value)
        return jnp.concatenate([lower, upper], axis=1).reshape(count * rows, cols).astype(BF16)

    def share_tiles(tiles, z):
        return jnp.concatenate(
            [tiles[pl.ds((p * lines + z) * MATES, MATES)].reshape(MATES * half, cols) for p in range(planes)],
            axis=0,
        )

    def sort_share(tiles, far, first, last):
        z = lax.rem(line + far, lines)
        turned = share_tiles(tiles, z).astype(F32).T.astype(BF16)
        left = jnp.concatenate([turned[: cols // 2], turned[cols // 2 :]], axis=1)
        at = pl.ds(pl.multiple_of(z * share, share), share)
        span = 3 * depth if wide % (3 * depth) == 0 else wide
        tail = None
        for k in reversed(range(wide // span)):
            here = pl.ds(k * span, span)
            total = jnp.dot(left, hot_adj[at, here], preferred_element_type=F32)
            if not first:
                total += sorting[:, here]
            if not last:
                sorting[:, here] = total
                continue
            lined[:, pl.ds(border + k * span, span)] = total.astype(BF16)
            pieces = [
                pltpu.roll(total[:, i * cols : (i + 1) * cols], cols // 2, 1) for i in range(span // cols)
            ]
            pieces.append(jnp.zeros_like(pieces[0]) if tail is None else tail)
            tail = pieces[0]
            for i in range(span // cols):
                shifted[:, pl.ds(border + k * span + i * cols, cols)] = jnp.where(
                    lane < cols // 2, pieces[i], pieces[i + 1]
                ).astype(BF16)
        if last:
            shifted[:, pl.ds(border - cols, cols)] = jnp.where(lane < cols // 2, 0.0, tail).astype(BF16)

    near_first = by_distance(lines)[::-1]

    def receive(tiles, block_rows, sems, own_there, out, sort):
        lower = jnp.zeros((MATES * 2 * rows, cols), F32)
        upper = jnp.zeros((MATES * 2 * rows, cols), F32)
        for step, far in enumerate(near_first):
            z = lax.rem(line + far, lines)
            with jax.named_scope("wait_a%d" % step):
                wait_for(tiles, MATES * (planes - (own_there and step == 0)), sems.at[z])
            with jax.named_scope("propagate"):
                packed = share_tiles(tiles, z)
                at = pl.ds(pl.multiple_of(z * share, share), share // 2)
                lower += jnp.dot(
                    block_rows[:, :, :, at].reshape(MATES * 2 * rows, share // 2),
                    packed, preferred_element_type=F32,
                )
                at = pl.ds(pl.multiple_of(z * share + share // 2, share // 2), share // 2)
                upper += jnp.dot(
                    block_rows[:, :, :, at].reshape(MATES * 2 * rows, share // 2),
                    packed, preferred_element_type=F32,
                )
            last = step == lines - 1
            if last:
                mixed = jnp.where(lane < cols // 2, lower, upper)
                total = mixed + pltpu.roll(mixed, cols // 2, 1)
                total = total.reshape(MATES, 2, rows, cols)
                cross = pltpu.roll(total[:, 1].reshape(MATES * rows, cols), slice_b, 1)
                cross = cross.reshape(MATES, rows, cols)
                result = total[:, 0] + jnp.where(in_slice < slice_b, -cross, cross)
                out[...] = jnp.where(
                    lane < cols // 2, result[:, :half], result[:, half:]
                ).astype(BF16)
                if sort:
                    to_sibling_mates(out, landed, 13, land_sem)
            if sort:
                with jax.named_scope("sort0"):
                    sort_share(tiles, far, step == 0, last)

    def sort_all():
        with jax.named_scope("sorta"):
            for step, far in enumerate(near_first):
                sort_share(adj, far, step == 0, step == lines - 1)

    def first_layer():
        with jax.named_scope("forward1"):
            to_clans(outgoing, adj_two, 6, two_sem.at[line], group, offsets[:-1])
            adj_two[clan_tiles] = outgoing[...]
            to_mates(outgoing, landed, 7, land_sem)

    @pl.when(group == top)
    def _():
        wait_rows(0)
        receive(adj, rows_all, adj_sem, True, outgoing, False)
        first_layer()
        relay_rows(rows_two, 1)
        start_fields()
        build_fwd()
        wait_rows(1)
        pl.semaphore_signal(go_sem, inc=1, device_id=(sibling, me), device_id_type=MESH)
        receive(adj_two, rows_two, two_sem, True, outgoing_two, False)
        with jax.named_scope("forward2"):
            to_clans(outgoing_two, adj, 12, adj_sem.at[line], helper, offsets)
            to_sibling(adj_two, adj, 15, hand_sem.at[1])
            to_sibling_mates(outgoing_two, landed, 13, land_sem)
        relay_fields()
        build_adj()
        sort_all()

    with jax.named_scope("wait_f"):
        wait_for(fwd, peers - MATES, fwd_sem)
    with jax.named_scope("sortf"):
        for k in range(steps):
            count = depth // rows
            flat_fwd = unpack(fwd[pl.ds(k * count, count)])
            stretched[pl.ds(k * depth, depth), :] = flat_fwd
        sign = jnp.where(in_slice < slice_b, 1.0, -1.0)
        quads = chunk // band

        @pl.loop(0, harm // chunk)
        def _(r):
            at = pl.ds(pl.multiple_of(r * chunk, chunk), chunk)
            total = jnp.zeros((chunk, cols), F32)
            for k in range(steps):
                total += jnp.dot(
                    hot_fwd[at, pl.ds(k * depth, depth)], stretched[pl.ds(k * depth, depth), :],
                    preferred_element_type=F32,
                )
            real = total * sign
            imag = pltpu.roll(total, slice_b, 1)
            for pair in range(quads // 2):
                lo, mid, hi = 2 * pair * band, (2 * pair + 1) * band, (2 * pair + 2) * band
                upper = jnp.where(lane < cols // 2, real[lo:mid], real[mid:hi])
                lower = jnp.where(lane < cols // 2, imag[lo:mid], imag[mid:hi])
                both = jnp.concatenate([upper, lower], axis=0)
                factor[r, :, pl.ds(pair * cols, cols)] = both.astype(BF16)

    def correlate(made, into):
        with jax.named_scope("gram"):
            quad = chunk // band
            view = (MATES + 2) * band
            gram = jnp.zeros((2 * band, view), F32)
            for n in range(harm // chunk):
                start = (MATES * clan + quad * n) * band
                window = []
                for k in range(quad):
                    buffer = shifted if k % 2 else lined
                    at = pl.ds(pl.multiple_of(start + (k - k % 2) * band, 2 * band), view)
                    window.append(buffer[:, at])
                gram += jnp.dot(made[n], jnp.concatenate(window, axis=0), preferred_element_type=F32)
            for m in range(MATES):
                if m % 2:
                    both = gram[:, (m - 1) * band : (m + 3) * band]
                    turned = pltpu.roll(both, 2 * band + 1, 1, stride=1, stride_axis=0)[:, : 2 * band]
                else:
                    both = gram[:, m * band : (m + 2) * band]
                    turned = pltpu.roll(both, band + 1, 1, stride=1, stride_axis=0)
                real = jnp.sum(turned[:band], axis=0, keepdims=True)
                imag = jnp.sum(turned[band:], axis=0, keepdims=True)
                into[m] = jnp.where(lane < band, real, imag)

    @pl.when(group == 0)
    def _():
        to_sibling(factor, factor_two, 16, hand_sem.at[1])

    @pl.when(group == top - 1)
    def _():
        with jax.named_scope("wait_adj"):
            wait_for(adj, peers, hand_sem.at[1])
        sort_all()

    @pl.when(group == helper)
    def _():
        wait_rows(0)
        receive(adj, rows_all, adj_sem, False, outgoing, False)
        first_layer()
        sort_all()

    @pl.when(group > 0)
    def _():
        correlate(factor, partial)
        to_mates(partial, gathered, 8, part_sem)

    @pl.when(group == helper)
    def _():
        wait_rows(1)
        with jax.named_scope("wait_factor"):
            wait_for(factor_two, harm // chunk, hand_sem.at[1])
        receive(adj_two, rows_two, two_sem, True, outgoing_two, True)
        correlate(factor_two, partial_two)
        to_sibling_mates(partial_two, gathered, 14, part_sem)

    with jax.named_scope("land"):
        @pl.when(chain)
        def _():
            wait_for(landed, MATES - 1, land_sem)

        @pl.when(jnp.logical_not(chain))
        def _():
            wait_for(landed, MATES, land_sem)

        pieces = [landed[m].astype(F32) for m in range(MATES)]
        for plane in range(2):
            for upper in range(2):
                where = 2 * upper + plane
                tile = None
                for m in range(MATES):
                    shift = (m - where) * slice_b % cols
                    moved = pltpu.roll(pieces[m], shift, 1) if shift else pieces[m]
                    tile = moved if m == 0 else jnp.where(lane < m * slice_b, tile, moved)
                bound_ref[0, plane, pl.ds(upper * half, half), :] = tile.astype(BF16)

    with jax.named_scope("sum"):
        @pl.when(group > 0)
        def _():
            wait_for(gathered, MATES - 1, part_sem)

        @pl.when(group == 0)
        def _():
            wait_for(gathered, MATES, part_sem)

        total = gathered[0]
        for m in range(1, MATES):
            total = total + gathered[m]
        total = total * scale
        grads_ref[0, 0:1, :] = total[:, :band]
        grads_ref[0, 1:2, :] = total[:, band:]

    with jax.named_scope("drain"):
        wait_for(stage_fld, MATES - 1, send_sem.at[2])
        wait_for(fwd, peers - MATES, send_sem.at[3])

        @pl.when(chain)
        def _():
            for turn in (0, 1):
                wait_for(rows_all, 2, send_sem.at[9 * turn])
                wait_for(rows_all, 1, send_sem.at[9 * turn + 1])
            wait_for(stage_src, MATES - 1, send_sem.at[4])
            wait_for(adj, peers - MATES, send_sem.at[6])
            wait_for(landed, MATES - 1, send_sem.at[7])
            wait_for(landed, MATES, send_sem.at[13])

        @pl.when(jnp.logical_not(chain))
        def _():
            wait_for(rows_all, 1, send_sem.at[11])

        @pl.when(group > 0)
        def _():
            wait_for(gathered, MATES - 1, send_sem.at[8])

        @pl.when(group == top)
        def _():
            wait_for(adj, MATES * len(near), send_sem.at[5])
            wait_for(adj, peers, send_sem.at[12])
            wait_for(adj, peers, send_sem.at[15])

        @pl.when(group == helper)
        def _():
            wait_for(adj, MATES * len(far), send_sem.at[5])
            wait_for(gathered, MATES, send_sem.at[14])

        @pl.when(group == 0)
        def _():
            wait_for(factor, harm // chunk, send_sem.at[16])


def solution(mesh):
    layers, peers = mesh.shape["layer"], mesh.shape["harm"]

    def per_device(source, transfer, fields, orders):
        rows, cols = source.shape[1], source.shape[2]
        harm = rows * peers
        band = 2 * rows
        chunk = min(256, harm)
        vmem = pl.BlockSpec(memory_space=pltpu.VMEM)
        hbm = pl.BlockSpec(memory_space=pltpu.HBM)
        tile = (rows // 2, cols)
        return pl.pallas_call(
            functools.partial(kernel, layers, peers, 1.0 / math.sqrt(harm * cols)),
            out_shape=(
                jax.ShapeDtypeStruct((1, 2, band), F32),
                jax.ShapeDtypeStruct((1, 2, rows, cols), BF16),
            ),
            in_specs=[hbm] * 4,
            out_specs=(vmem, vmem),
            scratch_shapes=[
                pltpu.VMEM((2, rows, cols), BF16),
                pltpu.VMEM((2, rows, cols), BF16),
                pltpu.VMEM((1, harm), jnp.int32),
                pltpu.VMEM((2, rows, harm), BF16),
                *[pltpu.VMEM((MATES, 2, rows, harm), BF16)] * 2,
                *[pltpu.VMEM((peers, *tile), BF16)] * 3,
                pltpu.VMEM((harm, cols), BF16),
                pltpu.VMEM((harm, cols), F32),
                pltpu.VMEM((harm, harm), BF16),
                pltpu.VMEM((harm, harm + 2 * cols), BF16),
                pltpu.VMEM((2 * cols // MATES, 3 * harm), BF16),
                pltpu.VMEM((2 * cols // MATES, 3 * harm), BF16),
                *[pltpu.VMEM((harm // chunk, 2 * band, chunk // band * 2 * (cols // MATES)), BF16)] * 2,
                *[pltpu.VMEM((MATES, *tile), BF16)] * 7,
                *[pltpu.VMEM((MATES, 1, cols), F32)] * 3,
                pltpu.VMEM((2 * cols // MATES, harm + 2 * cols), F32),
                pltpu.SemaphoreType.DMA((4,)),
                pltpu.SemaphoreType.DMA((17,)),
                pltpu.SemaphoreType.DMA((12,)),
                pltpu.SemaphoreType.DMA((LINES,)),
                pltpu.SemaphoreType.DMA((LINES,)),
                pltpu.SemaphoreType.DMA((2,)),
                pltpu.SemaphoreType.DMA,
                pltpu.SemaphoreType.DMA((2,)),
                pltpu.SemaphoreType.DMA,
                pltpu.SemaphoreType.DMA,
                *[pltpu.SemaphoreType.REGULAR] * 4,
            ],
            compiler_params=pltpu.CompilerParams(
                collective_id=0, has_side_effects=True, vmem_limit_bytes=44 * 1024 * 1024
            ),
        )(
            *(
                pltpu.with_memory_space_constraint(value, pltpu.HBM)
                for value in (source, transfer, fields, orders.reshape(1, harm))
            )
        )

    return jax.shard_map(
        per_device,
        mesh=mesh,
        in_specs=(
            P(None, "harm", None),
            P("layer", None, "harm", None),
            P("layer", None, "harm", None),
            P(),
        ),
        out_specs=(P("layer", None, "harm"), P("layer", None, "harm", None)),
        check_vma=False,
    )
```

```python
import functools
import math

import jax
import jax.numpy as jnp
from jax import lax
from jax.experimental import pallas as pl
from jax.experimental.pallas import tpu as pltpu
from jax.sharding import PartitionSpec as P

MESH = pl.DeviceIdType.MESH
F32 = jnp.float32
BF16 = jnp.bfloat16
MATES = 4
LINES = 4


def kernel(
    layers, peers, scale,
    source_hbm, transfer_hbm, fields_hbm, orders_hbm, grads_ref, bound_ref,
    source, fields, orders, rows_own, rows_all, rows_two, adj, adj_two, fwd, stretched, column, hot_fwd, hot_adj, lined, shifted, factor, factor_two,
    packed_src, packed_fld, stage_src, stage_fld, outgoing, outgoing_two, landed, partial, partial_two, gathered, sorting,
    load_sem, send_sem, rows_sem, adj_sem, two_sem, hand_sem, fwd_sem, stage_sem, land_sem, part_sem, clear_sem, line_sem, plane_sem, go_sem,
):
    group = lax.axis_index("layer")
    me = lax.axis_index("harm")
    mate = me % MATES
    clan = me // MATES
    clans = peers // MATES
    lines = min(LINES, clans)
    planes = clans // lines
    line = clan % lines
    plane_at = clan // lines
    rows = source.shape[1]
    half = rows // 2
    cols = source.shape[2]
    slice_b = cols // MATES
    harm = rows * peers
    band = 2 * rows
    depth = min(256, harm)
    steps = harm // depth
    top = layers - 1
    helper = top - 2
    chain = (group == top) | (group == helper)
    sibling = jnp.where(chain, jnp.maximum(group - 1, 0), jnp.minimum(group + 1, top))
    far_line = lines // 2
    clan_rows = MATES * rows
    share = planes * clan_rows

    loads = [
        pltpu.make_async_copy(transfer_hbm.at[0], rows_own, load_sem.at[3]),
        pltpu.make_async_copy(source_hbm, source, load_sem.at[0]),
        pltpu.make_async_copy(fields_hbm.at[0], fields, load_sem.at[2]),
        pltpu.make_async_copy(orders_hbm, orders, load_sem.at[1]),
    ]
    barrier = pltpu.get_barrier_semaphore()

    def mate_index(j):
        return clan * MATES + lax.rem(mate + j, MATES)

    def place(plane, line_of):
        return (plane * lines + line_of) * MATES + mate

    def clan_index(far_line, far_plane):
        return place(lax.rem(plane_at + far_plane, planes), lax.rem(line + far_line, lines))

    def by_distance(size):
        return sorted(range(size), key=lambda d: -min(d, size - d))

    offsets = [(a, b) for a in by_distance(lines) for b in by_distance(planes)]

    near_lines = [place(plane_at, lax.rem(line + far, lines)) for far in (1, lines - 1)]
    near_planes = [place(lax.rem(plane_at + far, planes), line) for far in (2, 1, 3)]

    with jax.named_scope("signal"):
        for index in near_lines + near_planes + [mate_index(j) for j in (2, 1, 3)]:
            pl.semaphore_signal(barrier, inc=1, device_id=(group, index), device_id_type=MESH)

        @pl.when(chain)
        def _():
            pl.semaphore_signal(barrier, inc=1, device_id=(sibling, me), device_id_type=MESH)

        @pl.when(group == top)
        def _():
            pl.semaphore_signal(barrier, inc=1, device_id=(helper, me), device_id_type=MESH)
            pl.semaphore_signal(
                barrier, inc=1, device_id=(helper, clan_index(far_line, 0)), device_id_type=MESH
            )

    for load in loads:
        load.start()

    lane = lax.broadcasted_iota(jnp.int32, (1, cols), 1)
    in_slice = lax.rem(lane, 2 * slice_b)

    def pack(block, into):
        value = block[...].astype(F32)
        for m in range(MATES):
            parts = []
            for where in range(4):
                plane, upper = where % 2, where // 2
                piece = value[plane, upper * half : (upper + 1) * half, :]
                shift = (where - m) * slice_b % cols
                parts.append(pltpu.roll(piece, shift, 1) if shift else piece)
            tile = parts[3]
            for where in range(2, -1, -1):
                tile = jnp.where(lane < (where + 1) * slice_b, parts[where], tile)
            into[m] = tile.astype(BF16)

    border = harm - cols
    wide = harm + 2 * cols
    chunk = min(256, harm)

    with jax.named_scope("pack"):
        loads[1].wait()
        pack(source, packed_src)
        loads[2].wait()
        pack(fields, packed_fld)
        for buffer in (lined, shifted):
            buffer[:, pl.ds(0, border)] = jnp.zeros((2 * slice_b, border), BF16)
            buffer[:, pl.ds(border + wide, border)] = jnp.zeros((2 * slice_b, border), BF16)
        loads[3].wait()

    def arrange():
        value = rows_own[...].reshape(2 * rows, harm)
        count = harm // clan_rows
        stacked = jnp.concatenate(
            [value[:, k * clan_rows : (k + 1) * clan_rows] for k in range(count)], axis=0
        )
        at = lax.broadcasted_iota(jnp.int32, (clan_rows, 2 * clan_rows), 0)
        to = lax.broadcasted_iota(jnp.int32, (clan_rows, 2 * clan_rows), 1)
        inside = to % clan_rows
        upper = (inside // (clan_rows // 2) + to // clan_rows) % 2
        origin = inside % (clan_rows // 2) // half * rows + upper * half + inside % half
        order = jnp.where(at == origin, 1.0, 0.0).astype(BF16)
        moved = jnp.dot(stacked, order, preferred_element_type=F32)
        moved = moved.reshape(count, 2, rows, 2 * clan_rows)
        for z in range(lines):
            for pair in range(planes // 2):
                first = moved[2 * pair * lines + z]
                second = moved[(2 * pair + 1) * lines + z]
                lower = jnp.where(lane < cols // 2, first[:, :, :clan_rows], second[:, :, clan_rows:])
                upper = jnp.where(lane < cols // 2, first[:, :, clan_rows:], second[:, :, :clan_rows])
                start = z * share + pair * clan_rows
                rows_all[mate, :, :, pl.ds(start, clan_rows)] = lower.astype(BF16)
                rows_all[mate, :, :, pl.ds(start + share // 2, clan_rows)] = upper.astype(BF16)

    with jax.named_scope("arrange"):
        loads[0].wait()
        arrange()

    def build_fwd():
        with jax.named_scope("hotf"):

            @pl.loop(0, harm // chunk)
            def _(r):
                index = lax.broadcasted_iota(jnp.int32, (chunk, depth), 0)
                order = r * chunk + (index // band) * band + (band - 1) - index % band
                for k in range(steps):
                    hit = orders[:, pl.ds(k * depth, depth)] == order
                    hot_fwd[
                        pl.ds(pl.multiple_of(r * chunk, chunk), chunk), pl.ds(k * depth, depth)
                    ] = jnp.where(hit, 1.0, 0.0).astype(BF16)

    def build_adj():
        with jax.named_scope("hota"):
            for k in range(harm // cols):
                row = orders[:, pl.ds(k * cols, cols)].astype(F32)
                column[pl.ds(k * cols, cols), :] = jnp.broadcast_to(row, (cols, cols)).T

            @pl.loop(0, peers)
            def _(tile):
                owner = tile // MATES
                spot = (owner // lines) * MATES + tile % MATES
                for upper in range(2):
                    order = column[pl.ds(pl.multiple_of(tile * rows + upper * half, half), half), :]
                    row = (owner % lines) * share + upper * (share // 2) + spot * half
                    row = pl.ds(pl.multiple_of(row, half), half)
                    for k in range(wide // cols):
                        want = (lane + (k * cols - cols + 1)).astype(F32)
                        hot_adj[row, pl.ds(k * cols, cols)] = jnp.where(order == want, 1.0, 0.0).astype(BF16)

    with jax.named_scope("barrier"):

        close = len(near_lines) + len(near_planes) + MATES - 1

        @pl.when(jnp.logical_not(chain))
        def _():
            pl.semaphore_wait(barrier, close + 1)

        @pl.when(group == helper)
        def _():
            pl.semaphore_wait(barrier, close + 2)

        @pl.when(group == top)
        def _():
            pl.semaphore_wait(barrier, close)

        for index in near_planes:
            pl.semaphore_signal(plane_sem, inc=1, device_id=(group, index), device_id_type=MESH)

    def near_here():
        with jax.named_scope("near"):
            pl.semaphore_wait(plane_sem, len(near_planes))
            for index in near_lines:
                pl.semaphore_signal(line_sem, inc=1, device_id=(group, index), device_id_type=MESH)

    def all_here():
        with jax.named_scope("here"):
            pl.semaphore_wait(line_sem, len(near_lines))

            @pl.when(jnp.logical_not(chain))
            def _():
                pl.semaphore_signal(clear_sem, inc=1, device_id=(sibling, me), device_id_type=MESH)

            @pl.when(group == helper)
            def _():
                pl.semaphore_signal(clear_sem, inc=1, device_id=(top, me), device_id_type=MESH)

    def remote(src, dst, arrived, target, index):
        return pltpu.make_async_remote_copy(
            src_ref=src, dst_ref=dst, send_sem=send_sem, recv_sem=arrived,
            device_id=(target, index), device_id_type=MESH,
        )

    def wait_for(buffer, count, sem):
        part_of = buffer.at[pl.ds(0, count)]
        pltpu.make_async_copy(part_of, part_of, sem).wait()

    def to_mates(tiles, dst, arrived):
        for j in (2, 1, 3):
            other = lax.rem(mate + j, MATES)
            remote(
                tiles.at[other], dst.at[mate], arrived, group, clan * MATES + other
            ).start()
        dst[mate] = tiles[mate]

    clan_tiles = pl.ds(clan * MATES, MATES)

    def to_clans(tiles, dst, arrived, target, to):
        for a, b in to:
            remote(tiles, dst.at[clan_tiles], arrived, target, clan_index(a, b)).start()

    right, left = mate_index(1), mate_index(MATES - 1)
    from_left, from_right = lax.rem(mate + MATES - 1, MATES), lax.rem(mate + 1, MATES)

    def start_rows(buffer, turn):
        for first in (0, 1):
            to_right = buffer.at[mate, first]
            to_left = buffer.at[mate, 1 - first]
            for block, to, sem in ((to_right, right, 0), (to_left, left, 1)):
                remote(block, block, rows_sem.at[3 * turn + (2 if first else sem)], group, to).start()

    def wait_half(turn, sem):
        wait_for(rows_all.at[0], 1, rows_sem.at[3 * turn + sem])

    def relay_rows(buffer, turn):
        with jax.named_scope("relay_t%d" % turn):
            wait_half(turn, 0)
            block = buffer.at[from_left, 0]
            remote(block, block, rows_sem.at[3 * turn + 2], group, right).start()
            wait_half(turn, 1)
            block = buffer.at[from_right, 1]
            remote(block, block, rows_sem.at[3 * turn + 2], group, left).start()

    def wait_rows(turn):
        with jax.named_scope("wait_t%d" % turn):
            wait_for(rows_all, 2, rows_sem.at[3 * turn + 2])

    def to_sibling(src, dst, arrived):
        remote(src, dst, arrived, sibling, me).start()

    def to_sibling_mates(tiles, dst, arrived):
        for j in (2, 1, 3, 0):
            other = lax.rem(mate + j, MATES)
            remote(
                tiles.at[other], dst.at[mate], arrived, sibling, clan * MATES + other
            ).start()

    def start_fields():
        to_mates(packed_fld, stage_fld, stage_sem.at[0])

    def relay_fields():
        with jax.named_scope("relay_f"):
            wait_for(stage_fld, MATES - 1, stage_sem.at[0])
            to_clans(stage_fld, fwd, fwd_sem, group, offsets[:-1])
            fwd[clan_tiles] = stage_fld[...]

    with jax.named_scope("spread"):

        near = [offset for offset in offsets[:-1] if offset[0] != far_line]
        far = [offset for offset in offsets if offset[0] == far_line]

        def relay_source(to):
            with jax.named_scope("relay_s"):
                wait_for(stage_src, MATES - 1, stage_sem.at[1])
                to_clans(stage_src, adj, adj_sem.at[line], top, to)

        @pl.when(group == top)
        def _():
            to_mates(packed_src, stage_src, stage_sem.at[1])
            start_rows(rows_all, 0)
            near_here()
            relay_source(near)
            adj[clan_tiles] = stage_src[...]
            relay_rows(rows_all, 0)
            wait_for(rows_all, 1, hand_sem.at[0])
            start_rows(rows_two, 1)
            all_here()
            pl.semaphore_wait(clear_sem, 2)

        @pl.when(group == helper)
        def _():
            to_mates(packed_src, stage_src, stage_sem.at[1])
            near_here()
            relay_source(far)
            all_here()
            start_fields()
            start_rows(rows_all, 0)
            build_fwd()
            relay_fields()
            relay_rows(rows_all, 0)
            wait_for(rows_all, 1, hand_sem.at[0])
            start_rows(rows_two, 1)
            build_adj()
            relay_rows(rows_two, 1)
            pl.semaphore_wait(clear_sem, 1)

        @pl.when(jnp.logical_not(chain))
        def _():
            to_sibling(rows_all.at[mate], rows_two.at[mate], hand_sem.at[0])
            near_here()
            all_here()
            start_fields()
            build_fwd()

            @pl.when(group == top - 1)
            def _():
                build_adj()
                pl.semaphore_wait(go_sem, 1)

            relay_fields()

    def unpack(tiles):
        count = tiles.shape[0]
        value = tiles.astype(F32)
        turned = pltpu.roll(value.reshape(count * half, cols), cols // 2, 1).reshape(value.shape)
        lower = jnp.where(lane < cols // 2, value, turned)
        upper = jnp.where(lane < cols // 2, turned, value)
        return jnp.concatenate([lower, upper], axis=1).reshape(count * rows, cols).astype(BF16)

    def share_tiles(tiles, z):
        return jnp.concatenate(
            [tiles[pl.ds((p * lines + z) * MATES, MATES)].reshape(MATES * half, cols) for p in range(planes)],
            axis=0,
        )

    def sort_share(tiles, far, first, last):
        z = lax.rem(line + far, lines)
        turned = share_tiles(tiles, z).astype(F32).T.astype(BF16)
        left = jnp.concatenate([turned[: cols // 2], turned[cols // 2 :]], axis=1)
        at = pl.ds(pl.multiple_of(z * share, share), share)
        span = 3 * depth if wide % (3 * depth) == 0 else wide
        tail = None
        for k in reversed(range(wide // span)):
            here = pl.ds(k * span, span)
            total = jnp.dot(left, hot_adj[at, here], preferred_element_type=F32)
            if not first:
                total += sorting[:, here]
            if not last:
                sorting[:, here] = total
                continue
            lined[:, pl.ds(border + k * span, span)] = total.astype(BF16)
            pieces = [
                pltpu.roll(total[:, i * cols : (i + 1) * cols], cols // 2, 1) for i in range(span // cols)
            ]
            pieces.append(jnp.zeros_like(pieces[0]) if tail is None else tail)
            tail = pieces[0]
            for i in range(span // cols):
                shifted[:, pl.ds(border + k * span + i * cols, cols)] = jnp.where(
                    lane < cols // 2, pieces[i], pieces[i + 1]
                ).astype(BF16)
        if last:
            shifted[:, pl.ds(border - cols, cols)] = jnp.where(lane < cols // 2, 0.0, tail).astype(BF16)

    near_first = by_distance(lines)[::-1]
    one_by_one = [[far] for far in near_first]
    near_and_rest = [near_first[:1], near_first[1:]]

    def receive(tiles, block_rows, sems, own_there, out, sort):
        lower = jnp.zeros((MATES * 2 * rows, cols), F32)
        upper = jnp.zeros((MATES * 2 * rows, cols), F32)
        turns = one_by_one if sort else near_and_rest
        for step, fars in enumerate(turns):
            spots = [lax.rem(line + far, lines) for far in fars]
            with jax.named_scope("wait_a%d" % step):
                for z in spots:
                    wait_for(tiles, MATES * (planes - (own_there and step == 0)), sems.at[z])
            with jax.named_scope("propagate"):
                for z in spots:
                    packed = share_tiles(tiles, z)
                    at = pl.ds(pl.multiple_of(z * share, share), share // 2)
                    lower += jnp.dot(
                        block_rows[:, :, :, at].reshape(MATES * 2 * rows, share // 2),
                        packed, preferred_element_type=F32,
                    )
                    at = pl.ds(pl.multiple_of(z * share + share // 2, share // 2), share // 2)
                    upper += jnp.dot(
                        block_rows[:, :, :, at].reshape(MATES * 2 * rows, share // 2),
                        packed, preferred_element_type=F32,
                    )
            last = step == len(turns) - 1
            if last:
                mixed = jnp.where(lane < cols // 2, lower, upper).reshape(MATES, 2, rows, cols)
                head, rest = mixed[:, :, :half], mixed[:, :, half:]
                here = jnp.where(lane < cols // 2, head, rest)
                there = jnp.where(lane < cols // 2, rest, head).reshape(MATES * 2 * half, cols)
                total = here + pltpu.roll(there, cols // 2, 1).reshape(MATES, 2, half, cols)
                cross = total[:, 1].reshape(MATES * half, cols)
                cross = jnp.where(
                    in_slice < slice_b,
                    -pltpu.roll(cross, cols - slice_b, 1),
                    pltpu.roll(cross, slice_b, 1),
                )
                out[...] = (total[:, 0] + cross.reshape(MATES, half, cols)).astype(BF16)
                if sort:
                    to_sibling_mates(out, landed, land_sem)
            if sort:
                with jax.named_scope("sort0"):
                    sort_share(tiles, fars[0], step == 0, last)

    def sort_all():
        with jax.named_scope("sorta"):
            for step, far in enumerate(near_first):
                sort_share(adj, far, step == 0, step == lines - 1)

    def first_layer():
        with jax.named_scope("forward1"):
            to_clans(outgoing, adj_two, two_sem.at[line], group, offsets[:-1])
            adj_two[clan_tiles] = outgoing[...]
            to_mates(outgoing, landed, land_sem)

    @pl.when(group == top)
    def _():
        wait_rows(0)
        receive(adj, rows_all, adj_sem, True, outgoing, False)
        first_layer()
        relay_rows(rows_two, 1)
        start_fields()
        build_fwd()
        wait_rows(1)
        pl.semaphore_signal(go_sem, inc=1, device_id=(sibling, me), device_id_type=MESH)
        receive(adj_two, rows_two, two_sem, True, outgoing_two, False)
        with jax.named_scope("forward2"):
            to_clans(outgoing_two, adj, adj_sem.at[line], helper, offsets)
            to_sibling(adj_two, adj, hand_sem.at[1])
            to_sibling_mates(outgoing_two, landed, land_sem)
        relay_fields()
        build_adj()
        sort_all()

    with jax.named_scope("wait_f"):
        wait_for(fwd, peers - MATES, fwd_sem)
    with jax.named_scope("sortf"):
        for k in range(steps):
            count = depth // rows
            flat_fwd = unpack(fwd[pl.ds(k * count, count)])
            stretched[pl.ds(k * depth, depth), :] = flat_fwd
        sign = jnp.where(in_slice < slice_b, 1.0, -1.0)
        quads = chunk // band

        @pl.loop(0, harm // chunk)
        def _(r):
            at = pl.ds(pl.multiple_of(r * chunk, chunk), chunk)
            total = jnp.zeros((chunk, cols), F32)
            for k in range(steps):
                total += jnp.dot(
                    hot_fwd[at, pl.ds(k * depth, depth)], stretched[pl.ds(k * depth, depth), :],
                    preferred_element_type=F32,
                )
            real = total * sign
            imag = pltpu.roll(total, slice_b, 1)
            for pair in range(quads // 2):
                lo, mid, hi = 2 * pair * band, (2 * pair + 1) * band, (2 * pair + 2) * band
                upper = jnp.where(lane < cols // 2, real[lo:mid], real[mid:hi])
                lower = jnp.where(lane < cols // 2, imag[lo:mid], imag[mid:hi])
                both = jnp.concatenate([upper, lower], axis=0)
                factor[r, :, pl.ds(pair * cols, cols)] = both.astype(BF16)

    def correlate(made, into):
        with jax.named_scope("gram"):
            quad = chunk // band
            view = (MATES + 2) * band
            gram = jnp.zeros((2 * band, view), F32)
            for n in range(harm // chunk):
                start = (MATES * clan + quad * n) * band
                window = []
                for k in range(quad):
                    buffer = shifted if k % 2 else lined
                    at = pl.ds(pl.multiple_of(start + (k - k % 2) * band, 2 * band), view)
                    window.append(buffer[:, at])
                gram += jnp.dot(made[n], jnp.concatenate(window, axis=0), preferred_element_type=F32)
            for m in range(MATES):
                if m % 2:
                    both = gram[:, (m - 1) * band : (m + 3) * band]
                    turned = pltpu.roll(both, 2 * band + 1, 1, stride=1, stride_axis=0)[:, : 2 * band]
                else:
                    both = gram[:, m * band : (m + 2) * band]
                    turned = pltpu.roll(both, band + 1, 1, stride=1, stride_axis=0)
                real = jnp.sum(turned[:band], axis=0, keepdims=True)
                imag = jnp.sum(turned[band:], axis=0, keepdims=True)
                into[m] = jnp.where(lane < band, real, imag)

    @pl.when(group == 0)
    def _():
        to_sibling(factor, factor_two, hand_sem.at[1])

    @pl.when(group == top - 1)
    def _():
        with jax.named_scope("wait_adj"):
            wait_for(adj, peers, hand_sem.at[1])
        sort_all()

    @pl.when(group == helper)
    def _():
        wait_rows(0)
        receive(adj, rows_all, adj_sem, False, outgoing, False)
        first_layer()
        sort_all()

    @pl.when(group > 0)
    def _():
        correlate(factor, partial)
        to_mates(partial, gathered, part_sem)

    @pl.when(group == helper)
    def _():
        wait_rows(1)
        with jax.named_scope("wait_factor"):
            wait_for(factor_two, harm // chunk, hand_sem.at[1])
        receive(adj_two, rows_two, two_sem, True, outgoing_two, True)
        correlate(factor_two, partial_two)
        to_sibling_mates(partial_two, gathered, part_sem)

    with jax.named_scope("land"):
        @pl.when(chain)
        def _():
            wait_for(landed, MATES - 1, land_sem)

        @pl.when(jnp.logical_not(chain))
        def _():
            wait_for(landed, MATES, land_sem)

        pieces = [landed[m].astype(F32) for m in range(MATES)]
        for plane in range(2):
            for upper in range(2):
                where = 2 * upper + plane
                tile = None
                for m in range(MATES):
                    shift = (m - where) * slice_b % cols
                    moved = pltpu.roll(pieces[m], shift, 1) if shift else pieces[m]
                    tile = moved if m == 0 else jnp.where(lane < m * slice_b, tile, moved)
                bound_ref[0, plane, pl.ds(upper * half, half), :] = tile.astype(BF16)

    with jax.named_scope("sum"):
        @pl.when(group > 0)
        def _():
            wait_for(gathered, MATES - 1, part_sem)

        @pl.when(group == 0)
        def _():
            wait_for(gathered, MATES, part_sem)

        total = gathered[0]
        for m in range(1, MATES):
            total = total + gathered[m]
        total = total * scale
        grads_ref[0, 0:1, :] = total[:, :band]
        grads_ref[0, 1:2, :] = total[:, band:]

    with jax.named_scope("drain"):
        wait_for(stage_fld, MATES - 1, send_sem)
        wait_for(fwd, peers - MATES, send_sem)

        @pl.when(chain)
        def _():
            for turn in (0, 1):
                wait_for(rows_all, 2, send_sem)
                wait_for(rows_all, 1, send_sem)
            wait_for(stage_src, MATES - 1, send_sem)
            wait_for(adj, peers - MATES, send_sem)
            wait_for(landed, MATES - 1, send_sem)
            wait_for(landed, MATES, send_sem)

        @pl.when(jnp.logical_not(chain))
        def _():
            wait_for(rows_all, 1, send_sem)

        @pl.when(group > 0)
        def _():
            wait_for(gathered, MATES - 1, send_sem)

        @pl.when(group == top)
        def _():
            wait_for(adj, MATES * len(near), send_sem)
            wait_for(adj, peers, send_sem)
            wait_for(adj, peers, send_sem)

        @pl.when(group == helper)
        def _():
            wait_for(adj, MATES * len(far), send_sem)
            wait_for(gathered, MATES, send_sem)

        @pl.when(group == 0)
        def _():
            wait_for(factor, harm // chunk, send_sem)


def put_out(grads_ref, bound_ref, grads_hbm, bound_hbm, sems):
    copies = [
        pltpu.make_async_copy(bound_ref, bound_hbm, sems.at[0]),
        pltpu.make_async_copy(grads_ref, grads_hbm, sems.at[1]),
    ]
    for copy in copies:
        copy.start()
    for copy in copies:
        copy.wait()


def solution(mesh):
    layers, peers = mesh.shape["layer"], mesh.shape["harm"]

    def per_device(source, transfer, fields, orders):
        rows, cols = source.shape[1], source.shape[2]
        harm = rows * peers
        band = 2 * rows
        chunk = min(256, harm)
        vmem = pl.BlockSpec(memory_space=pltpu.VMEM)
        hbm = pl.BlockSpec(memory_space=pltpu.HBM)
        tile = (rows // 2, cols)
        made = pl.pallas_call(
            functools.partial(kernel, layers, peers, 1.0 / math.sqrt(harm * cols)),
            out_shape=(
                jax.ShapeDtypeStruct((1, 2, band), F32),
                jax.ShapeDtypeStruct((1, 2, rows, cols), BF16),
            ),
            in_specs=[hbm] * 4,
            out_specs=(vmem, vmem),
            scratch_shapes=[
                pltpu.VMEM((2, rows, cols), BF16),
                pltpu.VMEM((2, rows, cols), BF16),
                pltpu.VMEM((1, harm), jnp.int32),
                pltpu.VMEM((2, rows, harm), BF16),
                *[pltpu.VMEM((MATES, 2, rows, harm), BF16)] * 2,
                *[pltpu.VMEM((peers, *tile), BF16)] * 3,
                pltpu.VMEM((harm, cols), BF16),
                pltpu.VMEM((harm, cols), F32),
                pltpu.VMEM((harm, harm), BF16),
                pltpu.VMEM((harm, harm + 2 * cols), BF16),
                pltpu.VMEM((2 * cols // MATES, 3 * harm), BF16),
                pltpu.VMEM((2 * cols // MATES, 3 * harm), BF16),
                *[pltpu.VMEM((harm // chunk, 2 * band, chunk // band * 2 * (cols // MATES)), BF16)] * 2,
                *[pltpu.VMEM((MATES, *tile), BF16)] * 7,
                *[pltpu.VMEM((MATES, 1, cols), F32)] * 3,
                pltpu.VMEM((2 * cols // MATES, harm + 2 * cols), F32),
                pltpu.SemaphoreType.DMA((4,)),
                pltpu.SemaphoreType.DMA,
                pltpu.SemaphoreType.DMA((6,)),
                pltpu.SemaphoreType.DMA((LINES,)),
                pltpu.SemaphoreType.DMA((LINES,)),
                pltpu.SemaphoreType.DMA((2,)),
                pltpu.SemaphoreType.DMA,
                pltpu.SemaphoreType.DMA((2,)),
                pltpu.SemaphoreType.DMA,
                pltpu.SemaphoreType.DMA,
                *[pltpu.SemaphoreType.REGULAR] * 4,
            ],
            compiler_params=pltpu.CompilerParams(
                collective_id=0, has_side_effects=True, vmem_limit_bytes=44 * 1024 * 1024
            ),
        )(
            *(
                pltpu.with_memory_space_constraint(value, pltpu.HBM)
                for value in (source, transfer, fields, orders.reshape(1, harm))
            )
        )
        return pl.pallas_call(
            put_out,
            out_shape=[jax.ShapeDtypeStruct(value.shape, value.dtype) for value in made],
            in_specs=[vmem] * 2,
            out_specs=[hbm] * 2,
            scratch_shapes=[pltpu.SemaphoreType.DMA((2,))],
            compiler_params=pltpu.CompilerParams(vmem_limit_bytes=1 << 20),
        )(*(pltpu.with_memory_space_constraint(value, pltpu.VMEM) for value in made))

    return jax.shard_map(
        per_device,
        mesh=mesh,
        in_specs=(
            P(None, "harm", None),
            P("layer", None, "harm", None),
            P("layer", None, "harm", None),
            P(),
        ),
        out_specs=(P("layer", None, "harm"), P("layer", None, "harm", None)),
        check_vma=False,
    )
```

```python
import functools
import math

import jax
import jax.numpy as jnp
from jax import lax
from jax.experimental import pallas as pl
from jax.experimental.pallas import tpu as pltpu
from jax.sharding import PartitionSpec as P

MESH = pl.DeviceIdType.MESH
F32 = jnp.float32
BF16 = jnp.bfloat16
MATES = 4
LINES = 4


def kernel(
    layers, peers, scale,
    source_hbm, transfer_hbm, fields_hbm, orders_hbm, grads_ref, bound_ref,
    source, fields, orders, rows_own, rows_all, rows_two, adj, adj_two, fwd, stretched, column, hot_fwd, hot_adj, lined, shifted, factor, factor_two,
    packed_src, packed_fld, stage_src, stage_fld, outgoing, outgoing_two, landed, partial, partial_two, gathered, sorting,
    load_sem, send_sem, rows_sem, adj_sem, two_sem, hand_sem, fwd_sem, stage_sem, land_sem, part_sem, clear_sem, line_sem, plane_sem, go_sem,
):
    group = lax.axis_index("layer")
    me = lax.axis_index("harm")
    mate = me % MATES
    clan = me // MATES
    clans = peers // MATES
    lines = min(LINES, clans)
    planes = clans // lines
    line = clan % lines
    plane_at = clan // lines
    rows = source.shape[1]
    half = rows // 2
    cols = source.shape[2]
    slice_b = cols // MATES
    harm = rows * peers
    band = 2 * rows
    depth = min(256, harm)
    steps = harm // depth
    top = layers - 1
    helper = top - 2
    chain = (group == top) | (group == helper)
    sibling = jnp.where(chain, jnp.maximum(group - 1, 0), jnp.minimum(group + 1, top))
    far_line = lines // 2
    clan_rows = MATES * rows
    share = planes * clan_rows

    loads = [
        pltpu.make_async_copy(transfer_hbm.at[0], rows_own, load_sem.at[3]),
        pltpu.make_async_copy(source_hbm, source, load_sem.at[0]),
        pltpu.make_async_copy(fields_hbm.at[0], fields, load_sem.at[2]),
        pltpu.make_async_copy(orders_hbm, orders, load_sem.at[1]),
    ]
    barrier = pltpu.get_barrier_semaphore()

    def mate_index(j):
        return clan * MATES + lax.rem(mate + j, MATES)

    def place(plane, line_of):
        return (plane * lines + line_of) * MATES + mate

    def clan_index(far_line, far_plane):
        return place(lax.rem(plane_at + far_plane, planes), lax.rem(line + far_line, lines))

    def by_distance(size):
        return sorted(range(size), key=lambda d: -min(d, size - d))

    offsets = [(a, b) for a in by_distance(lines) for b in by_distance(planes)]

    near_lines = [place(plane_at, lax.rem(line + far, lines)) for far in (1, lines - 1)]
    near_planes = [place(lax.rem(plane_at + far, planes), line) for far in (2, 1, 3)]

    with jax.named_scope("signal"):
        for index in near_lines + near_planes + [mate_index(j) for j in (2, 1, 3)]:
            pl.semaphore_signal(barrier, inc=1, device_id=(group, index), device_id_type=MESH)

        @pl.when(chain)
        def _():
            pl.semaphore_signal(barrier, inc=1, device_id=(sibling, me), device_id_type=MESH)

        @pl.when(group == top)
        def _():
            pl.semaphore_signal(barrier, inc=1, device_id=(helper, me), device_id_type=MESH)
            pl.semaphore_signal(
                barrier, inc=1, device_id=(helper, clan_index(far_line, 0)), device_id_type=MESH
            )

    for load in loads:
        load.start()

    lane = lax.broadcasted_iota(jnp.int32, (1, cols), 1)
    in_slice = lax.rem(lane, 2 * slice_b)

    def pack(block, into):
        value = block[...].astype(F32)
        for m in range(MATES):
            parts = []
            for where in range(4):
                plane, upper = where % 2, where // 2
                piece = value[plane, upper * half : (upper + 1) * half, :]
                shift = (where - m) * slice_b % cols
                parts.append(pltpu.roll(piece, shift, 1) if shift else piece)
            tile = parts[3]
            for where in range(2, -1, -1):
                tile = jnp.where(lane < (where + 1) * slice_b, parts[where], tile)
            into[m] = tile.astype(BF16)

    border = harm - cols
    wide = harm + 2 * cols
    chunk = min(256, harm)

    with jax.named_scope("pack"):
        loads[1].wait()
        pack(source, packed_src)
        loads[2].wait()
        pack(fields, packed_fld)
        for buffer in (lined, shifted):
            buffer[:, pl.ds(0, border)] = jnp.zeros((2 * slice_b, border), BF16)
            buffer[:, pl.ds(border + wide, border)] = jnp.zeros((2 * slice_b, border), BF16)
        loads[3].wait()

    def arrange():
        value = rows_own[...].reshape(2 * rows, harm)
        count = harm // clan_rows
        stacked = jnp.concatenate(
            [value[:, k * clan_rows : (k + 1) * clan_rows] for k in range(count)], axis=0
        )
        at = lax.broadcasted_iota(jnp.int32, (clan_rows, 2 * clan_rows), 0)
        to = lax.broadcasted_iota(jnp.int32, (clan_rows, 2 * clan_rows), 1)
        inside = to % clan_rows
        upper = (inside // (clan_rows // 2) + to // clan_rows) % 2
        origin = inside % (clan_rows // 2) // half * rows + upper * half + inside % half
        order = jnp.where(at == origin, 1.0, 0.0).astype(BF16)
        moved = jnp.dot(stacked, order, preferred_element_type=F32)
        moved = moved.reshape(count, 2, rows, 2 * clan_rows)
        for z in range(lines):
            for pair in range(planes // 2):
                first = moved[2 * pair * lines + z]
                second = moved[(2 * pair + 1) * lines + z]
                lower = jnp.where(lane < cols // 2, first[:, :, :clan_rows], second[:, :, clan_rows:])
                upper = jnp.where(lane < cols // 2, first[:, :, clan_rows:], second[:, :, :clan_rows])
                start = z * share + pair * clan_rows
                rows_all[mate, :, :, pl.ds(start, clan_rows)] = lower.astype(BF16)
                rows_all[mate, :, :, pl.ds(start + share // 2, clan_rows)] = upper.astype(BF16)

    with jax.named_scope("arrange"):
        loads[0].wait()
        arrange()

    def build_fwd():
        with jax.named_scope("hotf"):

            @pl.loop(0, harm // chunk)
            def _(r):
                index = lax.broadcasted_iota(jnp.int32, (chunk, depth), 0)
                order = r * chunk + (index // band) * band + (band - 1) - index % band
                for k in range(steps):
                    hit = orders[:, pl.ds(k * depth, depth)] == order
                    hot_fwd[
                        pl.ds(pl.multiple_of(r * chunk, chunk), chunk), pl.ds(k * depth, depth)
                    ] = jnp.where(hit, 1.0, 0.0).astype(BF16)

    def build_adj():
        with jax.named_scope("hota"):
            for k in range(harm // cols):
                row = orders[:, pl.ds(k * cols, cols)].astype(F32)
                column[pl.ds(k * cols, cols), :] = jnp.broadcast_to(row, (cols, cols)).T

            @pl.loop(0, peers)
            def _(tile):
                owner = tile // MATES
                spot = (owner // lines) * MATES + tile % MATES
                for upper in range(2):
                    order = column[pl.ds(pl.multiple_of(tile * rows + upper * half, half), half), :]
                    row = (owner % lines) * share + upper * (share // 2) + spot * half
                    row = pl.ds(pl.multiple_of(row, half), half)
                    for k in range(wide // cols):
                        want = (lane + (k * cols - cols + 1)).astype(F32)
                        hot_adj[row, pl.ds(k * cols, cols)] = jnp.where(order == want, 1.0, 0.0).astype(BF16)

    with jax.named_scope("barrier"):

        close = len(near_lines) + len(near_planes) + MATES - 1

        @pl.when(jnp.logical_not(chain))
        def _():
            pl.semaphore_wait(barrier, close + 1)

        @pl.when(group == helper)
        def _():
            pl.semaphore_wait(barrier, close + 2)

        @pl.when(group == top)
        def _():
            pl.semaphore_wait(barrier, close)

        for index in near_planes:
            pl.semaphore_signal(plane_sem, inc=1, device_id=(group, index), device_id_type=MESH)

    def near_here():
        with jax.named_scope("near"):
            pl.semaphore_wait(plane_sem, len(near_planes))
            for index in near_lines:
                pl.semaphore_signal(line_sem, inc=1, device_id=(group, index), device_id_type=MESH)

    def all_here():
        with jax.named_scope("here"):
            pl.semaphore_wait(line_sem, len(near_lines))

            @pl.when(jnp.logical_not(chain))
            def _():
                pl.semaphore_signal(clear_sem, inc=1, device_id=(sibling, me), device_id_type=MESH)

            @pl.when(group == helper)
            def _():
                pl.semaphore_signal(clear_sem, inc=1, device_id=(top, me), device_id_type=MESH)

    def remote(src, dst, arrived, target, index):
        return pltpu.make_async_remote_copy(
            src_ref=src, dst_ref=dst, send_sem=send_sem, recv_sem=arrived,
            device_id=(target, index), device_id_type=MESH,
        )

    def wait_for(buffer, count, sem):
        part_of = buffer.at[pl.ds(0, count)]
        pltpu.make_async_copy(part_of, part_of, sem).wait()

    def to_mates(tiles, dst, arrived):
        for j in (2, 1, 3):
            other = lax.rem(mate + j, MATES)
            remote(
                tiles.at[other], dst.at[mate], arrived, group, clan * MATES + other
            ).start()
        dst[mate] = tiles[mate]

    clan_tiles = pl.ds(clan * MATES, MATES)

    def to_clans(tiles, dst, arrived, target, to):
        for a, b in to:
            remote(tiles, dst.at[clan_tiles], arrived, target, clan_index(a, b)).start()

    right, left = mate_index(1), mate_index(MATES - 1)
    from_left, from_right = lax.rem(mate + MATES - 1, MATES), lax.rem(mate + 1, MATES)

    def start_rows(buffer, turn):
        for first in (0, 1):
            to_right = buffer.at[mate, first]
            to_left = buffer.at[mate, 1 - first]
            for block, to, sem in ((to_right, right, 0), (to_left, left, 1)):
                remote(block, block, rows_sem.at[3 * turn + (2 if first else sem)], group, to).start()

    def wait_half(turn, sem):
        wait_for(rows_all.at[0], 1, rows_sem.at[3 * turn + sem])

    def relay_rows(buffer, turn):
        with jax.named_scope("relay_t%d" % turn):
            wait_half(turn, 0)
            block = buffer.at[from_left, 0]
            remote(block, block, rows_sem.at[3 * turn + 2], group, right).start()
            wait_half(turn, 1)
            block = buffer.at[from_right, 1]
            remote(block, block, rows_sem.at[3 * turn + 2], group, left).start()

    def wait_rows(turn):
        with jax.named_scope("wait_t%d" % turn):
            wait_for(rows_all, 2, rows_sem.at[3 * turn + 2])

    def to_sibling(src, dst, arrived):
        remote(src, dst, arrived, sibling, me).start()

    def to_sibling_mates(tiles, dst, arrived):
        for j in (2, 1, 3, 0):
            other = lax.rem(mate + j, MATES)
            remote(
                tiles.at[other], dst.at[mate], arrived, sibling, clan * MATES + other
            ).start()

    def start_fields():
        to_mates(packed_fld, stage_fld, stage_sem.at[0])

    def relay_fields():
        with jax.named_scope("relay_f"):
            wait_for(stage_fld, MATES - 1, stage_sem.at[0])
            to_clans(stage_fld, fwd, fwd_sem, group, offsets[:-1])
            fwd[clan_tiles] = stage_fld[...]

    with jax.named_scope("spread"):

        near = [offset for offset in offsets[:-1] if offset[0] != far_line]
        far = [offset for offset in offsets if offset[0] == far_line]

        def relay_source(to):
            with jax.named_scope("relay_s"):
                wait_for(stage_src, MATES - 1, stage_sem.at[1])
                to_clans(stage_src, adj, adj_sem.at[line], top, to)

        @pl.when(group == top)
        def _():
            to_mates(packed_src, stage_src, stage_sem.at[1])
            start_rows(rows_all, 0)
            near_here()
            relay_source(near)
            adj[clan_tiles] = stage_src[...]
            relay_rows(rows_all, 0)
            wait_for(rows_all, 1, hand_sem.at[0])
            start_rows(rows_two, 1)
            all_here()
            pl.semaphore_wait(clear_sem, 2)

        @pl.when(group == helper)
        def _():
            to_mates(packed_src, stage_src, stage_sem.at[1])
            near_here()
            relay_source(far)
            all_here()
            start_fields()
            start_rows(rows_all, 0)
            build_fwd()
            relay_fields()
            relay_rows(rows_all, 0)
            build_adj()
            pl.semaphore_wait(clear_sem, 1)
            pl.semaphore_signal(go_sem, inc=1, device_id=(sibling, me), device_id_type=MESH)

        @pl.when(jnp.logical_not(chain))
        def _():
            @pl.when(group == top - 1)
            def _():
                to_sibling(rows_all.at[mate], rows_two.at[mate], hand_sem.at[0])

            near_here()
            all_here()
            start_fields()

            @pl.when(group == 0)
            def _():
                start_rows(rows_all, 0)

            build_fwd()

            @pl.when(group == top - 1)
            def _():
                build_adj()

            @pl.when(group == 0)
            def _():
                relay_rows(rows_all, 0)

            pl.semaphore_wait(go_sem, 1)
            relay_fields()

    def unpack(tiles):
        count = tiles.shape[0]
        value = tiles.astype(F32)
        turned = pltpu.roll(value.reshape(count * half, cols), cols // 2, 1).reshape(value.shape)
        lower = jnp.where(lane < cols // 2, value, turned)
        upper = jnp.where(lane < cols // 2, turned, value)
        return jnp.concatenate([lower, upper], axis=1).reshape(count * rows, cols).astype(BF16)

    def share_tiles(tiles, z):
        return jnp.concatenate(
            [tiles[pl.ds((p * lines + z) * MATES, MATES)].reshape(MATES * half, cols) for p in range(planes)],
            axis=0,
        )

    def sort_shares(tiles, fars, first, last):
        shares = []
        for far in fars:
            z = lax.rem(line + far, lines)
            turned = share_tiles(tiles, z).astype(F32).T.astype(BF16)
            left = jnp.concatenate([turned[: cols // 2], turned[cols // 2 :]], axis=1)
            shares.append((left, pl.ds(pl.multiple_of(z * share, share), share)))
        span = 3 * depth if wide % (3 * depth) == 0 else wide
        tail = None
        for k in reversed(range(wide // span)):
            here = pl.ds(k * span, span)
            total = jnp.zeros((cols // 2, span), F32) if first else sorting[:, here]
            for left, at in shares:
                total += jnp.dot(left, hot_adj[at, here], preferred_element_type=F32)
            if not last:
                sorting[:, here] = total
                continue
            lined[:, pl.ds(border + k * span, span)] = total.astype(BF16)
            pieces = [
                pltpu.roll(total[:, i * cols : (i + 1) * cols], cols // 2, 1) for i in range(span // cols)
            ]
            pieces.append(jnp.zeros_like(pieces[0]) if tail is None else tail)
            tail = pieces[0]
            for i in range(span // cols):
                shifted[:, pl.ds(border + k * span + i * cols, cols)] = jnp.where(
                    lane < cols // 2, pieces[i], pieces[i + 1]
                ).astype(BF16)
        if last:
            shifted[:, pl.ds(border - cols, cols)] = jnp.where(lane < cols // 2, 0.0, tail).astype(BF16)

    near_first = by_distance(lines)[::-1]
    near_and_rest = [near_first[:1], near_first[1:]]

    def receive(tiles, block_rows, sems, own_there, out):
        lower = jnp.zeros((MATES * 2 * rows, cols), F32)
        upper = jnp.zeros((MATES * 2 * rows, cols), F32)
        for step, fars in enumerate(near_and_rest):
            spots = [lax.rem(line + far, lines) for far in fars]
            with jax.named_scope("wait_a%d" % step):
                for z in spots:
                    wait_for(tiles, MATES * (planes - (own_there and step == 0)), sems.at[z])
            with jax.named_scope("propagate"):
                for z in spots:
                    packed = share_tiles(tiles, z)
                    at = pl.ds(pl.multiple_of(z * share, share), share // 2)
                    lower += jnp.dot(
                        block_rows[:, :, :, at].reshape(MATES * 2 * rows, share // 2),
                        packed, preferred_element_type=F32,
                    )
                    at = pl.ds(pl.multiple_of(z * share + share // 2, share // 2), share // 2)
                    upper += jnp.dot(
                        block_rows[:, :, :, at].reshape(MATES * 2 * rows, share // 2),
                        packed, preferred_element_type=F32,
                    )
            if step == len(near_and_rest) - 1:
                mixed = jnp.where(lane < cols // 2, lower, upper).reshape(MATES, 2, rows, cols)
                head, rest = mixed[:, :, :half], mixed[:, :, half:]
                here = jnp.where(lane < cols // 2, head, rest)
                there = jnp.where(lane < cols // 2, rest, head).reshape(MATES * 2 * half, cols)
                total = here + pltpu.roll(there, cols // 2, 1).reshape(MATES, 2, half, cols)
                cross = total[:, 1].reshape(MATES * half, cols)
                cross = jnp.where(
                    in_slice < slice_b,
                    -pltpu.roll(cross, cols - slice_b, 1),
                    pltpu.roll(cross, slice_b, 1),
                )
                out[...] = (total[:, 0] + cross.reshape(MATES, half, cols)).astype(BF16)

    def receive_sorted(tiles, sems):
        for step, fars in enumerate(near_and_rest):
            for far in fars:
                z = lax.rem(line + far, lines)
                with jax.named_scope("wait_s%d" % far):
                    wait_for(tiles, MATES * (planes - (step == 0)), sems.at[z])
                for p in range(planes):
                    block = pl.ds((p * lines + z) * MATES, MATES)
                    to_sibling(tiles.at[block], tiles.at[block], sems.at[z])
            with jax.named_scope("sort0"):
                sort_shares(tiles, fars, step == 0, step == len(near_and_rest) - 1)

    def sort_all():
        with jax.named_scope("sorta"):
            sort_shares(adj, near_first, True, True)

    def first_layer():
        with jax.named_scope("forward1"):
            to_clans(outgoing, adj_two, two_sem.at[line], group, offsets[:-1])
            adj_two[clan_tiles] = outgoing[...]
            to_mates(outgoing, landed, land_sem)

    @pl.when(group == top)
    def _():
        wait_rows(0)
        receive(adj, rows_all, adj_sem, True, outgoing)
        first_layer()
        relay_rows(rows_two, 1)
        start_fields()
        build_fwd()
        wait_rows(1)
        pl.semaphore_signal(go_sem, inc=1, device_id=(sibling, me), device_id_type=MESH)
        receive(adj_two, rows_two, two_sem, True, outgoing_two)
        with jax.named_scope("forward2"):
            to_clans(outgoing_two, adj, adj_sem.at[line], helper, offsets)
            to_sibling(adj_two, adj, hand_sem.at[1])
            to_sibling_mates(outgoing_two, landed, land_sem)
        relay_fields()
        build_adj()
        sort_all()

    with jax.named_scope("wait_f"):
        wait_for(fwd, peers - MATES, fwd_sem)
    with jax.named_scope("sortf"):
        for k in range(steps):
            count = depth // rows
            flat_fwd = unpack(fwd[pl.ds(k * count, count)])
            stretched[pl.ds(k * depth, depth), :] = flat_fwd
        sign = jnp.where(in_slice < slice_b, 1.0, -1.0)
        quads = chunk // band

        @pl.loop(0, harm // chunk)
        def _(r):
            at = pl.ds(pl.multiple_of(r * chunk, chunk), chunk)
            total = jnp.zeros((chunk, cols), F32)
            for k in range(steps):
                total += jnp.dot(
                    hot_fwd[at, pl.ds(k * depth, depth)], stretched[pl.ds(k * depth, depth), :],
                    preferred_element_type=F32,
                )
            real = total * sign
            imag = pltpu.roll(total, slice_b, 1)
            for pair in range(quads // 2):
                lo, mid, hi = 2 * pair * band, (2 * pair + 1) * band, (2 * pair + 2) * band
                upper = jnp.where(lane < cols // 2, real[lo:mid], real[mid:hi])
                lower = jnp.where(lane < cols // 2, imag[lo:mid], imag[mid:hi])
                both = jnp.concatenate([upper, lower], axis=0)
                factor[r, :, pl.ds(pair * cols, cols)] = both.astype(BF16)

    def correlate(made, into):
        with jax.named_scope("gram"):
            quad = chunk // band
            view = (MATES + 2) * band
            gram = jnp.zeros((2 * band, view), F32)
            for n in range(harm // chunk):
                start = (MATES * clan + quad * n) * band
                window = []
                for k in range(quad):
                    buffer = shifted if k % 2 else lined
                    at = pl.ds(pl.multiple_of(start + (k - k % 2) * band, 2 * band), view)
                    window.append(buffer[:, at])
                gram += jnp.dot(made[n], jnp.concatenate(window, axis=0), preferred_element_type=F32)
            for m in range(MATES):
                if m % 2:
                    both = gram[:, (m - 1) * band : (m + 3) * band]
                    turned = pltpu.roll(both, 2 * band + 1, 1, stride=1, stride_axis=0)[:, : 2 * band]
                else:
                    both = gram[:, m * band : (m + 2) * band]
                    turned = pltpu.roll(both, band + 1, 1, stride=1, stride_axis=0)
                real = jnp.sum(turned[:band], axis=0, keepdims=True)
                imag = jnp.sum(turned[band:], axis=0, keepdims=True)
                into[m] = jnp.where(lane < band, real, imag)

    @pl.when(group == 0)
    def _():
        to_sibling(factor, factor_two, hand_sem.at[1])
        wait_rows(0)
        receive(adj_two, rows_all, two_sem, False, outgoing)
        to_mates(outgoing, landed, land_sem)

    @pl.when(group == top - 1)
    def _():
        with jax.named_scope("wait_adj"):
            wait_for(adj, peers, hand_sem.at[1])
        sort_all()

    @pl.when(group == helper)
    def _():
        wait_rows(0)
        receive(adj, rows_all, adj_sem, False, outgoing)
        first_layer()
        sort_all()

    @pl.when(group > 0)
    def _():
        correlate(factor, partial)
        to_mates(partial, gathered, part_sem)

    @pl.when(group == helper)
    def _():
        with jax.named_scope("wait_factor"):
            wait_for(factor_two, harm // chunk, hand_sem.at[1])
        receive_sorted(adj_two, two_sem)
        correlate(factor_two, partial_two)
        to_sibling_mates(partial_two, gathered, part_sem)

    with jax.named_scope("land"):
        @pl.when(group != top - 1)
        def _():
            wait_for(landed, MATES - 1, land_sem)

        @pl.when(group == top - 1)
        def _():
            wait_for(landed, MATES, land_sem)

        pieces = [landed[m].astype(F32) for m in range(MATES)]
        for plane in range(2):
            for upper in range(2):
                where = 2 * upper + plane
                tile = None
                for m in range(MATES):
                    shift = (m - where) * slice_b % cols
                    moved = pltpu.roll(pieces[m], shift, 1) if shift else pieces[m]
                    tile = moved if m == 0 else jnp.where(lane < m * slice_b, tile, moved)
                bound_ref[0, plane, pl.ds(upper * half, half), :] = tile.astype(BF16)

    with jax.named_scope("sum"):
        @pl.when(group > 0)
        def _():
            wait_for(gathered, MATES - 1, part_sem)

        @pl.when(group == 0)
        def _():
            wait_for(gathered, MATES, part_sem)

        total = gathered[0]
        for m in range(1, MATES):
            total = total + gathered[m]
        total = total * scale
        grads_ref[0, 0:1, :] = total[:, :band]
        grads_ref[0, 1:2, :] = total[:, band:]

    with jax.named_scope("drain"):
        wait_for(stage_fld, MATES - 1, send_sem)
        wait_for(fwd, peers - MATES, send_sem)

        @pl.when(group != top - 1)
        def _():
            wait_for(rows_all, 3, send_sem)
            wait_for(landed, MATES - 1, send_sem)

        @pl.when(chain)
        def _():
            wait_for(stage_src, MATES - 1, send_sem)
            wait_for(adj, peers - MATES, send_sem)
            wait_for(adj, peers, send_sem)

        @pl.when(group > 0)
        def _():
            wait_for(gathered, MATES - 1, send_sem)

        @pl.when(group == top)
        def _():
            wait_for(rows_all, 3, send_sem)
            wait_for(landed, MATES, send_sem)
            wait_for(adj, MATES * len(near), send_sem)
            wait_for(adj, peers, send_sem)

        @pl.when(group == top - 1)
        def _():
            wait_for(rows_all, 1, send_sem)

        @pl.when(group == helper)
        def _():
            wait_for(adj, MATES * len(far), send_sem)
            wait_for(gathered, MATES, send_sem)

        @pl.when(group == 0)
        def _():
            wait_for(factor, harm // chunk, send_sem)


def put_out(grads_ref, bound_ref, grads_hbm, bound_hbm, sems):
    copies = [
        pltpu.make_async_copy(bound_ref, bound_hbm, sems.at[0]),
        pltpu.make_async_copy(grads_ref, grads_hbm, sems.at[1]),
    ]
    for copy in copies:
        copy.start()
    for copy in copies:
        copy.wait()


def solution(mesh):
    layers, peers = mesh.shape["layer"], mesh.shape["harm"]

    def per_device(source, transfer, fields, orders):
        rows, cols = source.shape[1], source.shape[2]
        harm = rows * peers
        band = 2 * rows
        chunk = min(256, harm)
        vmem = pl.BlockSpec(memory_space=pltpu.VMEM)
        hbm = pl.BlockSpec(memory_space=pltpu.HBM)
        tile = (rows // 2, cols)
        made = pl.pallas_call(
            functools.partial(kernel, layers, peers, 1.0 / math.sqrt(harm * cols)),
            out_shape=(
                jax.ShapeDtypeStruct((1, 2, band), F32),
                jax.ShapeDtypeStruct((1, 2, rows, cols), BF16),
            ),
            in_specs=[hbm] * 4,
            out_specs=(vmem, vmem),
            scratch_shapes=[
                pltpu.VMEM((2, rows, cols), BF16),
                pltpu.VMEM((2, rows, cols), BF16),
                pltpu.VMEM((1, harm), jnp.int32),
                pltpu.VMEM((2, rows, harm), BF16),
                *[pltpu.VMEM((MATES, 2, rows, harm), BF16)] * 2,
                *[pltpu.VMEM((peers, *tile), BF16)] * 3,
                pltpu.VMEM((harm, cols), BF16),
                pltpu.VMEM((harm, cols), F32),
                pltpu.VMEM((harm, harm), BF16),
                pltpu.VMEM((harm, harm + 2 * cols), BF16),
                pltpu.VMEM((2 * cols // MATES, 3 * harm), BF16),
                pltpu.VMEM((2 * cols // MATES, 3 * harm), BF16),
                *[pltpu.VMEM((harm // chunk, 2 * band, chunk // band * 2 * (cols // MATES)), BF16)] * 2,
                *[pltpu.VMEM((MATES, *tile), BF16)] * 7,
                *[pltpu.VMEM((MATES, 1, cols), F32)] * 3,
                pltpu.VMEM((2 * cols // MATES, harm + 2 * cols), F32),
                pltpu.SemaphoreType.DMA((4,)),
                pltpu.SemaphoreType.DMA,
                pltpu.SemaphoreType.DMA((6,)),
                pltpu.SemaphoreType.DMA((LINES,)),
                pltpu.SemaphoreType.DMA((LINES,)),
                pltpu.SemaphoreType.DMA((2,)),
                pltpu.SemaphoreType.DMA,
                pltpu.SemaphoreType.DMA((2,)),
                pltpu.SemaphoreType.DMA,
                pltpu.SemaphoreType.DMA,
                *[pltpu.SemaphoreType.REGULAR] * 4,
            ],
            compiler_params=pltpu.CompilerParams(
                collective_id=0, has_side_effects=True, vmem_limit_bytes=44 * 1024 * 1024
            ),
        )(
            *(
                pltpu.with_memory_space_constraint(value, pltpu.HBM)
                for value in (source, transfer, fields, orders.reshape(1, harm))
            )
        )
        return pl.pallas_call(
            put_out,
            out_shape=[jax.ShapeDtypeStruct(value.shape, value.dtype) for value in made],
            in_specs=[vmem] * 2,
            out_specs=[hbm] * 2,
            scratch_shapes=[pltpu.SemaphoreType.DMA((2,))],
            compiler_params=pltpu.CompilerParams(vmem_limit_bytes=1 << 20),
        )(*(pltpu.with_memory_space_constraint(value, pltpu.VMEM) for value in made))

    return jax.shard_map(
        per_device,
        mesh=mesh,
        in_specs=(
            P(None, "harm", None),
            P("layer", None, "harm", None),
            P("layer", None, "harm", None),
            P(),
        ),
        out_specs=(P("layer", None, "harm"), P("layer", None, "harm", None)),
        check_vma=False,
    )
```

```python
import functools
import math

import jax
import jax.numpy as jnp
from jax import lax
from jax.experimental import pallas as pl
from jax.experimental.pallas import tpu as pltpu
from jax.sharding import PartitionSpec as P

MESH = pl.DeviceIdType.MESH
F32 = jnp.float32
BF16 = jnp.bfloat16
MATES = 4
LINES = 4


def kernel(
    layers, peers, scale,
    source_hbm, transfer_hbm, fields_hbm, orders_hbm, grads_ref, bound_ref,
    source, fields, orders, rows_own, rows_all, rows_two, adj, adj_two, fwd, stretched, column, hot_fwd, hot_adj, lined, shifted, factor, factor_two,
    packed_src, packed_fld, stage_src, stage_fld, outgoing, outgoing_two, landed, partial, partial_two, gathered, sorting,
    load_sem, send_sem, rows_sem, adj_sem, two_sem, hand_sem, fwd_sem, stage_sem, land_sem, part_sem, clear_sem, line_sem, plane_sem, go_sem,
):
    group = lax.axis_index("layer")
    me = lax.axis_index("harm")
    mate = me % MATES
    clan = me // MATES
    clans = peers // MATES
    lines = min(LINES, clans)
    planes = clans // lines
    line = clan % lines
    plane_at = clan // lines
    rows = source.shape[1]
    half = rows // 2
    cols = source.shape[2]
    slice_b = cols // MATES
    harm = rows * peers
    band = 2 * rows
    depth = min(256, harm)
    steps = harm // depth
    top = layers - 1
    helper = top - 2
    chain = (group == top) | (group == helper)
    sibling = jnp.where(chain, jnp.maximum(group - 1, 0), jnp.minimum(group + 1, top))
    far_line = lines // 2
    clan_rows = MATES * rows
    share = planes * clan_rows

    loads = [
        pltpu.make_async_copy(transfer_hbm.at[0], rows_own, load_sem.at[3]),
        pltpu.make_async_copy(source_hbm, source, load_sem.at[0]),
        pltpu.make_async_copy(fields_hbm.at[0], fields, load_sem.at[2]),
        pltpu.make_async_copy(orders_hbm, orders, load_sem.at[1]),
    ]
    barrier = pltpu.get_barrier_semaphore()

    def mate_index(j):
        return clan * MATES + lax.rem(mate + j, MATES)

    def place(plane, line_of):
        return (plane * lines + line_of) * MATES + mate

    def clan_index(far_line, far_plane):
        return place(lax.rem(plane_at + far_plane, planes), lax.rem(line + far_line, lines))

    def by_distance(size):
        return sorted(range(size), key=lambda d: -min(d, size - d))

    offsets = [(a, b) for a in by_distance(lines) for b in by_distance(planes)]

    near_lines = [place(plane_at, lax.rem(line + far, lines)) for far in (1, lines - 1)]
    near_planes = [place(lax.rem(plane_at + far, planes), line) for far in (2, 1, 3)]

    with jax.named_scope("signal"):
        for index in near_lines + near_planes + [mate_index(j) for j in (2, 1, 3)]:
            pl.semaphore_signal(barrier, inc=1, device_id=(group, index), device_id_type=MESH)

        @pl.when(chain)
        def _():
            pl.semaphore_signal(barrier, inc=1, device_id=(sibling, me), device_id_type=MESH)

        @pl.when(group == top)
        def _():
            pl.semaphore_signal(barrier, inc=1, device_id=(helper, me), device_id_type=MESH)
            pl.semaphore_signal(
                barrier, inc=1, device_id=(helper, clan_index(far_line, 0)), device_id_type=MESH
            )

    for load in loads:
        load.start()

    lane = lax.broadcasted_iota(jnp.int32, (1, cols), 1)
    in_slice = lax.rem(lane, 2 * slice_b)

    def pack(block, into):
        value = block[...].astype(F32)
        for m in range(MATES):
            parts = []
            for where in range(4):
                plane, upper = where % 2, where // 2
                piece = value[plane, upper * half : (upper + 1) * half, :]
                shift = (where - m) * slice_b % cols
                parts.append(pltpu.roll(piece, shift, 1) if shift else piece)
            tile = parts[3]
            for where in range(2, -1, -1):
                tile = jnp.where(lane < (where + 1) * slice_b, parts[where], tile)
            into[m] = tile.astype(BF16)

    border = harm - cols
    wide = harm + 2 * cols
    chunk = min(256, harm)

    with jax.named_scope("pack"):
        loads[1].wait()
        pack(source, packed_src)
        loads[2].wait()
        pack(fields, packed_fld)
        for buffer in (lined, shifted):
            buffer[:, pl.ds(0, border)] = jnp.zeros((2 * slice_b, border), BF16)
            buffer[:, pl.ds(border + wide, border)] = jnp.zeros((2 * slice_b, border), BF16)
        loads[3].wait()

    def arrange():
        value = rows_own[...].reshape(2 * rows, harm)
        count = harm // clan_rows
        stacked = jnp.concatenate(
            [value[:, k * clan_rows : (k + 1) * clan_rows] for k in range(count)], axis=0
        )
        at = lax.broadcasted_iota(jnp.int32, (clan_rows, 2 * clan_rows), 0)
        to = lax.broadcasted_iota(jnp.int32, (clan_rows, 2 * clan_rows), 1)
        inside = to % clan_rows
        upper = (inside // (clan_rows // 2) + to // clan_rows) % 2
        origin = inside % (clan_rows // 2) // half * rows + upper * half + inside % half
        order = jnp.where(at == origin, 1.0, 0.0).astype(BF16)
        moved = jnp.dot(stacked, order, preferred_element_type=F32)
        moved = moved.reshape(count, 2, rows, 2 * clan_rows)
        for z in range(lines):
            for pair in range(planes // 2):
                first = moved[2 * pair * lines + z]
                second = moved[(2 * pair + 1) * lines + z]
                lower = jnp.where(lane < cols // 2, first[:, :, :clan_rows], second[:, :, clan_rows:])
                upper = jnp.where(lane < cols // 2, first[:, :, clan_rows:], second[:, :, :clan_rows])
                start = z * share + pair * clan_rows
                rows_all[mate, :, :, pl.ds(start, clan_rows)] = lower.astype(BF16)
                rows_all[mate, :, :, pl.ds(start + share // 2, clan_rows)] = upper.astype(BF16)

    with jax.named_scope("arrange"):
        loads[0].wait()
        arrange()

    def build_fwd():
        with jax.named_scope("hotf"):

            @pl.loop(0, harm // chunk)
            def _(r):
                index = lax.broadcasted_iota(jnp.int32, (chunk, depth), 0)
                order = r * chunk + (index // band) * band + (band - 1) - index % band
                for k in range(steps):
                    hit = orders[:, pl.ds(k * depth, depth)] == order
                    hot_fwd[
                        pl.ds(pl.multiple_of(r * chunk, chunk), chunk), pl.ds(k * depth, depth)
                    ] = jnp.where(hit, 1.0, 0.0).astype(BF16)

    def build_adj():
        with jax.named_scope("hota"):
            for k in range(harm // cols):
                row = orders[:, pl.ds(k * cols, cols)].astype(F32)
                column[pl.ds(k * cols, cols), :] = jnp.broadcast_to(row, (cols, cols)).T

            @pl.loop(0, peers)
            def _(tile):
                owner = tile // MATES
                spot = (owner // lines) * MATES + tile % MATES
                for upper in range(2):
                    order = column[pl.ds(pl.multiple_of(tile * rows + upper * half, half), half), :]
                    row = (owner % lines) * share + upper * (share // 2) + spot * half
                    row = pl.ds(pl.multiple_of(row, half), half)
                    for k in range(wide // cols):
                        want = (lane + (k * cols - cols + 1)).astype(F32)
                        hot_adj[row, pl.ds(k * cols, cols)] = jnp.where(order == want, 1.0, 0.0).astype(BF16)

    with jax.named_scope("barrier"):

        close = len(near_lines) + len(near_planes) + MATES - 1

        @pl.when(jnp.logical_not(chain))
        def _():
            pl.semaphore_wait(barrier, close + 1)

        @pl.when(group == helper)
        def _():
            pl.semaphore_wait(barrier, close + 2)

        @pl.when(group == top)
        def _():
            pl.semaphore_wait(barrier, close)

        for index in near_planes:
            pl.semaphore_signal(plane_sem, inc=1, device_id=(group, index), device_id_type=MESH)

    def near_here():
        with jax.named_scope("near"):
            pl.semaphore_wait(plane_sem, len(near_planes))
            for index in near_lines:
                pl.semaphore_signal(line_sem, inc=1, device_id=(group, index), device_id_type=MESH)

    def all_here():
        with jax.named_scope("here"):
            pl.semaphore_wait(line_sem, len(near_lines))

            @pl.when(jnp.logical_not(chain))
            def _():
                pl.semaphore_signal(clear_sem, inc=1, device_id=(sibling, me), device_id_type=MESH)

            @pl.when(group == helper)
            def _():
                pl.semaphore_signal(clear_sem, inc=1, device_id=(top, me), device_id_type=MESH)

    def remote(src, dst, arrived, target, index):
        return pltpu.make_async_remote_copy(
            src_ref=src, dst_ref=dst, send_sem=send_sem, recv_sem=arrived,
            device_id=(target, index), device_id_type=MESH,
        )

    def wait_for(buffer, count, sem):
        part_of = buffer.at[pl.ds(0, count)]
        pltpu.make_async_copy(part_of, part_of, sem).wait()

    def to_mates(tiles, dst, arrived):
        for j in (2, 1, 3):
            other = lax.rem(mate + j, MATES)
            remote(
                tiles.at[other], dst.at[mate], arrived, group, clan * MATES + other
            ).start()
        dst[mate] = tiles[mate]

    clan_tiles = pl.ds(clan * MATES, MATES)

    def to_clans(tiles, dst, arrived, target, to):
        for a, b in to:
            remote(tiles, dst.at[clan_tiles], arrived, target, clan_index(a, b)).start()

    right, left = mate_index(1), mate_index(MATES - 1)
    from_left, from_right = lax.rem(mate + MATES - 1, MATES), lax.rem(mate + 1, MATES)

    def start_rows(buffer, turn):
        for first in (0, 1):
            to_right = buffer.at[mate, first]
            to_left = buffer.at[mate, 1 - first]
            for block, to, sem in ((to_right, right, 0), (to_left, left, 1)):
                remote(block, block, rows_sem.at[3 * turn + (2 if first else sem)], group, to).start()

    def wait_half(turn, sem):
        wait_for(rows_all.at[0], 1, rows_sem.at[3 * turn + sem])

    def relay_rows(buffer, turn):
        with jax.named_scope("relay_t%d" % turn):
            wait_half(turn, 0)
            block = buffer.at[from_left, 0]
            remote(block, block, rows_sem.at[3 * turn + 2], group, right).start()
            wait_half(turn, 1)
            block = buffer.at[from_right, 1]
            remote(block, block, rows_sem.at[3 * turn + 2], group, left).start()

    def wait_rows(turn):
        with jax.named_scope("wait_t%d" % turn):
            wait_for(rows_all, 2, rows_sem.at[3 * turn + 2])

    def to_sibling(src, dst, arrived):
        remote(src, dst, arrived, sibling, me).start()

    def to_sibling_mates(tiles, dst, arrived):
        for j in (2, 1, 3, 0):
            other = lax.rem(mate + j, MATES)
            remote(
                tiles.at[other], dst.at[mate], arrived, sibling, clan * MATES + other
            ).start()

    def start_fields():
        to_mates(packed_fld, stage_fld, stage_sem.at[0])

    def relay_fields():
        with jax.named_scope("relay_f"):
            wait_for(stage_fld, MATES - 1, stage_sem.at[0])
            to_clans(stage_fld, fwd, fwd_sem, group, offsets[:-1])
            fwd[clan_tiles] = stage_fld[...]

    with jax.named_scope("spread"):

        near = [offset for offset in offsets[:-1] if offset[0] != far_line]
        far = [offset for offset in offsets if offset[0] == far_line]

        def relay_source(to):
            with jax.named_scope("relay_s"):
                wait_for(stage_src, MATES - 1, stage_sem.at[1])
                to_clans(stage_src, adj, adj_sem.at[line], top, to)

        @pl.when(group == top)
        def _():
            to_mates(packed_src, stage_src, stage_sem.at[1])
            start_rows(rows_all, 0)
            near_here()
            relay_source(near)
            adj[clan_tiles] = stage_src[...]
            relay_rows(rows_all, 0)
            wait_for(rows_all, 1, hand_sem.at[0])
            start_rows(rows_two, 1)
            all_here()
            pl.semaphore_wait(clear_sem, 2)

        @pl.when(group == helper)
        def _():
            to_mates(packed_src, stage_src, stage_sem.at[1])
            near_here()
            relay_source(far)
            all_here()
            start_fields()
            start_rows(rows_all, 0)
            build_fwd()
            relay_fields()
            relay_rows(rows_all, 0)
            build_adj()
            pl.semaphore_wait(clear_sem, 1)
            pl.semaphore_signal(go_sem, inc=1, device_id=(sibling, me), device_id_type=MESH)

        @pl.when(jnp.logical_not(chain))
        def _():
            @pl.when(group == top - 1)
            def _():
                to_sibling(rows_all.at[mate], rows_two.at[mate], hand_sem.at[0])

            near_here()
            all_here()
            start_fields()

            @pl.when(group == 0)
            def _():
                start_rows(rows_all, 0)

            build_fwd()

            @pl.when(group == top - 1)
            def _():
                build_adj()

            @pl.when(group == 0)
            def _():
                relay_rows(rows_all, 0)

            pl.semaphore_wait(go_sem, 1)
            relay_fields()

    def unpack(tiles):
        count = tiles.shape[0]
        value = tiles.astype(F32)
        turned = pltpu.roll(value.reshape(count * half, cols), cols // 2, 1).reshape(value.shape)
        lower = jnp.where(lane < cols // 2, value, turned)
        upper = jnp.where(lane < cols // 2, turned, value)
        return jnp.concatenate([lower, upper], axis=1).reshape(count * rows, cols).astype(BF16)

    def share_tiles(tiles, z):
        return jnp.concatenate(
            [tiles[pl.ds((p * lines + z) * MATES, MATES)].reshape(MATES * half, cols) for p in range(planes)],
            axis=0,
        )

    def sort_shares(tiles, fars, first, last):
        shares = []
        for far in fars:
            z = lax.rem(line + far, lines)
            turned = share_tiles(tiles, z).astype(F32).T.astype(BF16)
            left = jnp.concatenate([turned[: cols // 2], turned[cols // 2 :]], axis=1)
            shares.append((left, pl.ds(pl.multiple_of(z * share, share), share)))
        left = jnp.concatenate([piece for piece, _ in shares], axis=1)
        span = 3 * depth if wide % (3 * depth) == 0 else wide
        tail = None
        for k in reversed(range(wide // span)):
            here = pl.ds(k * span, span)
            hot = jnp.concatenate([hot_adj[at, here] for _, at in shares], axis=0)
            total = jnp.dot(left, hot, preferred_element_type=F32)
            if not first:
                total += sorting[:, here]
            if not last:
                sorting[:, here] = total
                continue
            lined[:, pl.ds(border + k * span, span)] = total.astype(BF16)
            pieces = [
                pltpu.roll(total[:, i * cols : (i + 1) * cols], cols // 2, 1) for i in range(span // cols)
            ]
            pieces.append(jnp.zeros_like(pieces[0]) if tail is None else tail)
            tail = pieces[0]
            for i in range(span // cols):
                shifted[:, pl.ds(border + k * span + i * cols, cols)] = jnp.where(
                    lane < cols // 2, pieces[i], pieces[i + 1]
                ).astype(BF16)
        if last:
            shifted[:, pl.ds(border - cols, cols)] = jnp.where(lane < cols // 2, 0.0, tail).astype(BF16)

    near_first = by_distance(lines)[::-1]
    by_arrival = [near_first[:1], near_first[1:-1], near_first[-1:]]

    def receive(tiles, block_rows, sems, own_there, out):
        lower = jnp.zeros((MATES * 2 * rows, cols), F32)
        upper = jnp.zeros((MATES * 2 * rows, cols), F32)
        for step, fars in enumerate(by_arrival):
            spots = [lax.rem(line + far, lines) for far in fars]
            with jax.named_scope("wait_a%d" % step):
                for z in spots:
                    wait_for(tiles, MATES * (planes - (own_there and step == 0)), sems.at[z])
            with jax.named_scope("propagate"):
                packed = jnp.concatenate([share_tiles(tiles, z) for z in spots], axis=0)

                def product(upper_half):
                    starts = [z * share + upper_half * (share // 2) for z in spots]
                    matrix = jnp.concatenate(
                        [
                            block_rows[
                                :, :, :, pl.ds(pl.multiple_of(start, share // 2), share // 2)
                            ].reshape(MATES * 2 * rows, share // 2)
                            for start in starts
                        ],
                        axis=1,
                    )
                    return jnp.dot(matrix, packed, preferred_element_type=F32)

                lower += product(0)
                upper += product(1)
            if step == len(by_arrival) - 1:
                mixed = jnp.where(lane < cols // 2, lower, upper).reshape(MATES, 2, rows, cols)
                head, rest = mixed[:, :, :half], mixed[:, :, half:]
                here = jnp.where(lane < cols // 2, head, rest)
                there = jnp.where(lane < cols // 2, rest, head).reshape(MATES * 2 * half, cols)
                total = here + pltpu.roll(there, cols // 2, 1).reshape(MATES, 2, half, cols)
                cross = total[:, 1].reshape(MATES * half, cols)
                cross = jnp.where(
                    in_slice < slice_b,
                    -pltpu.roll(cross, cols - slice_b, 1),
                    pltpu.roll(cross, slice_b, 1),
                )
                out[...] = (total[:, 0] + cross.reshape(MATES, half, cols)).astype(BF16)

    def receive_sorted(tiles, sems):
        sorts = [near_first[:1], near_first[1:2], near_first[2:]]
        for step, fars in enumerate(by_arrival):
            for far in fars:
                z = lax.rem(line + far, lines)
                with jax.named_scope("wait_s%d" % far):
                    wait_for(tiles, MATES * (planes - (step == 0)), sems.at[z])
                for p in range(planes):
                    block = pl.ds((p * lines + z) * MATES, MATES)
                    to_sibling(tiles.at[block], tiles.at[block], sems.at[z])
            with jax.named_scope("sort0"):
                sort_shares(tiles, sorts[step], step == 0, step == len(by_arrival) - 1)

    def sort_all():
        with jax.named_scope("sorta"):
            sort_shares(adj, near_first, True, True)

    def first_layer():
        with jax.named_scope("forward1"):
            to_clans(outgoing, adj_two, two_sem.at[line], group, offsets[:-1])
            adj_two[clan_tiles] = outgoing[...]
            to_mates(outgoing, landed, land_sem)

    @pl.when(group == top)
    def _():
        wait_rows(0)
        receive(adj, rows_all, adj_sem, True, outgoing)
        first_layer()
        relay_rows(rows_two, 1)
        start_fields()
        build_fwd()
        wait_rows(1)
        pl.semaphore_signal(go_sem, inc=1, device_id=(sibling, me), device_id_type=MESH)
        receive(adj_two, rows_two, two_sem, True, outgoing_two)
        with jax.named_scope("forward2"):
            to_clans(outgoing_two, adj, adj_sem.at[line], helper, offsets)
            to_sibling(adj_two, adj, hand_sem.at[1])
            to_sibling_mates(outgoing_two, landed, land_sem)
        relay_fields()
        build_adj()
        sort_all()

    with jax.named_scope("wait_f"):
        wait_for(fwd, peers - MATES, fwd_sem)
    with jax.named_scope("sortf"):
        for k in range(steps):
            count = depth // rows
            flat_fwd = unpack(fwd[pl.ds(k * count, count)])
            stretched[pl.ds(k * depth, depth), :] = flat_fwd
        sign = jnp.where(in_slice < slice_b, 1.0, -1.0)
        quads = chunk // band

        @pl.loop(0, harm // chunk)
        def _(r):
            at = pl.ds(pl.multiple_of(r * chunk, chunk), chunk)
            total = jnp.dot(hot_fwd[at, :], stretched[...], preferred_element_type=F32)
            real = total * sign
            imag = pltpu.roll(total, slice_b, 1)
            for pair in range(quads // 2):
                lo, mid, hi = 2 * pair * band, (2 * pair + 1) * band, (2 * pair + 2) * band
                upper = jnp.where(lane < cols // 2, real[lo:mid], real[mid:hi])
                lower = jnp.where(lane < cols // 2, imag[lo:mid], imag[mid:hi])
                both = jnp.concatenate([upper, lower], axis=0)
                factor[r, :, pl.ds(pair * cols, cols)] = both.astype(BF16)

    def correlate(made, into):
        with jax.named_scope("gram"):
            quad = chunk // band
            view = (MATES + 2) * band
            window = []
            for n in range(harm // chunk):
                start = (MATES * clan + quad * n) * band
                for k in range(quad):
                    buffer = shifted if k % 2 else lined
                    at = pl.ds(pl.multiple_of(start + (k - k % 2) * band, 2 * band), view)
                    window.append(buffer[:, at])
            left = jnp.concatenate([made[n] for n in range(harm // chunk)], axis=1)
            gram = jnp.dot(left, jnp.concatenate(window, axis=0), preferred_element_type=F32)
            for m in range(MATES):
                if m % 2:
                    both = gram[:, (m - 1) * band : (m + 3) * band]
                    turned = pltpu.roll(both, 2 * band + 1, 1, stride=1, stride_axis=0)[:, : 2 * band]
                else:
                    both = gram[:, m * band : (m + 2) * band]
                    turned = pltpu.roll(both, band + 1, 1, stride=1, stride_axis=0)
                real = jnp.sum(turned[:band], axis=0, keepdims=True)
                imag = jnp.sum(turned[band:], axis=0, keepdims=True)
                into[m] = jnp.where(lane < band, real, imag)

    @pl.when(group == 0)
    def _():
        to_sibling(factor, factor_two, hand_sem.at[1])
        wait_rows(0)
        receive(adj_two, rows_all, two_sem, False, outgoing)
        to_mates(outgoing, landed, land_sem)

    @pl.when(group == top - 1)
    def _():
        with jax.named_scope("wait_adj"):
            wait_for(adj, peers, hand_sem.at[1])
        sort_all()

    @pl.when(group == helper)
    def _():
        wait_rows(0)
        receive(adj, rows_all, adj_sem, False, outgoing)
        first_layer()
        sort_all()

    @pl.when(group > 0)
    def _():
        correlate(factor, partial)
        to_mates(partial, gathered, part_sem)

    @pl.when(group == helper)
    def _():
        with jax.named_scope("wait_factor"):
            wait_for(factor_two, harm // chunk, hand_sem.at[1])
        receive_sorted(adj_two, two_sem)
        correlate(factor_two, partial_two)
        to_sibling_mates(partial_two, gathered, part_sem)

    with jax.named_scope("land"):
        @pl.when(group != top - 1)
        def _():
            wait_for(landed, MATES - 1, land_sem)

        @pl.when(group == top - 1)
        def _():
            wait_for(landed, MATES, land_sem)

        pieces = [landed[m].astype(F32) for m in range(MATES)]
        for plane in range(2):
            for upper in range(2):
                where = 2 * upper + plane
                tile = None
                for m in range(MATES):
                    shift = (m - where) * slice_b % cols
                    moved = pltpu.roll(pieces[m], shift, 1) if shift else pieces[m]
                    tile = moved if m == 0 else jnp.where(lane < m * slice_b, tile, moved)
                bound_ref[0, plane, pl.ds(upper * half, half), :] = tile.astype(BF16)

    with jax.named_scope("sum"):
        @pl.when(group > 0)
        def _():
            wait_for(gathered, MATES - 1, part_sem)

        @pl.when(group == 0)
        def _():
            wait_for(gathered, MATES, part_sem)

        total = gathered[0]
        for m in range(1, MATES):
            total = total + gathered[m]
        total = total * scale
        grads_ref[0, 0:1, :] = total[:, :band]
        grads_ref[0, 1:2, :] = total[:, band:]

    with jax.named_scope("drain"):
        wait_for(stage_fld, MATES - 1, send_sem)
        wait_for(fwd, peers - MATES, send_sem)

        @pl.when(group != top - 1)
        def _():
            wait_for(rows_all, 3, send_sem)
            wait_for(landed, MATES - 1, send_sem)

        @pl.when(chain)
        def _():
            wait_for(stage_src, MATES - 1, send_sem)
            wait_for(adj, peers - MATES, send_sem)
            wait_for(adj, peers, send_sem)

        @pl.when(group > 0)
        def _():
            wait_for(gathered, MATES - 1, send_sem)

        @pl.when(group == top)
        def _():
            wait_for(rows_all, 3, send_sem)
            wait_for(landed, MATES, send_sem)
            wait_for(adj, MATES * len(near), send_sem)
            wait_for(adj, peers, send_sem)

        @pl.when(group == top - 1)
        def _():
            wait_for(rows_all, 1, send_sem)

        @pl.when(group == helper)
        def _():
            wait_for(adj, MATES * len(far), send_sem)
            wait_for(gathered, MATES, send_sem)

        @pl.when(group == 0)
        def _():
            wait_for(factor, harm // chunk, send_sem)


def put_out(grads_ref, bound_ref, grads_hbm, bound_hbm, sems):
    copies = [
        pltpu.make_async_copy(bound_ref, bound_hbm, sems.at[0]),
        pltpu.make_async_copy(grads_ref, grads_hbm, sems.at[1]),
    ]
    for copy in copies:
        copy.start()
    for copy in copies:
        copy.wait()


def solution(mesh):
    layers, peers = mesh.shape["layer"], mesh.shape["harm"]

    def per_device(source, transfer, fields, orders):
        rows, cols = source.shape[1], source.shape[2]
        harm = rows * peers
        band = 2 * rows
        chunk = min(256, harm)
        vmem = pl.BlockSpec(memory_space=pltpu.VMEM)
        hbm = pl.BlockSpec(memory_space=pltpu.HBM)
        tile = (rows // 2, cols)
        made = pl.pallas_call(
            functools.partial(kernel, layers, peers, 1.0 / math.sqrt(harm * cols)),
            out_shape=(
                jax.ShapeDtypeStruct((1, 2, band), F32),
                jax.ShapeDtypeStruct((1, 2, rows, cols), BF16),
            ),
            in_specs=[hbm] * 4,
            out_specs=(vmem, vmem),
            scratch_shapes=[
                pltpu.VMEM((2, rows, cols), BF16),
                pltpu.VMEM((2, rows, cols), BF16),
                pltpu.VMEM((1, harm), jnp.int32),
                pltpu.VMEM((2, rows, harm), BF16),
                *[pltpu.VMEM((MATES, 2, rows, harm), BF16)] * 2,
                *[pltpu.VMEM((peers, *tile), BF16)] * 3,
                pltpu.VMEM((harm, cols), BF16),
                pltpu.VMEM((harm, cols), F32),
                pltpu.VMEM((harm, harm), BF16),
                pltpu.VMEM((harm, harm + 2 * cols), BF16),
                pltpu.VMEM((2 * cols // MATES, 3 * harm), BF16),
                pltpu.VMEM((2 * cols // MATES, 3 * harm), BF16),
                *[pltpu.VMEM((harm // chunk, 2 * band, chunk // band * 2 * (cols // MATES)), BF16)] * 2,
                *[pltpu.VMEM((MATES, *tile), BF16)] * 7,
                *[pltpu.VMEM((MATES, 1, cols), F32)] * 3,
                pltpu.VMEM((2 * cols // MATES, harm + 2 * cols), F32),
                pltpu.SemaphoreType.DMA((4,)),
                pltpu.SemaphoreType.DMA,
                pltpu.SemaphoreType.DMA((6,)),
                pltpu.SemaphoreType.DMA((LINES,)),
                pltpu.SemaphoreType.DMA((LINES,)),
                pltpu.SemaphoreType.DMA((2,)),
                pltpu.SemaphoreType.DMA,
                pltpu.SemaphoreType.DMA((2,)),
                pltpu.SemaphoreType.DMA,
                pltpu.SemaphoreType.DMA,
                *[pltpu.SemaphoreType.REGULAR] * 4,
            ],
            compiler_params=pltpu.CompilerParams(
                collective_id=0, has_side_effects=True, vmem_limit_bytes=44 * 1024 * 1024
            ),
        )(
            *(
                pltpu.with_memory_space_constraint(value, pltpu.HBM)
                for value in (source, transfer, fields, orders.reshape(1, harm))
            )
        )
        return pl.pallas_call(
            put_out,
            out_shape=[jax.ShapeDtypeStruct(value.shape, value.dtype) for value in made],
            in_specs=[vmem] * 2,
            out_specs=[hbm] * 2,
            scratch_shapes=[pltpu.SemaphoreType.DMA((2,))],
            compiler_params=pltpu.CompilerParams(vmem_limit_bytes=1 << 20),
        )(*(pltpu.with_memory_space_constraint(value, pltpu.VMEM) for value in made))

    return jax.shard_map(
        per_device,
        mesh=mesh,
        in_specs=(
            P(None, "harm", None),
            P("layer", None, "harm", None),
            P("layer", None, "harm", None),
            P(),
        ),
        out_specs=(P("layer", None, "harm"), P("layer", None, "harm", None)),
        check_vma=False,
    )
```

```python
import functools
import math

import jax
import jax.numpy as jnp
from jax import lax
from jax.experimental import pallas as pl
from jax.experimental.pallas import tpu as pltpu
from jax.sharding import PartitionSpec as P

MESH = pl.DeviceIdType.MESH
F32 = jnp.float32
BF16 = jnp.bfloat16
MATES = 4
LINES = 4


def kernel(
    layers, peers, scale,
    source_hbm, transfer_hbm, fields_hbm, orders_hbm, grads_ref, bound_ref,
    source, fields, orders, rows_own, rows_all, rows_two, adj, adj_two, fwd, stretched, column, hot_fwd, hot_adj, lined, shifted, factor, factor_two,
    packed_src, packed_fld, stage_src, stage_fld, outgoing, outgoing_two, landed, partial, partial_two, gathered, sorting,
    load_sem, send_sem, rows_sem, adj_sem, two_sem, hand_sem, fwd_sem, stage_sem, land_sem, part_sem, clear_sem, line_sem, plane_sem, go_sem,
):
    group = lax.axis_index("layer")
    me = lax.axis_index("harm")
    mate = me % MATES
    clan = me // MATES
    clans = peers // MATES
    lines = min(LINES, clans)
    planes = clans // lines
    line = clan % lines
    plane_at = clan // lines
    rows = source.shape[1]
    half = rows // 2
    cols = source.shape[2]
    slice_b = cols // MATES
    harm = rows * peers
    band = 2 * rows
    depth = min(256, harm)
    steps = harm // depth
    top = layers - 1
    helper = top - 2
    chain = (group == top) | (group == helper)
    sibling = jnp.where(chain, jnp.maximum(group - 1, 0), jnp.minimum(group + 1, top))
    far_line = lines // 2
    clan_rows = MATES * rows
    share = planes * clan_rows

    loads = [
        pltpu.make_async_copy(transfer_hbm.at[0], rows_own, load_sem.at[3]),
        pltpu.make_async_copy(source_hbm, source, load_sem.at[0]),
        pltpu.make_async_copy(fields_hbm.at[0], fields, load_sem.at[2]),
        pltpu.make_async_copy(orders_hbm, orders, load_sem.at[1]),
    ]
    barrier = pltpu.get_barrier_semaphore()

    def mate_index(j):
        return clan * MATES + lax.rem(mate + j, MATES)

    def place(plane, line_of):
        return (plane * lines + line_of) * MATES + mate

    def clan_index(far_line, far_plane):
        return place(lax.rem(plane_at + far_plane, planes), lax.rem(line + far_line, lines))

    def by_distance(size):
        return sorted(range(size), key=lambda d: -min(d, size - d))

    offsets = [(a, b) for a in by_distance(lines) for b in by_distance(planes)]

    near_lines = [place(plane_at, lax.rem(line + far, lines)) for far in (1, lines - 1)]
    near_planes = [place(lax.rem(plane_at + far, planes), line) for far in (2, 1, 3)]

    with jax.named_scope("signal"):
        for index in near_lines + near_planes + [mate_index(j) for j in (2, 1, 3)]:
            pl.semaphore_signal(barrier, inc=1, device_id=(group, index), device_id_type=MESH)

        @pl.when(chain)
        def _():
            pl.semaphore_signal(barrier, inc=1, device_id=(sibling, me), device_id_type=MESH)

        @pl.when(group == top)
        def _():
            pl.semaphore_signal(barrier, inc=1, device_id=(helper, me), device_id_type=MESH)
            pl.semaphore_signal(
                barrier, inc=1, device_id=(helper, clan_index(far_line, 0)), device_id_type=MESH
            )

    for load in loads:
        load.start()

    lane = lax.broadcasted_iota(jnp.int32, (1, cols), 1)
    in_slice = lax.rem(lane, 2 * slice_b)

    def pack(block, into):
        value = block[...].astype(F32)
        for m in range(MATES):
            parts = []
            for where in range(4):
                plane, upper = where % 2, where // 2
                piece = value[plane, upper * half : (upper + 1) * half, :]
                shift = (where - m) * slice_b % cols
                parts.append(pltpu.roll(piece, shift, 1) if shift else piece)
            tile = parts[3]
            for where in range(2, -1, -1):
                tile = jnp.where(lane < (where + 1) * slice_b, parts[where], tile)
            into[m] = tile.astype(BF16)

    border = harm - cols
    wide = harm + 2 * cols
    chunk = min(256, harm)

    with jax.named_scope("pack"):
        loads[1].wait()
        pack(source, packed_src)
        loads[2].wait()
        pack(fields, packed_fld)
        for buffer in (lined, shifted):
            buffer[:, pl.ds(0, border)] = jnp.zeros((2 * slice_b, border), BF16)
            buffer[:, pl.ds(border + wide, border)] = jnp.zeros((2 * slice_b, border), BF16)
        loads[3].wait()

    def arrange():
        value = rows_own[...].reshape(2 * rows, harm)
        count = harm // clan_rows
        stacked = jnp.concatenate(
            [value[:, k * clan_rows : (k + 1) * clan_rows] for k in range(count)], axis=0
        )
        at = lax.broadcasted_iota(jnp.int32, (clan_rows, 2 * clan_rows), 0)
        to = lax.broadcasted_iota(jnp.int32, (clan_rows, 2 * clan_rows), 1)
        inside = to % clan_rows
        upper = (inside // (clan_rows // 2) + to // clan_rows) % 2
        origin = inside % (clan_rows // 2) // half * rows + upper * half + inside % half
        order = jnp.where(at == origin, 1.0, 0.0).astype(BF16)
        moved = jnp.dot(stacked, order, preferred_element_type=F32)
        moved = moved.reshape(count, 2, rows, 2 * clan_rows)
        for z in range(lines):
            for pair in range(planes // 2):
                first = moved[2 * pair * lines + z]
                second = moved[(2 * pair + 1) * lines + z]
                lower = jnp.where(lane < cols // 2, first[:, :, :clan_rows], second[:, :, clan_rows:])
                upper = jnp.where(lane < cols // 2, first[:, :, clan_rows:], second[:, :, :clan_rows])
                start = z * share + pair * clan_rows
                rows_all[mate, :, :, pl.ds(start, clan_rows)] = lower.astype(BF16)
                rows_all[mate, :, :, pl.ds(start + share // 2, clan_rows)] = upper.astype(BF16)

    with jax.named_scope("arrange"):
        loads[0].wait()
        arrange()

    def build_fwd():
        with jax.named_scope("hotf"):

            @pl.loop(0, harm // chunk)
            def _(r):
                index = lax.broadcasted_iota(jnp.int32, (chunk, depth), 0)
                order = r * chunk + (index // band) * band + (band - 1) - index % band
                for k in range(steps):
                    hit = orders[:, pl.ds(k * depth, depth)] == order
                    hot_fwd[
                        pl.ds(pl.multiple_of(r * chunk, chunk), chunk), pl.ds(k * depth, depth)
                    ] = jnp.where(hit, 1.0, 0.0).astype(BF16)

    def build_adj():
        with jax.named_scope("hota"):
            for k in range(harm // cols):
                row = orders[:, pl.ds(k * cols, cols)].astype(F32)
                column[pl.ds(k * cols, cols), :] = jnp.broadcast_to(row, (cols, cols)).T

            @pl.loop(0, peers)
            def _(tile):
                owner = tile // MATES
                spot = (owner // lines) * MATES + tile % MATES
                for upper in range(2):
                    order = column[pl.ds(pl.multiple_of(tile * rows + upper * half, half), half), :]
                    row = (owner % lines) * share + upper * (share // 2) + spot * half
                    row = pl.ds(pl.multiple_of(row, half), half)
                    for k in range(wide // cols):
                        want = (lane + (k * cols - cols + 1)).astype(F32)
                        hot_adj[row, pl.ds(k * cols, cols)] = jnp.where(order == want, 1.0, 0.0).astype(BF16)

    with jax.named_scope("barrier"):

        close = len(near_lines) + len(near_planes) + MATES - 1

        @pl.when(jnp.logical_not(chain))
        def _():
            pl.semaphore_wait(barrier, close + 1)

        @pl.when(group == helper)
        def _():
            pl.semaphore_wait(barrier, close + 2)

        @pl.when(group == top)
        def _():
            pl.semaphore_wait(barrier, close)

        for index in near_planes:
            pl.semaphore_signal(plane_sem, inc=1, device_id=(group, index), device_id_type=MESH)

    def near_here():
        with jax.named_scope("near"):
            pl.semaphore_wait(plane_sem, len(near_planes))
            for index in near_lines:
                pl.semaphore_signal(line_sem, inc=1, device_id=(group, index), device_id_type=MESH)

    def all_here():
        with jax.named_scope("here"):
            pl.semaphore_wait(line_sem, len(near_lines))

            @pl.when(jnp.logical_not(chain))
            def _():
                pl.semaphore_signal(clear_sem, inc=1, device_id=(sibling, me), device_id_type=MESH)

            @pl.when(group == helper)
            def _():
                pl.semaphore_signal(clear_sem, inc=1, device_id=(top, me), device_id_type=MESH)

    def remote(src, dst, arrived, target, index):
        return pltpu.make_async_remote_copy(
            src_ref=src, dst_ref=dst, send_sem=send_sem, recv_sem=arrived,
            device_id=(target, index), device_id_type=MESH,
        )

    def wait_for(buffer, count, sem):
        part_of = buffer.at[pl.ds(0, count)]
        pltpu.make_async_copy(part_of, part_of, sem).wait()

    def to_mates(tiles, dst, arrived):
        for j in (2, 1, 3):
            other = lax.rem(mate + j, MATES)
            remote(
                tiles.at[other], dst.at[mate], arrived, group, clan * MATES + other
            ).start()
        dst[mate] = tiles[mate]

    clan_tiles = pl.ds(clan * MATES, MATES)

    def to_clans(tiles, dst, arrived, target, to):
        for a, b in to:
            remote(tiles, dst.at[clan_tiles], arrived, target, clan_index(a, b)).start()

    right, left = mate_index(1), mate_index(MATES - 1)
    from_left, from_right = lax.rem(mate + MATES - 1, MATES), lax.rem(mate + 1, MATES)

    def start_rows(buffer, turn):
        for first in (0, 1):
            to_right = buffer.at[mate, first]
            to_left = buffer.at[mate, 1 - first]
            for block, to, sem in ((to_right, right, 0), (to_left, left, 1)):
                remote(block, block, rows_sem.at[3 * turn + (2 if first else sem)], group, to).start()

    def wait_half(turn, sem):
        wait_for(rows_all.at[0], 1, rows_sem.at[3 * turn + sem])

    def relay_rows(buffer, turn):
        with jax.named_scope("relay_t%d" % turn):
            wait_half(turn, 0)
            block = buffer.at[from_left, 0]
            remote(block, block, rows_sem.at[3 * turn + 2], group, right).start()
            wait_half(turn, 1)
            block = buffer.at[from_right, 1]
            remote(block, block, rows_sem.at[3 * turn + 2], group, left).start()

    def wait_rows(turn):
        with jax.named_scope("wait_t%d" % turn):
            wait_for(rows_all, 2, rows_sem.at[3 * turn + 2])

    def to_sibling(src, dst, arrived):
        remote(src, dst, arrived, sibling, me).start()

    def to_sibling_mates(tiles, dst, arrived):
        for j in (2, 1, 3, 0):
            other = lax.rem(mate + j, MATES)
            remote(
                tiles.at[other], dst.at[mate], arrived, sibling, clan * MATES + other
            ).start()

    def start_fields():
        to_mates(packed_fld, stage_fld, stage_sem.at[0])

    def relay_fields():
        with jax.named_scope("relay_f"):
            wait_for(stage_fld, MATES - 1, stage_sem.at[0])
            to_clans(stage_fld, fwd, fwd_sem, group, offsets[:-1])
            fwd[clan_tiles] = stage_fld[...]

    with jax.named_scope("spread"):

        near = [offset for offset in offsets[:-1] if offset[0] != far_line]
        far = [offset for offset in offsets if offset[0] == far_line]

        def relay_source(to):
            with jax.named_scope("relay_s"):
                wait_for(stage_src, MATES - 1, stage_sem.at[1])
                to_clans(stage_src, adj, adj_sem.at[line], top, to)

        @pl.when(group == top)
        def _():
            to_mates(packed_src, stage_src, stage_sem.at[1])
            start_rows(rows_all, 0)
            near_here()
            relay_source(near)
            adj[clan_tiles] = stage_src[...]
            relay_rows(rows_all, 0)
            wait_for(rows_all, 1, hand_sem.at[0])
            start_rows(rows_two, 1)
            all_here()
            pl.semaphore_wait(clear_sem, 2)

        @pl.when(group == helper)
        def _():
            to_mates(packed_src, stage_src, stage_sem.at[1])
            near_here()
            relay_source(far)
            all_here()
            start_fields()
            start_rows(rows_all, 0)
            build_fwd()
            relay_fields()
            relay_rows(rows_all, 0)
            build_adj()
            pl.semaphore_wait(clear_sem, 1)
            pl.semaphore_signal(go_sem, inc=1, device_id=(sibling, me), device_id_type=MESH)

        @pl.when(jnp.logical_not(chain))
        def _():
            @pl.when(group == top - 1)
            def _():
                to_sibling(rows_all.at[mate], rows_two.at[mate], hand_sem.at[0])

            near_here()
            all_here()
            start_fields()

            @pl.when(group == 0)
            def _():
                start_rows(rows_all, 0)

            build_fwd()

            @pl.when(group == top - 1)
            def _():
                build_adj()

            @pl.when(group == 0)
            def _():
                relay_rows(rows_all, 0)

            pl.semaphore_wait(go_sem, 1)
            relay_fields()

    def unpack(tiles):
        count = tiles.shape[0]
        value = tiles.astype(F32)
        turned = pltpu.roll(value.reshape(count * half, cols), cols // 2, 1).reshape(value.shape)
        lower = jnp.where(lane < cols // 2, value, turned)
        upper = jnp.where(lane < cols // 2, turned, value)
        return jnp.concatenate([lower, upper], axis=1).reshape(count * rows, cols).astype(BF16)

    def share_tiles(tiles, z):
        return jnp.concatenate(
            [tiles[pl.ds((p * lines + z) * MATES, MATES)].reshape(MATES * half, cols) for p in range(planes)],
            axis=0,
        )

    def sort_shares(tiles, fars, first, last):
        shares = []
        for far in fars:
            z = lax.rem(line + far, lines)
            turned = share_tiles(tiles, z).astype(F32).T.astype(BF16)
            left = jnp.concatenate([turned[: cols // 2], turned[cols // 2 :]], axis=1)
            shares.append((left, pl.ds(pl.multiple_of(z * share, share), share)))
        left = jnp.concatenate([piece for piece, _ in shares], axis=1)
        span = 3 * depth if wide % (3 * depth) == 0 else wide
        tail = None
        for k in reversed(range(wide // span)):
            here = pl.ds(k * span, span)
            hot = jnp.concatenate([hot_adj[at, here] for _, at in shares], axis=0)
            total = jnp.dot(left, hot, preferred_element_type=F32)
            if not first:
                total += sorting[:, here]
            if not last:
                sorting[:, here] = total
                continue
            lined[:, pl.ds(border + k * span, span)] = total.astype(BF16)
            pieces = [
                pltpu.roll(total[:, i * cols : (i + 1) * cols], cols // 2, 1) for i in range(span // cols)
            ]
            pieces.append(jnp.zeros_like(pieces[0]) if tail is None else tail)
            tail = pieces[0]
            for i in range(span // cols):
                shifted[:, pl.ds(border + k * span + i * cols, cols)] = jnp.where(
                    lane < cols // 2, pieces[i], pieces[i + 1]
                ).astype(BF16)
        if last:
            shifted[:, pl.ds(border - cols, cols)] = jnp.where(lane < cols // 2, 0.0, tail).astype(BF16)

    near_first = by_distance(lines)[::-1]
    by_arrival = [near_first[:1], near_first[1:-1], near_first[-1:]]

    def receive(tiles, block_rows, sems, own_there, out):
        lower = jnp.zeros((MATES * 2 * rows, cols), F32)
        upper = jnp.zeros((MATES * 2 * rows, cols), F32)
        for step, fars in enumerate(by_arrival):
            spots = [lax.rem(line + far, lines) for far in fars]
            with jax.named_scope("wait_a%d" % step):
                for z in spots:
                    wait_for(tiles, MATES * (planes - (own_there and step == 0)), sems.at[z])
            with jax.named_scope("propagate"):
                packed = jnp.concatenate([share_tiles(tiles, z) for z in spots], axis=0)

                def product(upper_half):
                    starts = [z * share + upper_half * (share // 2) for z in spots]
                    matrix = jnp.concatenate(
                        [
                            block_rows[
                                :, :, :, pl.ds(pl.multiple_of(start, share // 2), share // 2)
                            ].reshape(MATES * 2 * rows, share // 2)
                            for start in starts
                        ],
                        axis=1,
                    )
                    return jnp.dot(matrix, packed, preferred_element_type=F32)

                lower += product(0)
                upper += product(1)
            if step == len(by_arrival) - 1:
                mixed = jnp.where(lane < cols // 2, lower, upper).reshape(MATES, 2, rows, cols)
                head, rest = mixed[:, :, :half], mixed[:, :, half:]
                here = jnp.where(lane < cols // 2, head, rest)
                there = jnp.where(lane < cols // 2, rest, head).reshape(MATES * 2 * half, cols)
                total = here + pltpu.roll(there, cols // 2, 1).reshape(MATES, 2, half, cols)
                cross = total[:, 1].reshape(MATES * half, cols)
                cross = jnp.where(
                    in_slice < slice_b,
                    -pltpu.roll(cross, cols - slice_b, 1),
                    pltpu.roll(cross, slice_b, 1),
                )
                out[...] = (total[:, 0] + cross.reshape(MATES, half, cols)).astype(BF16)

    def receive_sorted(tiles, sems):
        sorts = [near_first[:1], near_first[1:2], near_first[2:]]
        for step, fars in enumerate(by_arrival):
            for far in fars:
                z = lax.rem(line + far, lines)
                with jax.named_scope("wait_s%d" % far):
                    wait_for(tiles, MATES * (planes - (step == 0)), sems.at[z])
                for p in range(planes):
                    block = pl.ds((p * lines + z) * MATES, MATES)
                    to_sibling(tiles.at[block], tiles.at[block], sems.at[z])
            with jax.named_scope("sort0"):
                sort_shares(tiles, sorts[step], step == 0, step == len(by_arrival) - 1)

    def sort_all():
        with jax.named_scope("sorta"):
            sort_shares(adj, near_first, True, True)

    def first_layer():
        with jax.named_scope("forward1"):
            to_clans(outgoing, adj_two, two_sem.at[line], group, offsets[:-1])
            adj_two[clan_tiles] = outgoing[...]
            to_mates(outgoing, landed, land_sem)

    @pl.when(group == top)
    def _():
        wait_rows(0)
        receive(adj, rows_all, adj_sem, True, outgoing)
        first_layer()
        relay_rows(rows_two, 1)
        start_fields()
        build_fwd()
        build_adj()
        wait_rows(1)
        pl.semaphore_signal(go_sem, inc=1, device_id=(sibling, me), device_id_type=MESH)
        receive(adj_two, rows_two, two_sem, True, outgoing_two)
        with jax.named_scope("forward2"):
            to_clans(outgoing_two, adj, adj_sem.at[line], helper, offsets)
            to_sibling(adj_two, adj, hand_sem.at[1])
            to_sibling_mates(outgoing_two, landed, land_sem)
        sort_all()
        relay_fields()

    with jax.named_scope("wait_f"):
        wait_for(fwd, peers - MATES, fwd_sem)
    with jax.named_scope("sortf"):
        for k in range(steps):
            count = depth // rows
            flat_fwd = unpack(fwd[pl.ds(k * count, count)])
            stretched[pl.ds(k * depth, depth), :] = flat_fwd
        sign = jnp.where(in_slice < slice_b, 1.0, -1.0)
        quads = chunk // band

        @pl.loop(0, harm // chunk)
        def _(r):
            at = pl.ds(pl.multiple_of(r * chunk, chunk), chunk)
            total = jnp.dot(hot_fwd[at, :], stretched[...], preferred_element_type=F32)
            real = total * sign
            imag = pltpu.roll(total, slice_b, 1)
            for pair in range(quads // 2):
                lo, mid, hi = 2 * pair * band, (2 * pair + 1) * band, (2 * pair + 2) * band
                upper = jnp.where(lane < cols // 2, real[lo:mid], real[mid:hi])
                lower = jnp.where(lane < cols // 2, imag[lo:mid], imag[mid:hi])
                both = jnp.concatenate([upper, lower], axis=0)
                factor[r, :, pl.ds(pair * cols, cols)] = both.astype(BF16)

    def correlate(made, into):
        with jax.named_scope("gram"):
            quad = chunk // band
            view = (MATES + 2) * band
            window = []
            for n in range(harm // chunk):
                start = (MATES * clan + quad * n) * band
                for k in range(quad):
                    buffer = shifted if k % 2 else lined
                    at = pl.ds(pl.multiple_of(start + (k - k % 2) * band, 2 * band), view)
                    window.append(buffer[:, at])
            left = jnp.concatenate([made[n] for n in range(harm // chunk)], axis=1)
            gram = jnp.dot(left, jnp.concatenate(window, axis=0), preferred_element_type=F32)
            for m in range(MATES):
                if m % 2:
                    both = gram[:, (m - 1) * band : (m + 3) * band]
                    turned = pltpu.roll(both, 2 * band + 1, 1, stride=1, stride_axis=0)[:, : 2 * band]
                else:
                    both = gram[:, m * band : (m + 2) * band]
                    turned = pltpu.roll(both, band + 1, 1, stride=1, stride_axis=0)
                real = jnp.sum(turned[:band], axis=0, keepdims=True)
                imag = jnp.sum(turned[band:], axis=0, keepdims=True)
                into[m] = jnp.where(lane < band, real, imag)

    @pl.when(group == 0)
    def _():
        to_sibling(factor, factor_two, hand_sem.at[1])
        wait_rows(0)
        receive(adj_two, rows_all, two_sem, False, outgoing)
        to_mates(outgoing, landed, land_sem)

    @pl.when(group == top - 1)
    def _():
        with jax.named_scope("wait_adj"):
            wait_for(adj, peers, hand_sem.at[1])
        sort_all()

    @pl.when(group == helper)
    def _():
        wait_rows(0)
        receive(adj, rows_all, adj_sem, False, outgoing)
        first_layer()
        sort_all()

    @pl.when(group > 0)
    def _():
        correlate(factor, partial)
        to_mates(partial, gathered, part_sem)

    @pl.when(group == helper)
    def _():
        with jax.named_scope("wait_factor"):
            wait_for(factor_two, harm // chunk, hand_sem.at[1])
        receive_sorted(adj_two, two_sem)
        correlate(factor_two, partial_two)
        to_sibling_mates(partial_two, gathered, part_sem)

    with jax.named_scope("land"):
        @pl.when(group != top - 1)
        def _():
            wait_for(landed, MATES - 1, land_sem)

        @pl.when(group == top - 1)
        def _():
            wait_for(landed, MATES, land_sem)

        pieces = [landed[m].astype(F32) for m in range(MATES)]
        for plane in range(2):
            for upper in range(2):
                where = 2 * upper + plane
                tile = None
                for m in range(MATES):
                    shift = (m - where) * slice_b % cols
                    moved = pltpu.roll(pieces[m], shift, 1) if shift else pieces[m]
                    tile = moved if m == 0 else jnp.where(lane < m * slice_b, tile, moved)
                bound_ref[0, plane, pl.ds(upper * half, half), :] = tile.astype(BF16)

    with jax.named_scope("sum"):
        @pl.when(group > 0)
        def _():
            wait_for(gathered, MATES - 1, part_sem)

        @pl.when(group == 0)
        def _():
            wait_for(gathered, MATES, part_sem)

        total = gathered[0]
        for m in range(1, MATES):
            total = total + gathered[m]
        total = total * scale
        grads_ref[0, 0:1, :] = total[:, :band]
        grads_ref[0, 1:2, :] = total[:, band:]

    with jax.named_scope("drain"):
        wait_for(stage_fld, MATES - 1, send_sem)
        wait_for(fwd, peers - MATES, send_sem)

        @pl.when(group != top - 1)
        def _():
            wait_for(rows_all, 3, send_sem)
            wait_for(landed, MATES - 1, send_sem)

        @pl.when(chain)
        def _():
            wait_for(stage_src, MATES - 1, send_sem)
            wait_for(adj, peers - MATES, send_sem)
            wait_for(adj, peers, send_sem)

        @pl.when(group > 0)
        def _():
            wait_for(gathered, MATES - 1, send_sem)

        @pl.when(group == top)
        def _():
            wait_for(rows_all, 3, send_sem)
            wait_for(landed, MATES, send_sem)
            wait_for(adj, MATES * len(near), send_sem)
            wait_for(adj, peers, send_sem)

        @pl.when(group == top - 1)
        def _():
            wait_for(rows_all, 1, send_sem)

        @pl.when(group == helper)
        def _():
            wait_for(adj, MATES * len(far), send_sem)
            wait_for(gathered, MATES, send_sem)

        @pl.when(group == 0)
        def _():
            wait_for(factor, harm // chunk, send_sem)


def put_out(grads_ref, bound_ref, grads_hbm, bound_hbm, sems):
    copies = [
        pltpu.make_async_copy(bound_ref, bound_hbm, sems.at[0]),
        pltpu.make_async_copy(grads_ref, grads_hbm, sems.at[1]),
    ]
    for copy in copies:
        copy.start()
    for copy in copies:
        copy.wait()


def solution(mesh):
    layers, peers = mesh.shape["layer"], mesh.shape["harm"]

    def per_device(source, transfer, fields, orders):
        rows, cols = source.shape[1], source.shape[2]
        harm = rows * peers
        band = 2 * rows
        chunk = min(256, harm)
        vmem = pl.BlockSpec(memory_space=pltpu.VMEM)
        hbm = pl.BlockSpec(memory_space=pltpu.HBM)
        tile = (rows // 2, cols)
        made = pl.pallas_call(
            functools.partial(kernel, layers, peers, 1.0 / math.sqrt(harm * cols)),
            out_shape=(
                jax.ShapeDtypeStruct((1, 2, band), F32),
                jax.ShapeDtypeStruct((1, 2, rows, cols), BF16),
            ),
            in_specs=[hbm] * 4,
            out_specs=(vmem, vmem),
            scratch_shapes=[
                pltpu.VMEM((2, rows, cols), BF16),
                pltpu.VMEM((2, rows, cols), BF16),
                pltpu.VMEM((1, harm), jnp.int32),
                pltpu.VMEM((2, rows, harm), BF16),
                *[pltpu.VMEM((MATES, 2, rows, harm), BF16)] * 2,
                *[pltpu.VMEM((peers, *tile), BF16)] * 3,
                pltpu.VMEM((harm, cols), BF16),
                pltpu.VMEM((harm, cols), F32),
                pltpu.VMEM((harm, harm), BF16),
                pltpu.VMEM((harm, harm + 2 * cols), BF16),
                pltpu.VMEM((2 * cols // MATES, 3 * harm), BF16),
                pltpu.VMEM((2 * cols // MATES, 3 * harm), BF16),
                *[pltpu.VMEM((harm // chunk, 2 * band, chunk // band * 2 * (cols // MATES)), BF16)] * 2,
                *[pltpu.VMEM((MATES, *tile), BF16)] * 7,
                *[pltpu.VMEM((MATES, 1, cols), F32)] * 3,
                pltpu.VMEM((2 * cols // MATES, harm + 2 * cols), F32),
                pltpu.SemaphoreType.DMA((4,)),
                pltpu.SemaphoreType.DMA,
                pltpu.SemaphoreType.DMA((6,)),
                pltpu.SemaphoreType.DMA((LINES,)),
                pltpu.SemaphoreType.DMA((LINES,)),
                pltpu.SemaphoreType.DMA((2,)),
                pltpu.SemaphoreType.DMA,
                pltpu.SemaphoreType.DMA((2,)),
                pltpu.SemaphoreType.DMA,
                pltpu.SemaphoreType.DMA,
                *[pltpu.SemaphoreType.REGULAR] * 4,
            ],
            compiler_params=pltpu.CompilerParams(
                collective_id=0, has_side_effects=True, vmem_limit_bytes=44 * 1024 * 1024
            ),
        )(
            *(
                pltpu.with_memory_space_constraint(value, pltpu.HBM)
                for value in (source, transfer, fields, orders.reshape(1, harm))
            )
        )
        return pl.pallas_call(
            put_out,
            out_shape=[jax.ShapeDtypeStruct(value.shape, value.dtype) for value in made],
            in_specs=[vmem] * 2,
            out_specs=[hbm] * 2,
            scratch_shapes=[pltpu.SemaphoreType.DMA((2,))],
            compiler_params=pltpu.CompilerParams(vmem_limit_bytes=1 << 20),
        )(*(pltpu.with_memory_space_constraint(value, pltpu.VMEM) for value in made))

    return jax.shard_map(
        per_device,
        mesh=mesh,
        in_specs=(
            P(None, "harm", None),
            P("layer", None, "harm", None),
            P("layer", None, "harm", None),
            P(),
        ),
        out_specs=(P("layer", None, "harm"), P("layer", None, "harm", None)),
        check_vma=False,
    )
```

```python
import functools
import math

import jax
import jax.numpy as jnp
from jax import lax
from jax.experimental import pallas as pl
from jax.experimental.pallas import tpu as pltpu
from jax.sharding import PartitionSpec as P

MESH = pl.DeviceIdType.MESH
F32 = jnp.float32
BF16 = jnp.bfloat16
MATES = 4
LINES = 4


def kernel(
    layers, peers, scale,
    source_hbm, transfer_hbm, fields_hbm, orders_hbm, grads_ref, bound_ref,
    source, fields, orders, rows_own, rows_all, rows_two, adj, adj_two, fwd, stretched, column, hot_fwd, hot_adj, lined, shifted, factor, factor_two,
    packed_src, packed_fld, stage_src, stage_fld, outgoing, outgoing_two, landed, partial, partial_two, gathered, sorting,
    load_sem, send_sem, rows_sem, adj_sem, two_sem, hand_sem, fwd_sem, stage_sem, land_sem, part_sem, clear_sem, line_sem, plane_sem, go_sem,
):
    group = lax.axis_index("layer")
    me = lax.axis_index("harm")
    mate = me % MATES
    clan = me // MATES
    clans = peers // MATES
    lines = min(LINES, clans)
    planes = clans // lines
    line = clan % lines
    plane_at = clan // lines
    rows = source.shape[1]
    half = rows // 2
    cols = source.shape[2]
    slice_b = cols // MATES
    harm = rows * peers
    band = 2 * rows
    depth = min(256, harm)
    steps = harm // depth
    top = layers - 1
    helper = top - 2
    chain = (group == top) | (group == helper)
    sibling = jnp.where(chain, jnp.maximum(group - 1, 0), jnp.minimum(group + 1, top))
    far_line = lines // 2
    clan_rows = MATES * rows
    share = planes * clan_rows

    loads = [
        pltpu.make_async_copy(transfer_hbm.at[0], rows_own, load_sem.at[3]),
        pltpu.make_async_copy(source_hbm, source, load_sem.at[0]),
        pltpu.make_async_copy(fields_hbm.at[0], fields, load_sem.at[2]),
        pltpu.make_async_copy(orders_hbm, orders, load_sem.at[1]),
    ]
    barrier = pltpu.get_barrier_semaphore()

    def mate_index(j):
        return clan * MATES + lax.rem(mate + j, MATES)

    def place(plane, line_of):
        return (plane * lines + line_of) * MATES + mate

    def clan_index(far_line, far_plane):
        return place(lax.rem(plane_at + far_plane, planes), lax.rem(line + far_line, lines))

    def by_distance(size):
        return sorted(range(size), key=lambda d: -min(d, size - d))

    offsets = [(a, b) for a in by_distance(lines) for b in by_distance(planes)]

    near_lines = [place(plane_at, lax.rem(line + far, lines)) for far in (1, lines - 1)]
    near_planes = [place(lax.rem(plane_at + far, planes), line) for far in (2, 1, 3)]

    with jax.named_scope("signal"):
        for index in near_lines + near_planes + [mate_index(j) for j in (2, 1, 3)]:
            pl.semaphore_signal(barrier, inc=1, device_id=(group, index), device_id_type=MESH)

        @pl.when(chain)
        def _():
            pl.semaphore_signal(barrier, inc=1, device_id=(sibling, me), device_id_type=MESH)

        @pl.when(group == top)
        def _():
            pl.semaphore_signal(barrier, inc=1, device_id=(helper, me), device_id_type=MESH)
            pl.semaphore_signal(
                barrier, inc=1, device_id=(helper, clan_index(far_line, 0)), device_id_type=MESH
            )

    for load in loads:
        load.start()

    lane = lax.broadcasted_iota(jnp.int32, (1, cols), 1)
    in_slice = lax.rem(lane, 2 * slice_b)

    def pack(block, into):
        value = block[...].astype(F32)
        for m in range(MATES):
            parts = []
            for where in range(4):
                plane, upper = where % 2, where // 2
                piece = value[plane, upper * half : (upper + 1) * half, :]
                shift = (where - m) * slice_b % cols
                parts.append(pltpu.roll(piece, shift, 1) if shift else piece)
            tile = parts[3]
            for where in range(2, -1, -1):
                tile = jnp.where(lane < (where + 1) * slice_b, parts[where], tile)
            into[m] = tile.astype(BF16)

    border = harm - cols
    wide = harm + 2 * cols
    chunk = min(256, harm)

    with jax.named_scope("pack"):
        loads[1].wait()
        pack(source, packed_src)
        loads[2].wait()
        pack(fields, packed_fld)
        for buffer in (lined, shifted):
            buffer[:, pl.ds(0, border)] = jnp.zeros((2 * slice_b, border), BF16)
            buffer[:, pl.ds(border + wide, border)] = jnp.zeros((2 * slice_b, border), BF16)
        loads[3].wait()

    def arrange():
        value = rows_own[...].reshape(2 * rows, harm)
        count = harm // clan_rows
        stacked = jnp.concatenate(
            [value[:, k * clan_rows : (k + 1) * clan_rows] for k in range(count)], axis=0
        )
        at = lax.broadcasted_iota(jnp.int32, (clan_rows, 2 * clan_rows), 0)
        to = lax.broadcasted_iota(jnp.int32, (clan_rows, 2 * clan_rows), 1)
        inside = to % clan_rows
        upper = (inside // (clan_rows // 2) + to // clan_rows) % 2
        origin = inside % (clan_rows // 2) // half * rows + upper * half + inside % half
        order = jnp.where(at == origin, 1.0, 0.0).astype(BF16)
        moved = jnp.dot(stacked, order, preferred_element_type=F32)
        moved = moved.reshape(count, 2, rows, 2 * clan_rows)
        for z in range(lines):
            for pair in range(planes // 2):
                first = moved[2 * pair * lines + z]
                second = moved[(2 * pair + 1) * lines + z]
                lower = jnp.where(lane < cols // 2, first[:, :, :clan_rows], second[:, :, clan_rows:])
                upper = jnp.where(lane < cols // 2, first[:, :, clan_rows:], second[:, :, :clan_rows])
                start = z * share + pair * clan_rows
                rows_all[mate, :, :, pl.ds(start, clan_rows)] = lower.astype(BF16)
                rows_all[mate, :, :, pl.ds(start + share // 2, clan_rows)] = upper.astype(BF16)

    with jax.named_scope("arrange"):
        loads[0].wait()
        arrange()

    def build_fwd():
        with jax.named_scope("hotf"):

            @pl.loop(0, harm // chunk)
            def _(r):
                index = lax.broadcasted_iota(jnp.int32, (chunk, depth), 0)
                order = r * chunk + (index // band) * band + (band - 1) - index % band
                for k in range(steps):
                    hit = orders[:, pl.ds(k * depth, depth)] == order
                    hot_fwd[
                        pl.ds(pl.multiple_of(r * chunk, chunk), chunk), pl.ds(k * depth, depth)
                    ] = jnp.where(hit, 1.0, 0.0).astype(BF16)

    def build_adj():
        with jax.named_scope("hota"):
            for k in range(harm // cols):
                row = orders[:, pl.ds(k * cols, cols)].astype(F32)
                column[pl.ds(k * cols, cols), :] = jnp.broadcast_to(row, (cols, cols)).T

            @pl.loop(0, peers)
            def _(tile):
                owner = tile // MATES
                spot = (owner // lines) * MATES + tile % MATES
                for upper in range(2):
                    order = column[pl.ds(pl.multiple_of(tile * rows + upper * half, half), half), :]
                    row = (owner % lines) * share + upper * (share // 2) + spot * half
                    row = pl.ds(pl.multiple_of(row, half), half)
                    for k in range(wide // cols):
                        want = (lane + (k * cols - cols + 1)).astype(F32)
                        hot_adj[row, pl.ds(k * cols, cols)] = jnp.where(order == want, 1.0, 0.0).astype(BF16)

    with jax.named_scope("barrier"):

        close = len(near_lines) + len(near_planes) + MATES - 1

        @pl.when(jnp.logical_not(chain))
        def _():
            pl.semaphore_wait(barrier, close + 1)

        @pl.when(group == helper)
        def _():
            pl.semaphore_wait(barrier, close + 2)

        @pl.when(group == top)
        def _():
            pl.semaphore_wait(barrier, close)

        for index in near_planes:
            pl.semaphore_signal(plane_sem, inc=1, device_id=(group, index), device_id_type=MESH)

    def near_here():
        with jax.named_scope("near"):
            pl.semaphore_wait(plane_sem, len(near_planes))
            for index in near_lines:
                pl.semaphore_signal(line_sem, inc=1, device_id=(group, index), device_id_type=MESH)

    def all_here():
        with jax.named_scope("here"):
            pl.semaphore_wait(line_sem, len(near_lines))

            @pl.when(jnp.logical_not(chain))
            def _():
                pl.semaphore_signal(clear_sem, inc=1, device_id=(sibling, me), device_id_type=MESH)

            @pl.when(group == helper)
            def _():
                pl.semaphore_signal(clear_sem, inc=1, device_id=(top, me), device_id_type=MESH)

    def remote(src, dst, arrived, target, index):
        return pltpu.make_async_remote_copy(
            src_ref=src, dst_ref=dst, send_sem=send_sem, recv_sem=arrived,
            device_id=(target, index), device_id_type=MESH,
        )

    def wait_for(buffer, count, sem):
        part_of = buffer.at[pl.ds(0, count)]
        pltpu.make_async_copy(part_of, part_of, sem).wait()

    def to_mates(tiles, dst, arrived):
        for j in (2, 1, 3):
            other = lax.rem(mate + j, MATES)
            remote(
                tiles.at[other], dst.at[mate], arrived, group, clan * MATES + other
            ).start()
        dst[mate] = tiles[mate]

    clan_tiles = pl.ds(clan * MATES, MATES)

    def to_clans(tiles, dst, arrived, target, to):
        for a, b in to:
            remote(tiles, dst.at[clan_tiles], arrived, target, clan_index(a, b)).start()

    right, left = mate_index(1), mate_index(MATES - 1)
    from_left, from_right = lax.rem(mate + MATES - 1, MATES), lax.rem(mate + 1, MATES)

    def start_rows(buffer, turn):
        for first in (0, 1):
            to_right = buffer.at[mate, first]
            to_left = buffer.at[mate, 1 - first]
            for block, to, sem in ((to_right, right, 0), (to_left, left, 1)):
                remote(block, block, rows_sem.at[3 * turn + (2 if first else sem)], group, to).start()

    def wait_half(turn, sem):
        wait_for(rows_all.at[0], 1, rows_sem.at[3 * turn + sem])

    def relay_rows(buffer, turn):
        with jax.named_scope("relay_t%d" % turn):
            wait_half(turn, 0)
            block = buffer.at[from_left, 0]
            remote(block, block, rows_sem.at[3 * turn + 2], group, right).start()
            wait_half(turn, 1)
            block = buffer.at[from_right, 1]
            remote(block, block, rows_sem.at[3 * turn + 2], group, left).start()

    def wait_rows(turn):
        with jax.named_scope("wait_t%d" % turn):
            wait_for(rows_all, 2, rows_sem.at[3 * turn + 2])

    def to_sibling(src, dst, arrived):
        remote(src, dst, arrived, sibling, me).start()

    def to_sibling_mates(tiles, dst, arrived):
        for j in (2, 1, 3, 0):
            other = lax.rem(mate + j, MATES)
            remote(
                tiles.at[other], dst.at[mate], arrived, sibling, clan * MATES + other
            ).start()

    def start_fields():
        to_mates(packed_fld, stage_fld, stage_sem.at[0])

    def relay_fields():
        with jax.named_scope("relay_f"):
            wait_for(stage_fld, MATES - 1, stage_sem.at[0])
            to_clans(stage_fld, fwd, fwd_sem, group, offsets[:-1])
            fwd[clan_tiles] = stage_fld[...]

    with jax.named_scope("spread"):

        near = [offset for offset in offsets[:-1] if offset[0] != far_line]
        far = [offset for offset in offsets if offset[0] == far_line]

        def relay_source(to):
            with jax.named_scope("relay_s"):
                wait_for(stage_src, MATES - 1, stage_sem.at[1])
                to_clans(stage_src, adj, adj_sem.at[line], top, to)

        @pl.when(group == top)
        def _():
            to_mates(packed_src, stage_src, stage_sem.at[1])
            start_rows(rows_all, 0)
            near_here()
            relay_source(near)
            adj[clan_tiles] = stage_src[...]
            relay_rows(rows_all, 0)
            wait_for(rows_all, 1, hand_sem.at[0])
            start_rows(rows_two, 1)
            all_here()
            pl.semaphore_wait(clear_sem, 2)

        @pl.when(group == helper)
        def _():
            to_mates(packed_src, stage_src, stage_sem.at[1])
            near_here()
            relay_source(far)
            all_here()
            start_fields()
            start_rows(rows_all, 0)
            build_fwd()
            relay_fields()
            relay_rows(rows_all, 0)
            build_adj()
            pl.semaphore_wait(clear_sem, 1)

        @pl.when(jnp.logical_not(chain))
        def _():
            @pl.when(group == top - 1)
            def _():
                to_sibling(rows_all.at[mate], rows_two.at[mate], hand_sem.at[0])

            near_here()
            all_here()
            start_fields()

            @pl.when(group == 0)
            def _():
                start_rows(rows_all, 0)

            build_fwd()

            @pl.when(group == top - 1)
            def _():
                build_adj()

            @pl.when(group == 0)
            def _():
                relay_rows(rows_all, 0)

            pl.semaphore_wait(go_sem, 1)
            relay_fields()

    def unpack(tiles):
        count = tiles.shape[0]
        value = tiles.astype(F32)
        turned = pltpu.roll(value.reshape(count * half, cols), cols // 2, 1).reshape(value.shape)
        lower = jnp.where(lane < cols // 2, value, turned)
        upper = jnp.where(lane < cols // 2, turned, value)
        return jnp.concatenate([lower, upper], axis=1).reshape(count * rows, cols).astype(BF16)

    def share_tiles(tiles, z):
        return jnp.concatenate(
            [tiles[pl.ds((p * lines + z) * MATES, MATES)].reshape(MATES * half, cols) for p in range(planes)],
            axis=0,
        )

    def sort_shares(tiles, fars, first, last):
        shares = []
        for far in fars:
            z = lax.rem(line + far, lines)
            turned = share_tiles(tiles, z).astype(F32).T.astype(BF16)
            left = jnp.concatenate([turned[: cols // 2], turned[cols // 2 :]], axis=1)
            shares.append((left, pl.ds(pl.multiple_of(z * share, share), share)))
        left = jnp.concatenate([piece for piece, _ in shares], axis=1)
        span = 3 * depth if wide % (3 * depth) == 0 else wide
        tail = None
        for k in reversed(range(wide // span)):
            here = pl.ds(k * span, span)
            hot = jnp.concatenate([hot_adj[at, here] for _, at in shares], axis=0)
            total = jnp.dot(left, hot, preferred_element_type=F32)
            if not first:
                total += sorting[:, here]
            if not last:
                sorting[:, here] = total
                continue
            lined[:, pl.ds(border + k * span, span)] = total.astype(BF16)
            pieces = [
                pltpu.roll(total[:, i * cols : (i + 1) * cols], cols // 2, 1) for i in range(span // cols)
            ]
            pieces.append(jnp.zeros_like(pieces[0]) if tail is None else tail)
            tail = pieces[0]
            for i in range(span // cols):
                shifted[:, pl.ds(border + k * span + i * cols, cols)] = jnp.where(
                    lane < cols // 2, pieces[i], pieces[i + 1]
                ).astype(BF16)
        if last:
            shifted[:, pl.ds(border - cols, cols)] = jnp.where(lane < cols // 2, 0.0, tail).astype(BF16)

    near_first = by_distance(lines)[::-1]
    by_arrival = [near_first[:1], near_first[1:-1], near_first[-1:]]

    def receive(tiles, block_rows, sems, own_there, out):
        lower = jnp.zeros((MATES * 2 * rows, cols), F32)
        upper = jnp.zeros((MATES * 2 * rows, cols), F32)
        for step, fars in enumerate(by_arrival):
            spots = [lax.rem(line + far, lines) for far in fars]
            with jax.named_scope("wait_a%d" % step):
                for z in spots:
                    wait_for(tiles, MATES * (planes - (own_there and step == 0)), sems.at[z])
            with jax.named_scope("propagate"):
                packed = jnp.concatenate([share_tiles(tiles, z) for z in spots], axis=0)

                def product(upper_half):
                    starts = [z * share + upper_half * (share // 2) for z in spots]
                    matrix = jnp.concatenate(
                        [
                            block_rows[
                                :, :, :, pl.ds(pl.multiple_of(start, share // 2), share // 2)
                            ].reshape(MATES * 2 * rows, share // 2)
                            for start in starts
                        ],
                        axis=1,
                    )
                    return jnp.dot(matrix, packed, preferred_element_type=F32)

                lower += product(0)
                upper += product(1)
            if step == len(by_arrival) - 1:
                mixed = jnp.where(lane < cols // 2, lower, upper).reshape(MATES, 2, rows, cols)
                head, rest = mixed[:, :, :half], mixed[:, :, half:]
                here = jnp.where(lane < cols // 2, head, rest)
                there = jnp.where(lane < cols // 2, rest, head).reshape(MATES * 2 * half, cols)
                total = here + pltpu.roll(there, cols // 2, 1).reshape(MATES, 2, half, cols)
                cross = total[:, 1].reshape(MATES * half, cols)
                cross = jnp.where(
                    in_slice < slice_b,
                    -pltpu.roll(cross, cols - slice_b, 1),
                    pltpu.roll(cross, slice_b, 1),
                )
                out[...] = (total[:, 0] + cross.reshape(MATES, half, cols)).astype(BF16)

    def receive_sorted(tiles, sems):
        sorts = [near_first[:1], near_first[1:2], near_first[2:]]
        for step, fars in enumerate(by_arrival):
            for far in fars:
                z = lax.rem(line + far, lines)
                with jax.named_scope("wait_s%d" % far):
                    wait_for(tiles, MATES * (planes - (step == 0)), sems.at[z])
                for p in range(planes):
                    block = pl.ds((p * lines + z) * MATES, MATES)
                    to_sibling(tiles.at[block], tiles.at[block], sems.at[z])
            with jax.named_scope("sort0"):
                sort_shares(tiles, sorts[step], step == 0, step == len(by_arrival) - 1)

    def sort_all():
        with jax.named_scope("sorta"):
            sort_shares(adj, near_first, True, True)

    def first_layer():
        with jax.named_scope("forward1"):
            to_clans(outgoing, adj_two, two_sem.at[line], group, offsets[:-1])
            adj_two[clan_tiles] = outgoing[...]
            to_mates(outgoing, landed, land_sem)

    @pl.when(group == top)
    def _():
        wait_rows(0)
        receive(adj, rows_all, adj_sem, True, outgoing)
        first_layer()
        relay_rows(rows_two, 1)
        start_fields()
        build_fwd()
        wait_rows(1)
        pl.semaphore_signal(go_sem, inc=1, device_id=(sibling, me), device_id_type=MESH)
        receive(adj_two, rows_two, two_sem, True, outgoing_two)
        with jax.named_scope("forward2"):
            to_clans(outgoing_two, adj, adj_sem.at[line], helper, offsets)
            to_sibling(adj_two, adj, hand_sem.at[1])
            to_sibling_mates(outgoing_two, landed, land_sem)
        relay_fields()
        build_adj()
        sort_all()

    with jax.named_scope("wait_f"):
        wait_for(fwd, peers - MATES, fwd_sem)

        @pl.when(group == helper)
        def _():
            pl.semaphore_signal(go_sem, inc=1, device_id=(sibling, me), device_id_type=MESH)

    with jax.named_scope("sortf"):
        for k in range(steps):
            count = depth // rows
            flat_fwd = unpack(fwd[pl.ds(k * count, count)])
            stretched[pl.ds(k * depth, depth), :] = flat_fwd
        sign = jnp.where(in_slice < slice_b, 1.0, -1.0)
        quads = chunk // band

        @pl.loop(0, harm // chunk)
        def _(r):
            at = pl.ds(pl.multiple_of(r * chunk, chunk), chunk)
            total = jnp.dot(hot_fwd[at, :], stretched[...], preferred_element_type=F32)
            real = total * sign
            imag = pltpu.roll(total, slice_b, 1)
            for pair in range(quads // 2):
                lo, mid, hi = 2 * pair * band, (2 * pair + 1) * band, (2 * pair + 2) * band
                upper = jnp.where(lane < cols // 2, real[lo:mid], real[mid:hi])
                lower = jnp.where(lane < cols // 2, imag[lo:mid], imag[mid:hi])
                both = jnp.concatenate([upper, lower], axis=0)
                factor[r, :, pl.ds(pair * cols, cols)] = both.astype(BF16)

    def correlate(made, into):
        with jax.named_scope("gram"):
            quad = chunk // band
            view = (MATES + 2) * band
            window = []
            for n in range(harm // chunk):
                start = (MATES * clan + quad * n) * band
                for k in range(quad):
                    buffer = shifted if k % 2 else lined
                    at = pl.ds(pl.multiple_of(start + (k - k % 2) * band, 2 * band), view)
                    window.append(buffer[:, at])
            left = jnp.concatenate([made[n] for n in range(harm // chunk)], axis=1)
            gram = jnp.dot(left, jnp.concatenate(window, axis=0), preferred_element_type=F32)
            for m in range(MATES):
                if m % 2:
                    both = gram[:, (m - 1) * band : (m + 3) * band]
                    turned = pltpu.roll(both, 2 * band + 1, 1, stride=1, stride_axis=0)[:, : 2 * band]
                else:
                    both = gram[:, m * band : (m + 2) * band]
                    turned = pltpu.roll(both, band + 1, 1, stride=1, stride_axis=0)
                real = jnp.sum(turned[:band], axis=0, keepdims=True)
                imag = jnp.sum(turned[band:], axis=0, keepdims=True)
                into[m] = jnp.where(lane < band, real, imag)

    @pl.when(group == 0)
    def _():
        to_sibling(factor, factor_two, hand_sem.at[1])
        wait_rows(0)
        receive(adj_two, rows_all, two_sem, False, outgoing)
        to_mates(outgoing, landed, land_sem)

    @pl.when(group == top - 1)
    def _():
        with jax.named_scope("wait_adj"):
            wait_for(adj, peers, hand_sem.at[1])
        sort_all()

    @pl.when(group == helper)
    def _():
        wait_rows(0)
        receive(adj, rows_all, adj_sem, False, outgoing)
        first_layer()
        sort_all()

    @pl.when(group > 0)
    def _():
        correlate(factor, partial)
        to_mates(partial, gathered, part_sem)

    @pl.when(group == helper)
    def _():
        receive_sorted(adj_two, two_sem)
        with jax.named_scope("wait_factor"):
            wait_for(factor_two, harm // chunk, hand_sem.at[1])
        correlate(factor_two, partial_two)
        to_sibling_mates(partial_two, gathered, part_sem)

    with jax.named_scope("land"):
        @pl.when(group != top - 1)
        def _():
            wait_for(landed, MATES - 1, land_sem)

        @pl.when(group == top - 1)
        def _():
            wait_for(landed, MATES, land_sem)

        pieces = [landed[m].astype(F32) for m in range(MATES)]
        for plane in range(2):
            for upper in range(2):
                where = 2 * upper + plane
                tile = None
                for m in range(MATES):
                    shift = (m - where) * slice_b % cols
                    moved = pltpu.roll(pieces[m], shift, 1) if shift else pieces[m]
                    tile = moved if m == 0 else jnp.where(lane < m * slice_b, tile, moved)
                bound_ref[0, plane, pl.ds(upper * half, half), :] = tile.astype(BF16)

    with jax.named_scope("sum"):
        @pl.when(group > 0)
        def _():
            wait_for(gathered, MATES - 1, part_sem)

        @pl.when(group == 0)
        def _():
            wait_for(gathered, MATES, part_sem)

        total = gathered[0]
        for m in range(1, MATES):
            total = total + gathered[m]
        total = total * scale
        grads_ref[0, 0:1, :] = total[:, :band]
        grads_ref[0, 1:2, :] = total[:, band:]

    with jax.named_scope("drain"):
        wait_for(stage_fld, MATES - 1, send_sem)
        wait_for(fwd, peers - MATES, send_sem)

        @pl.when(group != top - 1)
        def _():
            wait_for(rows_all, 3, send_sem)
            wait_for(landed, MATES - 1, send_sem)

        @pl.when(chain)
        def _():
            wait_for(stage_src, MATES - 1, send_sem)
            wait_for(adj, peers - MATES, send_sem)
            wait_for(adj, peers, send_sem)

        @pl.when(group > 0)
        def _():
            wait_for(gathered, MATES - 1, send_sem)

        @pl.when(group == top)
        def _():
            wait_for(rows_all, 3, send_sem)
            wait_for(landed, MATES, send_sem)
            wait_for(adj, MATES * len(near), send_sem)
            wait_for(adj, peers, send_sem)

        @pl.when(group == top - 1)
        def _():
            wait_for(rows_all, 1, send_sem)

        @pl.when(group == helper)
        def _():
            wait_for(adj, MATES * len(far), send_sem)
            wait_for(gathered, MATES, send_sem)

        @pl.when(group == 0)
        def _():
            wait_for(factor, harm // chunk, send_sem)


def put_out(grads_ref, bound_ref, grads_hbm, bound_hbm, sems):
    copies = [
        pltpu.make_async_copy(bound_ref, bound_hbm, sems.at[0]),
        pltpu.make_async_copy(grads_ref, grads_hbm, sems.at[1]),
    ]
    for copy in copies:
        copy.start()
    for copy in copies:
        copy.wait()


def solution(mesh):
    layers, peers = mesh.shape["layer"], mesh.shape["harm"]

    def per_device(source, transfer, fields, orders):
        rows, cols = source.shape[1], source.shape[2]
        harm = rows * peers
        band = 2 * rows
        chunk = min(256, harm)
        vmem = pl.BlockSpec(memory_space=pltpu.VMEM)
        hbm = pl.BlockSpec(memory_space=pltpu.HBM)
        tile = (rows // 2, cols)
        made = pl.pallas_call(
            functools.partial(kernel, layers, peers, 1.0 / math.sqrt(harm * cols)),
            out_shape=(
                jax.ShapeDtypeStruct((1, 2, band), F32),
                jax.ShapeDtypeStruct((1, 2, rows, cols), BF16),
            ),
            in_specs=[hbm] * 4,
            out_specs=(vmem, vmem),
            scratch_shapes=[
                pltpu.VMEM((2, rows, cols), BF16),
                pltpu.VMEM((2, rows, cols), BF16),
                pltpu.VMEM((1, harm), jnp.int32),
                pltpu.VMEM((2, rows, harm), BF16),
                *[pltpu.VMEM((MATES, 2, rows, harm), BF16)] * 2,
                *[pltpu.VMEM((peers, *tile), BF16)] * 3,
                pltpu.VMEM((harm, cols), BF16),
                pltpu.VMEM((harm, cols), F32),
                pltpu.VMEM((harm, harm), BF16),
                pltpu.VMEM((harm, harm + 2 * cols), BF16),
                pltpu.VMEM((2 * cols // MATES, 3 * harm), BF16),
                pltpu.VMEM((2 * cols // MATES, 3 * harm), BF16),
                *[pltpu.VMEM((harm // chunk, 2 * band, chunk // band * 2 * (cols // MATES)), BF16)] * 2,
                *[pltpu.VMEM((MATES, *tile), BF16)] * 7,
                *[pltpu.VMEM((MATES, 1, cols), F32)] * 3,
                pltpu.VMEM((2 * cols // MATES, harm + 2 * cols), F32),
                pltpu.SemaphoreType.DMA((4,)),
                pltpu.SemaphoreType.DMA,
                pltpu.SemaphoreType.DMA((6,)),
                pltpu.SemaphoreType.DMA((LINES,)),
                pltpu.SemaphoreType.DMA((LINES,)),
                pltpu.SemaphoreType.DMA((2,)),
                pltpu.SemaphoreType.DMA,
                pltpu.SemaphoreType.DMA((2,)),
                pltpu.SemaphoreType.DMA,
                pltpu.SemaphoreType.DMA,
                *[pltpu.SemaphoreType.REGULAR] * 4,
            ],
            compiler_params=pltpu.CompilerParams(
                collective_id=0, has_side_effects=True, vmem_limit_bytes=44 * 1024 * 1024
            ),
        )(
            *(
                pltpu.with_memory_space_constraint(value, pltpu.HBM)
                for value in (source, transfer, fields, orders.reshape(1, harm))
            )
        )
        return pl.pallas_call(
            put_out,
            out_shape=[jax.ShapeDtypeStruct(value.shape, value.dtype) for value in made],
            in_specs=[vmem] * 2,
            out_specs=[hbm] * 2,
            scratch_shapes=[pltpu.SemaphoreType.DMA((2,))],
            compiler_params=pltpu.CompilerParams(vmem_limit_bytes=1 << 20),
        )(*(pltpu.with_memory_space_constraint(value, pltpu.VMEM) for value in made))

    return jax.shard_map(
        per_device,
        mesh=mesh,
        in_specs=(
            P(None, "harm", None),
            P("layer", None, "harm", None),
            P("layer", None, "harm", None),
            P(),
        ),
        out_specs=(P("layer", None, "harm"), P("layer", None, "harm", None)),
        check_vma=False,
    )
```
